32 devices in a mesh: group: 2 (over y), batch: 4 (over z), expert: 4 (over x, core).
Axes of the slice: x: 2, y: 2, z: 4, core: 2. Of those that a mesh axis runs over, the one named last changes fastest.
Arguments:
- residual_in: bfloat16 [128, 4096], P(('group', 'batch')), parts along dimension 0, may hold values from -11 to 11
- queries: bfloat16 [128, 16, 128], P(('group', 'batch'), 'expert'), parts along dimension 0, may hold values from -150 to 150
- key_new: bfloat16 [128, 4, 128], P(('group', 'batch'), 'expert'), parts along dimension 0, may hold values from -6 to 6
- value_new: bfloat16 [128, 4, 128], P(('group', 'batch'), 'expert'), parts along dimension 0, may hold values from -6 to 6
- key_cache: bfloat16 [128, 4, 256, 128], P(('group', 'batch'), 'expert'), parts along dimension 0, may hold values from -6 to 6
- value_cache: bfloat16 [128, 4, 256, 128], P(('group', 'batch'), 'expert'), parts along dimension 0, may hold values from -6 to 6
- cache_len: int32 [128], P(('group', 'batch')), parts along dimension 0, may hold values from 1 to 256, 8192 in all
- new_slot: int32 [128], P(('group', 'batch')), parts along dimension 0, may hold values 0 or 1
- out_weight: bfloat16 [2048, 4096], P('expert'), may hold values from -0.125 to 0.125
- norm_gain: float32 [4096], replicated, may hold values from 0.5 to 1.5
- router: bfloat16 [4096, 4], replicated, may hold values from -0.09375 to 0.09375
- chosen: int32 [128, 2], P(('group', 'batch')), parts along dimension 0, may hold values from 0 to 3, all different within a row; in each aligned block of 16 rows (0 to 15, 16 to 31, ...) at most 12 rows name the same one
- w_gate: bfloat16 [4, 4096, 8192], P('expert', None, 'batch'), may hold values from -0.09375 to 0.09375
- w_up: bfloat16 [4, 4096, 8192], P('expert', None, 'batch'), may hold values from -0.09375 to 0.09375
- w_down: bfloat16 [4, 8192, 4096], P('expert', 'batch'), may hold values from -0.0625 to 0.0625
Outputs:
- layer_out: bfloat16 [128, 4096], P(('group', 'batch', 'expert')), parts along dimension 0
The draws below stay inside these ranges and needn't reach their ends.
There are 2 independent parts, one for each index of `group`. The reference program is written for one: setup_inputs(seed, part) draws one part's arguments, and reference() takes and returns one part's arrays. A program takes and returns all parts, laid end to end along the dimension named above; an argument that names none is the same for every part. Nothing has to cross between parts.
Inputs may be any that keep to these rules, and one draw needn't show every extreme that they name: `chosen`: each row names 2 different experts. Among the rows of one device no expert is named by more than 12 rows, and in every draw some expert is named by exactly 12 rows of some device. `cache_len`: the lengths of a part sum to 8192, and the largest is exactly 256.
All inputs are finite; a program needn't handle non-finite values. No bound on the sum of `cache_len` or of `new_slot` on one device may be relied on, other than what follows from the above.
Results may differ from the reference program's by a relative error of at most 0.017.
Values may be sent and summed in bfloat16 or wider, within the bound.
No kernel may reach another device: no remote copies, remote signals or barrier semaphores. Data moves between devices by JAX's collectives and lax.ppermute only.
A program may use at most 128 MiB of HBM per device.

```python
import math
import jax
import jax.numpy as jnp
import numpy as np
from jax import lax

D = 4096
H = 16
KVH = 4
HD = 128
E = 4
TOP = 2
FF = 8192
SLOT_DEV = 16
CACHE = 256
CAP = 12
SLOTS = 64


def attention_parts(key):
    base = jax.random.fold_in(key, 1234)
    key_query, key_fresh, key_cached = jax.random.split(base, 3)
    queries = jnp.clip(jax.random.normal(key_query, (SLOTS, H, HD), jnp.float32), -6.0, 6.0)
    fresh_keys = jnp.clip(jax.random.normal(key_fresh, (SLOTS, KVH, HD), jnp.float32), -6.0, 6.0)
    cached = jnp.clip(jax.random.normal(key_cached, (SLOTS, KVH, CACHE, HD), jnp.float32), -6.0, 6.0)
    return (jnp.clip(queries, -150.0, 150.0), fresh_keys, cached)


def draw_queries(key, part):
    return attention_parts(key)[0].astype(jnp.bfloat16)


def draw_key_new(key, part):
    return attention_parts(key)[1].astype(jnp.bfloat16)


def draw_key_cache(key, part):
    return attention_parts(key)[2].astype(jnp.bfloat16)


def draw_residual_in(key, part):
    base = jax.random.fold_in(key, 77)
    key_drawn, key_rows, key_columns = jax.random.split(base, 3)
    drawn = jnp.clip(jax.random.normal(key_drawn, (SLOTS, D), jnp.float32), -3.0, 3.0)
    row_scale = jnp.exp(jax.random.uniform(key_rows, (SLOTS, 1), jnp.float32, jnp.log(0.1), jnp.log(1.0)))
    column_scale = jnp.exp(jax.random.uniform(key_columns, (1, D), jnp.float32, jnp.log(0.3), jnp.log(3.0)))
    return (drawn * row_scale * column_scale).astype(jnp.bfloat16)


def set_ends(entries, stream_key, smallest, largest):
    extent = entries.shape
    place = [jax.random.randint(jax.random.fold_in(stream_key, axis), (), 0, extent[axis]) for axis in range(len(extent))]
    entries = entries.at[tuple(place)].set(smallest)
    longest = extent.index(max(extent))
    place[longest] = (place[longest] + 1) % extent[longest]
    return entries.at[tuple(place)].set(largest)


def steps_of(key, extent, cuts, low, high):
    loudness, own = 1.0, jax.random.fold_in(key, 6)
    for axis_at, parts in cuts:
        heights = jnp.exp(jax.random.uniform(jax.random.fold_in(own, axis_at), (parts,), jnp.float32, low / len(cuts), high / len(cuts)))
        loudness = loudness * jnp.repeat(heights, extent[axis_at] // parts).reshape([-1 if axis == axis_at else 1 for axis in range(len(extent))])
    return loudness


def split_up(count, total, bound, lean):
    loads = [(1 << 20) // math.isqrt(standing ** lean) + 1 for standing in range(2, count + 1)]
    rest, holding = total - bound - (count - 1), [1] * (count - 1)
    while rest > 0:
        free = [i for i in range(count - 1) if holding[i] < bound]
        whole, budget = sum([loads[i] for i in free]), rest
        for i in free:
            more = min(bound - holding[i], max(1, budget * loads[i] // whole), rest)
            holding[i] = holding[i] + more
            rest = rest - more
    return np.array([bound] + holding)


def ragged(rng, amount, total, most, skew):
    if amount == 2:
        one = jax.random.randint(rng, (), max(1, total - most), min(most, total - 1) + 1)
        return jnp.stack([one, total - one])
    sizes = jnp.asarray(split_up(amount, total, most, skew), jnp.int32)
    couples = (amount - 1) // 2
    giver, sink = sizes[1:1 + 2 * couples:2], sizes[2:2 + 2 * couples:2]
    margin = jnp.minimum(giver - 1, most - sink)
    moved = jax.random.randint(jax.random.fold_in(rng, 1), (couples,), 0, 1 << 20) % (margin + 1)
    sizes = sizes.at[1:1 + 2 * couples:2].set(giver - moved).at[2:2 + 2 * couples:2].set(sink + moved)
    return sizes[jax.random.permutation(jax.random.fold_in(rng, 2), amount)]


def assign_block(rng, own, number, rows, count, top, most, skew):
    sequence = jax.random.permutation(rng, count)
    heavy_load, usual = shares(count, rows * top, most, skew, True), shares(count, rows * top, most, skew, False)
    places = jnp.arange(count)

    def named(sizes, offset_by):
        used = int((sizes > 0).sum())
        fixed = max(1, used // 4)
        shifted = fixed + (places - fixed + offset_by * (used - fixed)) % max(1, count - fixed)
        return jnp.zeros((count,), jnp.int32).at[sequence[jnp.where(places < fixed, places, shifted)]].set(jnp.asarray(sizes, jnp.int32))

    sizes = jnp.where(number % 4 == 0, named(heavy_load, number // 4), named(usual, number - number // 4 - 1))
    mixed = jax.random.permutation(jax.random.fold_in(own, 3), count)
    source_of, receiver = mixed[0:count // 2 * 2:2], mixed[1:count // 2 * 2:2]
    room = jnp.minimum(sizes[source_of] - 1, most - sizes[receiver]) // 2
    room = jnp.where((source_of == sequence[0]) | (receiver == sequence[0]) | (sizes[receiver] == 0), 0, jnp.maximum(room, 0))
    shifted = jax.random.randint(jax.random.fold_in(own, 4), (count // 2,), 0, 1 << 20) % (room + 1)
    sizes = sizes.at[source_of].add(-shifted).at[receiver].add(shifted)
    members = jnp.searchsorted(jnp.cumsum(sizes), jnp.arange(rows * top), side="right").astype(jnp.int32)
    grid = members.reshape(top, rows).T
    grid = grid[jax.random.permutation(jax.random.fold_in(own, 1), rows)]
    offset_by = jax.random.randint(jax.random.fold_in(own, 2), (rows, 1), 0, top)
    return jnp.take_along_axis(grid, (jnp.arange(top)[None, :] + offset_by) % top, axis=1)


def shares(count, total, most, lean, full):
    loads = [(1 << 20) // math.isqrt(rank ** lean) + 1 for rank in range(1, count + 1)]
    largest = most if full else min(most, max(-(-total // count), total * loads[0] // sum(loads)))
    least = 1 if total - largest >= count - 1 else 0
    counts, rest = [largest] + [least] * (count - 1), total - largest - least * (count - 1)
    while rest > 0:
        free = [i for i in range(1, count) if counts[i] < largest] or [i for i in range(1, count) if counts[i] < most]
        pool, remaining = sum([loads[i] for i in free]), rest
        for i in free:
            more = min(most - counts[i], max(1, remaining * loads[i] // pool), rest)
            counts[i] = counts[i] + more
            rest = rest - more
    return np.array(counts)


def centred(own_key, shape, deviation, bound, cuts=(), dtype=jnp.bfloat16):
    array = jax.random.normal(own_key, shape, jnp.float32) * deviation
    if len(cuts) > 0:
        array = steps_of(own_key, shape, cuts, -0.22, 0.18) * array
    return jnp.clip(array, min=-bound, max=bound).astype(dtype)


def setup_inputs(seed: int = 0, part: int = 0) -> dict:
    keys = jax.random.split(jax.random.key(seed), 16)
    part_keys = jax.random.split(jax.random.fold_in(keys[15], part), 16)
    residual_in = draw_residual_in(jax.random.fold_in(jax.random.fold_in(keys[15], part), 71), part)
    queries = draw_queries(jax.random.fold_in(jax.random.fold_in(keys[15], part), 71), part)
    key_new = draw_key_new(jax.random.fold_in(jax.random.fold_in(keys[15], part), 71), part)
    value_new = centred(part_keys[3], (SLOTS, KVH, HD), 1.0, 6.0, ((0, 4), (1, 4)))
    key_cache = draw_key_cache(jax.random.fold_in(jax.random.fold_in(keys[15], part), 71), part)
    value_cache = centred(part_keys[5], (SLOTS, KVH, CACHE, HD), 1.0, 6.0, ((0, 4), (1, 4)))
    cache_len = ragged(part_keys[6], SLOTS, SLOTS * CACHE // 2, CACHE, 2).astype(jnp.int32)
    new_slot = set_ends((jax.random.randint(part_keys[7], (SLOTS,), 0, 8) < 1).astype(jnp.int32), jax.random.fold_in(part_keys[7], 1), 0, 1)
    out_weight = centred(keys[8], (H * HD, D), (H * HD) ** -0.5, 0.125, ((0, 4),))
    norm_gain = jnp.clip(1.0 + 0.1 * jax.random.normal(keys[9], (D,), jnp.float32), 0.5, 1.5)
    router = centred(keys[10], (D, E), D ** -0.5, 0.09375)
    chosen_keys = jax.random.split(jax.random.fold_in(part_keys[11], 1), SLOTS // SLOT_DEV)
    chosen_turns = jax.random.permutation(jax.random.fold_in(part_keys[11], 3), SLOTS // SLOT_DEV)
    chosen = jax.vmap(lambda own, number: assign_block(jax.random.fold_in(part_keys[11], 2), own, number, SLOT_DEV, E, TOP, CAP, 2))(chosen_keys, chosen_turns).reshape((SLOTS, TOP))
    w_gate = centred(keys[12], (E, D, FF), D ** -0.5, 0.09375, ((0, 4), (2, 4)))
    w_up = centred(keys[13], (E, D, FF), D ** -0.5, 0.09375, ((0, 4), (2, 4)))
    w_down = centred(keys[14], (E, FF, D), FF ** -0.5, 0.0625, ((0, 4), (1, 4)))
    return {"residual_in": residual_in, "queries": queries, "key_new": key_new, "value_new": value_new, "key_cache": key_cache, "value_cache": value_cache, "cache_len": cache_len, "new_slot": new_slot, "out_weight": out_weight, "norm_gain": norm_gain, "router": router, "chosen": chosen, "w_gate": w_gate, "w_up": w_up, "w_down": w_down}


epsilon = 1e-05

def attend(queries, key_new, value_new, key_cache, value_cache, cache_len, new_slot):
    slot_count, head_count, head_width = queries.shape
    kv_count = key_cache.shape[1]
    length = key_cache.shape[2]
    group_size = head_count // kv_count
    grouped = queries.astype(jnp.float32).reshape(slot_count, kv_count, group_size, head_width)
    scaling = float(head_width) ** (-0.5)
    scores = jnp.einsum('skgd,sktd->skgt', grouped, key_cache.astype(jnp.float32)) * scaling
    own_score = jnp.einsum('skgd,skd->skg', grouped, key_new.astype(jnp.float32)) * scaling
    places = lax.broadcasted_iota(jnp.int32, (slot_count, length), 1)
    usable = (places < cache_len[:, None]) & (new_slot[:, None] == 0)
    usable = usable[:, None, None, :]
    scores = jnp.where(usable, scores, jnp.float32(-1e+30))
    highest = jnp.maximum(lax.optimization_barrier(jnp.max(scores, axis=3)), own_score)
    weights = jnp.where(usable, jnp.exp(scores - highest[..., None]), jnp.float32(0.0))
    own_weight = jnp.exp(own_score - highest)
    denominator = lax.optimization_barrier(jnp.sum(weights, axis=3)) + own_weight
    probabilities = (weights / denominator[..., None]).astype(jnp.bfloat16)
    own_prob = (own_weight / denominator).astype(jnp.bfloat16)
    attended = jnp.einsum('skgt,sktd->skgd', probabilities.astype(jnp.float32), value_cache.astype(jnp.float32))
    attended = attended + own_prob.astype(jnp.float32)[..., None] * value_new.astype(jnp.float32)[:, :, None, :]
    return attended.reshape(slot_count, head_count * head_width).astype(jnp.bfloat16)

def mixing(logits, chosen, expert_count):
    labels = lax.broadcasted_iota(jnp.int32, (1, 1, expert_count), 2)
    picking = (chosen[:, :, None] == labels).astype(jnp.float32)
    chosen_logits = lax.optimization_barrier(jnp.sum(picking * logits[:, None, :], axis=2))
    leading = jax.nn.sigmoid(chosen_logits[:, 0] - chosen_logits[:, 1])
    fractions = jnp.stack([leading, 1.0 - leading], axis=1)
    return lax.optimization_barrier(jnp.sum(picking * fractions[:, :, None], axis=1))

def reference(residual_in, queries, key_new, value_new, key_cache, value_cache, cache_len, new_slot, out_weight, norm_gain, router, chosen, w_gate, w_up, w_down):
    attended = attend(queries, key_new, value_new, key_cache, value_cache, cache_len, new_slot)
    projected = jnp.dot(attended, out_weight, preferred_element_type=jnp.float32)
    stream = (residual_in.astype(jnp.float32) + projected).astype(jnp.bfloat16)
    values = stream.astype(jnp.float32)
    scaling = lax.rsqrt(lax.optimization_barrier(jnp.mean(values * values, axis=1, keepdims=True)) + epsilon)
    normed = (values * scaling * norm_gain).astype(jnp.bfloat16)
    logits = jnp.dot(normed, router, preferred_element_type=jnp.float32)
    expert_count = router.shape[1]
    coef = mixing(logits, chosen, expert_count)
    result = values
    for expert in range(expert_count):
        gate_part = jnp.dot(normed, w_gate[expert], preferred_element_type=jnp.float32)
        up_part = jnp.dot(normed, w_up[expert], preferred_element_type=jnp.float32)
        hidden = (jax.nn.silu(gate_part) * up_part).astype(jnp.bfloat16)
        expert_out = jnp.dot(hidden, w_down[expert], preferred_element_type=jnp.float32)
        result = result + coef[:, expert:expert + 1] * expert_out
    return result.astype(jnp.bfloat16)
```

```python
import functools

import jax
import jax.numpy as jnp
from jax import lax
from jax.experimental import pallas as pl
from jax.experimental.pallas import tpu as pltpu
from jax.sharding import PartitionSpec as P

EPSILON = 1e-05
LANES = 128
MIB = 1 << 20

F32 = jnp.float32
BF16 = jnp.bfloat16


def vmem(count=1):
    return [pl.BlockSpec(memory_space=pltpu.VMEM)] * count


def attend_kernel(
    blocks,
    axis,
    len_ref,
    new_ref,
    q_ref,
    kn_ref,
    vn_ref,
    k_hbm,
    v_hbm,
    w_hbm,
    keep_ref,
    send_ref,
    k_ref,
    v_ref,
    w_ref,
    att_ref,
    sems,
):
    slots, heads, width = q_ref.shape
    length = k_ref.shape[2]
    per = slots // blocks
    me = lax.axis_index(axis)
    k_copy = pltpu.make_async_copy(k_hbm, k_ref, sems.at[0])
    v_copy = pltpu.make_async_copy(v_hbm, v_ref, sems.at[1])
    w_copy = pltpu.make_async_copy(w_hbm, w_ref, sems.at[2])
    k_copy.start()
    v_copy.start()
    w_copy.start()
    scaling = float(width) ** (-0.5)
    places = lax.broadcasted_iota(jnp.int32, (heads, length), 1)
    order = []
    for block in list(range(0, blocks, 2)) + list(range(1, blocks, 2)):
        owner = lax.bitwise_xor(me, block)
        order += [owner * per + i for i in range(per)]
    k_copy.wait()
    probs = []
    for slot in order:
        query = q_ref[slot]
        scores = (
            lax.dot_general(
                query, k_ref[slot, 0], (((1,), (1,)), ((), ())), preferred_element_type=F32
            )
            * scaling
        )
        own = (
            jnp.sum(query.astype(F32) * kn_ref[slot].astype(F32), axis=1, keepdims=True) * scaling
        )
        usable = (places < len_ref[slot]) & (new_ref[slot] == 0)
        scores = jnp.where(usable, scores, F32(-1e30))
        highest = jnp.maximum(jnp.max(scores, axis=1, keepdims=True), own)
        weights = jnp.where(usable, jnp.exp(scores - highest), F32(0.0))
        own_weight = jnp.exp(own - highest)
        total = jnp.sum(weights, axis=1, keepdims=True) + own_weight
        probs.append(((weights / total).astype(BF16), (own_weight / total).astype(BF16)))
    v_copy.wait()
    for place, slot in enumerate(order):
        prob, own_prob = probs[place]
        attended = jnp.dot(prob, v_ref[slot, 0], preferred_element_type=F32)
        attended = attended + own_prob.astype(F32) * vn_ref[slot].astype(F32)
        att_ref[pl.ds(place * 8, heads), :] = attended
    rows = jnp.concatenate(
        [att_ref[pl.ds(head, slots, stride=8), :] for head in range(heads)], axis=1
    ).astype(BF16)
    w_copy.wait()
    half = slots // 2
    columns = w_ref.shape[1]
    step = min(columns, 1024)
    for start in range(0, columns, step):
        part = jnp.dot(rows, w_ref[:, start : start + step], preferred_element_type=F32)
        keep_ref[:, start : start + step] = part[:half]
        send_ref[:, start : start + step] = part[half:].astype(send_ref.dtype)


def attend(blocks, axis, queries, key_new, value_new, key_cache, value_cache, lens, new, out_weight):
    slots, heads, width = queries.shape
    columns = out_weight.shape[1]
    half = slots // 2
    return pl.pallas_call(
        functools.partial(attend_kernel, blocks, axis),
        out_shape=(
            jax.ShapeDtypeStruct((half, columns), F32),
            jax.ShapeDtypeStruct((half, columns), F32),
        ),
        in_specs=[pl.BlockSpec(memory_space=pltpu.SMEM)] * 2
        + vmem(3)
        + [pl.BlockSpec(memory_space=pl.ANY)] * 3,
        out_specs=tuple(vmem(2)),
        scratch_shapes=[
            pltpu.VMEM(key_cache.shape, BF16),
            pltpu.VMEM(value_cache.shape, BF16),
            pltpu.VMEM(out_weight.shape, BF16),
            pltpu.VMEM((slots * 8, width), F32),
            pltpu.SemaphoreType.DMA((3,)),
        ],
        compiler_params=pltpu.CompilerParams(vmem_limit_bytes=9 * MIB),
        name="attend",
    )(lens, new, queries, key_new, value_new, key_cache, value_cache, out_weight)


def fold_kernel(keep_ref, got_ref, mine_ref, send_ref):
    total = keep_ref[...] + got_ref[...].astype(F32)
    mine_ref[...] = total
    half = total.shape[0] // 2
    send_ref[0:half, :] = total[half:].astype(send_ref.dtype)
    send_ref[half:, :] = total[:half].astype(send_ref.dtype)


def fold(keep, got):
    return pl.pallas_call(
        fold_kernel,
        out_shape=(
            jax.ShapeDtypeStruct(keep.shape, F32),
            jax.ShapeDtypeStruct(keep.shape, BF16),
        ),
        in_specs=vmem(2),
        out_specs=tuple(vmem(2)),
        compiler_params=pltpu.CompilerParams(vmem_limit_bytes=2 * MIB),
        name="fold",
    )(keep, got)


def norm_kernel(
    axis, mine_ref, got_ref, res_ref, gain_ref, router_ref, chosen_ref, stream_ref, packet_ref
):
    me = lax.axis_index(axis)
    low = lax.rem(me, 2) == 0
    upper = me < 2
    rows = mine_ref.shape[0]
    per = rows // 2
    model = mine_ref.shape[1]
    experts = router_ref.shape[1]

    def owned(values):
        def pick(part):
            return jnp.where(low, part[:per], part[per:])

        first, second = pick(values[:rows]), pick(values[rows:])
        return jnp.concatenate(
            [jnp.where(upper, first, second), jnp.where(upper, second, first)], axis=0
        )

    residual = owned(res_ref[...].astype(F32))
    stream = (residual + mine_ref[...] + got_ref[...].astype(F32)).astype(BF16)
    stream_ref[...] = stream[:per]
    values = stream.astype(F32)
    scaling = lax.rsqrt(jnp.mean(values * values, axis=1, keepdims=True) + EPSILON)
    normed = (values * scaling * gain_ref[...]).astype(BF16)
    packet_ref[:, :model] = normed
    logits = jnp.dot(normed, router_ref[...], preferred_element_type=F32)
    chosen = owned(chosen_ref[...])
    first, second = chosen[:, 0:1], chosen[:, 1:2]
    labels = lax.broadcasted_iota(jnp.int32, logits.shape, 1)
    first_logit = jnp.sum(jnp.where(labels == first, logits, 0.0), axis=1, keepdims=True)
    second_logit = jnp.sum(jnp.where(labels == second, logits, 0.0), axis=1, keepdims=True)
    leading = 1.0 / (1.0 + jnp.exp(second_logit - first_logit))
    lanes = lax.broadcasted_iota(jnp.int32, (rows, LANES), 1)
    expert = lax.rem(lanes, experts)
    coef = jnp.where(
        expert == first, leading, jnp.where(expert == second, 1.0 - leading, F32(0.0))
    )
    high = coef.astype(BF16).astype(F32)
    packet_ref[:, model:] = jnp.where(lanes < experts, high, coef - high).astype(BF16)


def norm(axis, mine, got, residual, gain, router, chosen):
    rows, model = mine.shape
    return pl.pallas_call(
        functools.partial(norm_kernel, axis),
        out_shape=(
            jax.ShapeDtypeStruct((rows // 2, model), BF16),
            jax.ShapeDtypeStruct((rows, model + LANES), BF16),
        ),
        in_specs=vmem(6),
        out_specs=tuple(vmem(2)),
        compiler_params=pltpu.CompilerParams(vmem_limit_bytes=4 * MIB),
        name="norm",
    )(mine, got, residual, gain.reshape(1, model), router, chosen)


def join_kernel(a_ref, b_ref, out_ref):
    rows = a_ref.shape[0]
    out_ref[0:rows, :] = a_ref[...]
    out_ref[rows:, :] = b_ref[...]


def join(a, b):
    return pl.pallas_call(
        join_kernel,
        out_shape=jax.ShapeDtypeStruct((2 * a.shape[0], a.shape[1]), a.dtype),
        in_specs=vmem(2),
        out_specs=vmem(1)[0],
        compiler_params=pltpu.CompilerParams(vmem_limit_bytes=2 * MIB),
        name="join",
    )(a, b)


def expert_kernel(
    axis, experts, parts, *refs
):
    packets = refs[:parts]
    gate_hbm, up_hbm, down_hbm, keep_ref, send_ref = refs[parts : parts + 5]
    gate_ref, up_ref, down_ref, x_ref, hidden_ref, sems = refs[parts + 5 :]
    me = lax.axis_index(axis)
    model, hidden = gate_ref.shape
    chunk = min(hidden, 512)
    count = hidden // chunk
    down_chunk = min(model, 1024)
    copies = []
    for j in range(count):
        cols = pl.ds(j * chunk, chunk)
        a = pltpu.make_async_copy(gate_hbm.at[0, :, cols], gate_ref.at[:, cols], sems.at[0, j])
        b = pltpu.make_async_copy(up_hbm.at[0, :, cols], up_ref.at[:, cols], sems.at[1, j])
        a.start()
        b.start()
        copies.append((a, b))
    down_copies = []
    for j in range(model // down_chunk):
        cols = pl.ds(j * down_chunk, down_chunk)
        c = pltpu.make_async_copy(down_hbm.at[0, :, cols], down_ref.at[:, cols], sems.at[2, j])
        c.start()
        down_copies.append(c)
    rows = packets[0].shape[0]
    coefs = []
    for i, packet in enumerate(packets):
        x_ref[i * rows : (i + 1) * rows, :] = packet[:, :model]
        tail = packet[:, model:].astype(F32)
        lanes = lax.broadcasted_iota(jnp.int32, tail.shape, 1)
        mine = (lanes == me) | (lanes == me + experts)
        coefs.append(jnp.sum(jnp.where(mine, tail, 0.0), axis=1, keepdims=True))
    coef = jnp.concatenate(coefs, axis=0)
    for j in range(count):
        cols = slice(j * chunk, (j + 1) * chunk)
        for copy in copies[j]:
            copy.wait()
        gate = jnp.dot(x_ref[...], gate_ref[:, cols], preferred_element_type=F32)
        up = jnp.dot(x_ref[...], up_ref[:, cols], preferred_element_type=F32)
        hidden_ref[:, cols] = (gate / (1.0 + jnp.exp(-gate)) * up).astype(BF16)
    half = x_ref.shape[0] // 2
    for j in range(model // down_chunk):
        cols = slice(j * down_chunk, (j + 1) * down_chunk)
        down_copies[j].wait()
        out = jnp.dot(hidden_ref[...], down_ref[:, cols], preferred_element_type=F32) * coef
        keep_ref[:, cols] = out[:half]
        send_ref[:, cols] = out[half:].astype(BF16)


def expert_ffn(axis, experts, packets, w_gate, w_up, w_down):
    parts = len(packets)
    rows = parts * packets[0].shape[0]
    model, hidden = w_gate.shape[1:]
    half = rows // 2
    limit = (3 * model * hidden * 2) + rows * model * 12 + 4 * MIB
    return pl.pallas_call(
        functools.partial(expert_kernel, axis, experts, parts),
        out_shape=(
            jax.ShapeDtypeStruct((half, model), F32),
            jax.ShapeDtypeStruct((half, model), BF16),
        ),
        in_specs=vmem(parts) + [pl.BlockSpec(memory_space=pltpu.HBM)] * 3,
        out_specs=tuple(vmem(2)),
        scratch_shapes=[
            pltpu.VMEM((model, hidden), BF16),
            pltpu.VMEM((model, hidden), BF16),
            pltpu.VMEM((hidden, model), BF16),
            pltpu.VMEM((rows, model), BF16),
            pltpu.VMEM((rows, hidden), BF16),
            pltpu.SemaphoreType.DMA((3, 8)),
        ],
        compiler_params=pltpu.CompilerParams(vmem_limit_bytes=limit),
        name="experts",
    )(*packets, w_gate, w_up, w_down)


def halve_kernel(keep_ref, got_ref, mine_ref, send_ref):
    half = keep_ref.shape[0] // 2
    total = keep_ref[...] + got_ref[...].astype(F32)
    mine_ref[...] = total[:half]
    send_ref[...] = total[half:].astype(BF16)


def halve(keep, got):
    rows, model = keep.shape
    return pl.pallas_call(
        halve_kernel,
        out_shape=(
            jax.ShapeDtypeStruct((rows // 2, model), F32),
            jax.ShapeDtypeStruct((rows // 2, model), BF16),
        ),
        in_specs=vmem(2),
        out_specs=tuple(vmem(2)),
        compiler_params=pltpu.CompilerParams(vmem_limit_bytes=rows * model * 12 + 2 * MIB),
        name="halve",
    )(keep, got)


def last_kernel(keep_ref, got_ref, stream_ref, out_ref):
    total = keep_ref[...] + got_ref[...].astype(F32) + stream_ref[...].astype(F32)
    out_ref[...] = total.astype(BF16)


def last(keep, got, stream):
    return pl.pallas_call(
        last_kernel,
        out_shape=jax.ShapeDtypeStruct(stream.shape, BF16),
        in_specs=vmem(3),
        out_specs=vmem(1)[0],
        compiler_params=pltpu.CompilerParams(vmem_limit_bytes=2 * MIB),
        name="last",
    )(keep, got, stream)


def body(
    experts,
    batches,
    residual_in,
    queries,
    key_new,
    value_new,
    key_cache,
    value_cache,
    cache_len,
    new_slot,
    out_weight,
    norm_gain,
    router,
    chosen,
    w_gate,
    w_up,
    w_down,
):
    def swap(x, axis, size, bit):
        return lax.ppermute(x, axis, [(i, i ^ bit) for i in range(size)])

    batch_bits = []
    bit = 1
    while bit < batches:
        batch_bits.append(bit)
        bit *= 2

    keep, send = attend(
        experts, "expert", queries, key_new, value_new, key_cache, value_cache, cache_len, new_slot,
        out_weight,
    )
    mine, send = fold(keep, swap(send, "expert", experts, 1))
    got = swap(send, "expert", experts, 2)
    stream, packet = norm("expert", mine, got, residual_in, norm_gain, router, chosen)
    for bit in batch_bits[:0:-1]:
        packet = join(packet, swap(packet, "batch", batches, bit))
    near = [packet] + [swap(packet, "batch", batches, bit) for bit in batch_bits[:1]]
    packets = near + [swap(p, "expert", experts, 1) for p in near]
    keep, send = expert_ffn("expert", experts, packets, w_gate, w_up, w_down)
    got = swap(send, "expert", experts, 1)
    for bit in batch_bits:
        keep, send = halve(keep, got)
        got = swap(send, "batch", batches, bit)
    keep, send = halve(keep, got)
    got = swap(send, "expert", experts, 2)
    return last(keep, got, stream)


def solution(mesh):
    rows = P(("group", "batch"), None)
    heads = P(("group", "batch"), "expert", None)
    cache = P(("group", "batch"), "expert", None, None)
    slot = P(("group", "batch"))
    in_specs = (
        rows,
        heads,
        heads,
        heads,
        cache,
        cache,
        slot,
        slot,
        P("expert", None),
        P(),
        P(),
        rows,
        P("expert", None, "batch"),
        P("expert", None, "batch"),
        P("expert", "batch", None),
    )
    out_specs = P(("group", "batch", "expert"), None)
    inner = functools.partial(body, mesh.shape["expert"], mesh.shape["batch"])
    return jax.shard_map(inner, mesh=mesh, in_specs=in_specs, out_specs=out_specs, check_vma=False)
```

```python
import functools

import jax
import jax.numpy as jnp
from jax import lax
from jax.experimental import pallas as pl
from jax.experimental.pallas import tpu as pltpu
from jax.sharding import PartitionSpec as P

EPSILON = 1e-05
LANES = 128
MIB = 1 << 20

F32 = jnp.float32
BF16 = jnp.bfloat16


def vmem(count=1):
    return [pl.BlockSpec(memory_space=pltpu.VMEM)] * count


def pinned(x):
    return pltpu.with_memory_space_constraint(x, pltpu.HBM)


def attend_kernel(blocks, axis, *refs):
    sources, outs, rest = refs[:11], refs[11:16], refs[16:]
    keep_ref, send_ref, base_ref, gain_ref, pick_ref = outs
    (
        k_ref,
        v_ref,
        w_ref,
        q_ref,
        kn_ref,
        vn_ref,
        len_ref,
        new_ref,
        chosen_ref,
        res_ref,
        own_key_ref,
        own_value_ref,
        att_ref,
        sems,
    ) = rest
    slots, heads, width = q_ref.shape
    length = k_ref.shape[2]
    per = slots // blocks
    half = slots // 2
    me = lax.axis_index(axis)
    targets = (len_ref, new_ref, q_ref, kn_ref, k_ref, vn_ref, v_ref, w_ref, chosen_ref, res_ref)
    targets += (gain_ref,)
    copies = []
    for i, (source, target) in enumerate(zip(sources, targets)):
        copies.append(pltpu.make_async_copy(source, target, sems.at[i]))
        copies[-1].start()
    scaling = float(width) ** (-0.5)
    places = lax.broadcasted_iota(jnp.int32, (heads, length), 1)
    order = []
    for block in list(range(0, blocks, 2)) + list(range(1, blocks, 2)):
        owner = lax.bitwise_xor(me, block)
        order += [owner * per + i for i in range(per)]
    for copy in copies[:4]:
        copy.wait()
    own_key_ref[...] = kn_ref[...].astype(F32)
    copies[4].wait()
    probs = []
    for slot in order:
        query = q_ref[slot]
        scores = (
            lax.dot_general(
                query, k_ref[slot, 0], (((1,), (1,)), ((), ())), preferred_element_type=F32
            )
            * scaling
        )
        own = (
            jnp.sum(query.astype(F32) * own_key_ref[pl.ds(slot, 1), :], axis=1, keepdims=True)
            * scaling
        )
        usable = (places < len_ref[slot]) & (new_ref[slot] == 0)
        scores = jnp.where(usable, scores, F32(-1e30))
        highest = jnp.maximum(jnp.max(scores, axis=1, keepdims=True), own)
        weights = jnp.where(usable, jnp.exp(scores - highest), F32(0.0))
        own_weight = jnp.exp(own - highest)
        total = jnp.sum(weights, axis=1, keepdims=True) + own_weight
        probs.append(((weights / total).astype(BF16), (own_weight / total).astype(BF16)))
    copies[5].wait()
    own_value_ref[...] = vn_ref[...].astype(F32)
    copies[6].wait()
    for place, slot in enumerate(order):
        prob, own_prob = probs[place]
        attended = jnp.dot(prob, v_ref[slot, 0], preferred_element_type=F32)
        attended = attended + own_prob.astype(F32) * own_value_ref[pl.ds(slot, 1), :]
        att_ref[pl.ds(place * 8, heads), :] = attended
    rows = jnp.concatenate(
        [att_ref[pl.ds(head, slots, stride=8), :] for head in range(heads)], axis=1
    ).astype(BF16)
    copies[7].wait()
    columns = w_ref.shape[1]
    step = min(columns, 1024)
    for start in range(0, columns, step):
        part = jnp.dot(rows, w_ref[:, start : start + step], preferred_element_type=F32)
        keep_ref[:, start : start + step] = part[:half]
        send_ref[:, start : start + step] = part[half:].astype(send_ref.dtype)
    for copy in copies[8:]:
        copy.wait()
    lines = lax.broadcasted_iota(jnp.int32, (half, LANES), 0)
    lanes = lax.broadcasted_iota(jnp.int32, (half, LANES), 1)
    picks = jnp.zeros((half, LANES), jnp.int32)
    for place, slot in enumerate(order[:half]):
        named = jnp.where(lanes == 0, chosen_ref[0, slot], chosen_ref[1, slot])
        picks = jnp.where(lines == place, named, picks)
    pick_ref[...] = picks
    residual = res_ref[...].astype(F32)
    kept = []
    for block in range(0, blocks, 2):
        owner = lax.bitwise_xor(me, block)
        value = residual[:per]
        for other in range(1, blocks):
            value = jnp.where(owner == other, residual[other * per : (other + 1) * per], value)
        kept.append(value)
    base_ref[...] = jnp.concatenate(kept, axis=0)


def attend(
    blocks, axis, queries, key_new, value_new, key_cache, value_cache, lens, new, out_weight,
    residual, gain, chosen,
):
    slots, heads, width = queries.shape
    columns = out_weight.shape[1]
    half = slots // 2
    sources = (
        lens,
        new,
        queries,
        key_new.reshape(slots, width),
        key_cache,
        value_new.reshape(slots, width),
        value_cache,
        out_weight,
        chosen.T,
        residual,
        gain.reshape(1, columns),
    )
    return pl.pallas_call(
        functools.partial(attend_kernel, blocks, axis),
        out_shape=(
            jax.ShapeDtypeStruct((half, columns), F32),
            jax.ShapeDtypeStruct((half, columns), F32),
            jax.ShapeDtypeStruct((half, columns), F32),
            jax.ShapeDtypeStruct((1, columns), F32),
            jax.ShapeDtypeStruct((half, LANES), jnp.int32),
        ),
        in_specs=[pl.BlockSpec(memory_space=pltpu.HBM)] * len(sources),
        out_specs=tuple(vmem(5)),
        scratch_shapes=[
            pltpu.VMEM(key_cache.shape, BF16),
            pltpu.VMEM(value_cache.shape, BF16),
            pltpu.VMEM(out_weight.shape, BF16),
            pltpu.VMEM(queries.shape, BF16),
            pltpu.VMEM((slots, width), BF16),
            pltpu.VMEM((slots, width), BF16),
            pltpu.SMEM(lens.shape, jnp.int32),
            pltpu.SMEM(new.shape, jnp.int32),
            pltpu.SMEM((chosen.shape[1], slots), jnp.int32),
            pltpu.VMEM(residual.shape, BF16),
            pltpu.VMEM((slots, width), F32),
            pltpu.VMEM((slots, width), F32),
            pltpu.VMEM((slots * 8, width), F32),
            pltpu.SemaphoreType.DMA((len(sources),)),
        ],
        compiler_params=pltpu.CompilerParams(vmem_limit_bytes=9 * MIB),
        name="attend",
    )(*[pinned(x) for x in sources])


def fold_kernel(keep_ref, got_ref, mine_ref, send_ref):
    total = keep_ref[...] + got_ref[...].astype(F32)
    mine_ref[...] = total
    half = total.shape[0] // 2
    send_ref[0:half, :] = total[half:].astype(send_ref.dtype)
    send_ref[half:, :] = total[:half].astype(send_ref.dtype)


def fold(keep, got):
    return pl.pallas_call(
        fold_kernel,
        out_shape=(
            jax.ShapeDtypeStruct(keep.shape, F32),
            jax.ShapeDtypeStruct(keep.shape, BF16),
        ),
        in_specs=vmem(2),
        out_specs=tuple(vmem(2)),
        compiler_params=pltpu.CompilerParams(vmem_limit_bytes=2 * MIB),
        name="fold",
    )(keep, got)


def norm_kernel(mine_ref, got_ref, base_ref, gain_ref, router_ref, pick_ref, stream_ref, packet_ref):
    rows, model = mine_ref.shape
    per = rows // 2
    experts = router_ref.shape[0]
    total = base_ref[...] + (mine_ref[...] + got_ref[...].astype(F32))
    stream = total.astype(BF16)
    stream_ref[...] = stream[:per]
    values = stream.astype(F32)
    scaling = lax.rsqrt(jnp.mean(values * values, axis=1, keepdims=True) + EPSILON)
    normed = (values * scaling * gain_ref[...]).astype(BF16)
    packet_ref[:, :model] = normed
    logits = lax.dot_general(
        normed, router_ref[...], (((1,), (1,)), ((), ())), preferred_element_type=F32
    )
    first, second = pick_ref[:, 0:1], pick_ref[:, 1:2]
    labels = lax.broadcasted_iota(jnp.int32, logits.shape, 1)
    first_logit = jnp.sum(jnp.where(labels == first, logits, 0.0), axis=1, keepdims=True)
    second_logit = jnp.sum(jnp.where(labels == second, logits, 0.0), axis=1, keepdims=True)
    leading = 1.0 / (1.0 + jnp.exp(second_logit - first_logit))
    lanes = lax.broadcasted_iota(jnp.int32, (rows, LANES), 1)
    expert = lax.rem(lanes, experts)
    coef = jnp.where(
        expert == first, leading, jnp.where(expert == second, 1.0 - leading, F32(0.0))
    )
    high = coef.astype(BF16).astype(F32)
    packet_ref[:, model:] = jnp.where(lanes < experts, high, coef - high).astype(BF16)


def norm(mine, got, base, gain, router, pick):
    rows, model = mine.shape
    return pl.pallas_call(
        norm_kernel,
        out_shape=(
            jax.ShapeDtypeStruct((rows // 2, model), BF16),
            jax.ShapeDtypeStruct((rows, model + LANES), BF16),
        ),
        in_specs=vmem(6),
        out_specs=tuple(vmem(2)),
        compiler_params=pltpu.CompilerParams(vmem_limit_bytes=2 * MIB),
        name="norm",
    )(mine, got, base, gain, router.T, pick)


def join_kernel(a_ref, b_ref, out_ref):
    rows = a_ref.shape[0]
    out_ref[0:rows, :] = a_ref[...]
    out_ref[rows:, :] = b_ref[...]


def join(a, b):
    return pl.pallas_call(
        join_kernel,
        out_shape=jax.ShapeDtypeStruct((2 * a.shape[0], a.shape[1]), a.dtype),
        in_specs=vmem(2),
        out_specs=vmem(1)[0],
        compiler_params=pltpu.CompilerParams(vmem_limit_bytes=2 * MIB),
        name="join",
    )(a, b)


def expert_kernel(
    axis, experts, parts, *refs
):
    packets = refs[:parts]
    gate_hbm, up_hbm, down_hbm, keep_ref, send_ref = refs[parts : parts + 5]
    gate_ref, up_ref, down_ref, x_ref, hidden_ref, sems = refs[parts + 5 :]
    me = lax.axis_index(axis)
    model, hidden = gate_ref.shape
    chunk = min(hidden, 512)
    count = hidden // chunk
    down_chunk = min(model, 1024)
    copies = []
    for j in range(count):
        cols = pl.ds(j * chunk, chunk)
        a = pltpu.make_async_copy(gate_hbm.at[0, :, cols], gate_ref.at[:, cols], sems.at[0, j])
        b = pltpu.make_async_copy(up_hbm.at[0, :, cols], up_ref.at[:, cols], sems.at[1, j])
        a.start()
        b.start()
        copies.append((a, b))
    down_copies = []
    for j in range(model // down_chunk):
        cols = pl.ds(j * down_chunk, down_chunk)
        c = pltpu.make_async_copy(down_hbm.at[0, :, cols], down_ref.at[:, cols], sems.at[2, j])
        c.start()
        down_copies.append(c)
    rows = packets[0].shape[0]
    coefs = []
    for i, packet in enumerate(packets):
        x_ref[i * rows : (i + 1) * rows, :] = packet[:, :model]
        tail = packet[:, model:].astype(F32)
        lanes = lax.broadcasted_iota(jnp.int32, tail.shape, 1)
        mine = (lanes == me) | (lanes == me + experts)
        coefs.append(jnp.sum(jnp.where(mine, tail, 0.0), axis=1, keepdims=True))
    coef = jnp.concatenate(coefs, axis=0)
    for j in range(count):
        cols = slice(j * chunk, (j + 1) * chunk)
        for copy in copies[j]:
            copy.wait()
        gate = jnp.dot(x_ref[...], gate_ref[:, cols], preferred_element_type=F32)
        up = jnp.dot(x_ref[...], up_ref[:, cols], preferred_element_type=F32)
        hidden_ref[:, cols] = (gate / (1.0 + jnp.exp(-gate)) * up).astype(BF16)
    half = x_ref.shape[0] // 2
    for j in range(model // down_chunk):
        cols = slice(j * down_chunk, (j + 1) * down_chunk)
        down_copies[j].wait()
        out = jnp.dot(hidden_ref[...], down_ref[:, cols], preferred_element_type=F32) * coef
        keep_ref[:, cols] = out[:half]
        send_ref[:, cols] = out[half:].astype(BF16)


def expert_ffn(axis, experts, packets, w_gate, w_up, w_down):
    parts = len(packets)
    rows = parts * packets[0].shape[0]
    model, hidden = w_gate.shape[1:]
    half = rows // 2
    limit = (3 * model * hidden * 2) + rows * model * 12 + 4 * MIB
    return pl.pallas_call(
        functools.partial(expert_kernel, axis, experts, parts),
        out_shape=(
            jax.ShapeDtypeStruct((half, model), F32),
            jax.ShapeDtypeStruct((half, model), BF16),
        ),
        in_specs=vmem(parts) + [pl.BlockSpec(memory_space=pltpu.HBM)] * 3,
        out_specs=tuple(vmem(2)),
        scratch_shapes=[
            pltpu.VMEM((model, hidden), BF16),
            pltpu.VMEM((model, hidden), BF16),
            pltpu.VMEM((hidden, model), BF16),
            pltpu.VMEM((rows, model), BF16),
            pltpu.VMEM((rows, hidden), BF16),
            pltpu.SemaphoreType.DMA((3, 8)),
        ],
        compiler_params=pltpu.CompilerParams(vmem_limit_bytes=limit),
        name="experts",
    )(*packets, w_gate, w_up, w_down)


def halve_kernel(keep_ref, got_ref, mine_ref, send_ref):
    half = keep_ref.shape[0] // 2
    total = keep_ref[...] + got_ref[...].astype(F32)
    mine_ref[...] = total[:half]
    send_ref[...] = total[half:].astype(BF16)


def halve(keep, got):
    rows, model = keep.shape
    return pl.pallas_call(
        halve_kernel,
        out_shape=(
            jax.ShapeDtypeStruct((rows // 2, model), F32),
            jax.ShapeDtypeStruct((rows // 2, model), BF16),
        ),
        in_specs=vmem(2),
        out_specs=tuple(vmem(2)),
        compiler_params=pltpu.CompilerParams(vmem_limit_bytes=rows * model * 12 + 2 * MIB),
        name="halve",
    )(keep, got)


def last_kernel(keep_ref, got_ref, stream_ref, out_ref):
    total = keep_ref[...] + got_ref[...].astype(F32) + stream_ref[...].astype(F32)
    out_ref[...] = total.astype(BF16)


def last(keep, got, stream):
    return pl.pallas_call(
        last_kernel,
        out_shape=jax.ShapeDtypeStruct(stream.shape, BF16),
        in_specs=vmem(3),
        out_specs=vmem(1)[0],
        compiler_params=pltpu.CompilerParams(vmem_limit_bytes=2 * MIB),
        name="last",
    )(keep, got, stream)


def body(
    experts,
    batches,
    residual_in,
    queries,
    key_new,
    value_new,
    key_cache,
    value_cache,
    cache_len,
    new_slot,
    out_weight,
    norm_gain,
    router,
    chosen,
    w_gate,
    w_up,
    w_down,
):
    def swap(x, axis, size, bit):
        return lax.ppermute(x, axis, [(i, i ^ bit) for i in range(size)])

    batch_bits = []
    bit = 1
    while bit < batches:
        batch_bits.append(bit)
        bit *= 2

    keep, send, base, gain, pick = attend(
        experts, "expert", queries, key_new, value_new, key_cache, value_cache, cache_len, new_slot,
        out_weight, residual_in, norm_gain, chosen,
    )
    mine, send = fold(keep, swap(send, "expert", experts, 1))
    got = swap(send, "expert", experts, 2)
    stream, packet = norm(mine, got, base, gain, router, pick)
    for bit in batch_bits[:0:-1]:
        packet = join(packet, swap(packet, "batch", batches, bit))
    near = [packet] + [swap(packet, "batch", batches, bit) for bit in batch_bits[:1]]
    packets = near + [swap(p, "expert", experts, 1) for p in near]
    keep, send = expert_ffn("expert", experts, packets, w_gate, w_up, w_down)
    got = swap(send, "expert", experts, 1)
    for bit in batch_bits:
        keep, send = halve(keep, got)
        got = swap(send, "batch", batches, bit)
    keep, send = halve(keep, got)
    got = swap(send, "expert", experts, 2)
    return last(keep, got, stream)


def solution(mesh):
    rows = P(("group", "batch"), None)
    heads = P(("group", "batch"), "expert", None)
    cache = P(("group", "batch"), "expert", None, None)
    slot = P(("group", "batch"))
    in_specs = (
        rows,
        heads,
        heads,
        heads,
        cache,
        cache,
        slot,
        slot,
        P("expert", None),
        P(),
        P(),
        rows,
        P("expert", None, "batch"),
        P("expert", None, "batch"),
        P("expert", "batch", None),
    )
    out_specs = P(("group", "batch", "expert"), None)
    inner = functools.partial(body, mesh.shape["expert"], mesh.shape["batch"])
    return jax.shard_map(inner, mesh=mesh, in_specs=in_specs, out_specs=out_specs, check_vma=False)
```

```python
import functools

import jax
import jax.numpy as jnp
from jax import lax
from jax.experimental import pallas as pl
from jax.experimental.pallas import tpu as pltpu
from jax.sharding import PartitionSpec as P

EPSILON = 1e-05
LANES = 128
MIB = 1 << 20
SLOTS = 4

F32 = jnp.float32
BF16 = jnp.bfloat16


def vmem(count=1):
    return [pl.BlockSpec(memory_space=pltpu.VMEM)] * count


def pinned(x):
    return pltpu.with_memory_space_constraint(x, pltpu.HBM)


def attend_kernel(blocks, axis, *refs):
    sources, outs, rest = refs[:11], refs[11:16], refs[16:]
    keep_ref, send_ref, base_ref, gain_ref, pick_ref = outs
    (
        k_ref,
        v_ref,
        w_ref,
        q_ref,
        kn_ref,
        vn_ref,
        len_ref,
        new_ref,
        chosen_ref,
        res_ref,
        own_key_ref,
        own_value_ref,
        att_ref,
        sems,
    ) = rest
    slots, heads, width = q_ref.shape
    length = k_ref.shape[2]
    per = slots // blocks
    half = slots // 2
    me = lax.axis_index(axis)
    targets = (len_ref, new_ref, q_ref, kn_ref, k_ref, vn_ref, v_ref, w_ref, chosen_ref, res_ref)
    targets += (gain_ref,)
    copies = []
    for i, (source, target) in enumerate(zip(sources, targets)):
        copies.append(pltpu.make_async_copy(source, target, sems.at[i]))
        copies[-1].start()
    scaling = float(width) ** (-0.5)
    places = lax.broadcasted_iota(jnp.int32, (heads, length), 1)
    order = []
    for block in list(range(0, blocks, 2)) + list(range(1, blocks, 2)):
        owner = lax.bitwise_xor(me, block)
        order += [owner * per + i for i in range(per)]
    for copy in copies[:4]:
        copy.wait()
    own_key_ref[...] = kn_ref[...].astype(F32)
    copies[4].wait()
    probs = []
    for slot in order:
        query = q_ref[slot]
        scores = (
            lax.dot_general(
                query, k_ref[slot, 0], (((1,), (1,)), ((), ())), preferred_element_type=F32
            )
            * scaling
        )
        own = (
            jnp.sum(query.astype(F32) * own_key_ref[pl.ds(slot, 1), :], axis=1, keepdims=True)
            * scaling
        )
        usable = (places < len_ref[slot]) & (new_ref[slot] == 0)
        scores = jnp.where(usable, scores, F32(-1e30))
        highest = jnp.maximum(jnp.max(scores, axis=1, keepdims=True), own)
        weights = jnp.where(usable, jnp.exp(scores - highest), F32(0.0))
        own_weight = jnp.exp(own - highest)
        total = jnp.sum(weights, axis=1, keepdims=True) + own_weight
        probs.append(((weights / total).astype(BF16), (own_weight / total).astype(BF16)))
    copies[5].wait()
    own_value_ref[...] = vn_ref[...].astype(F32)
    copies[6].wait()
    for place, slot in enumerate(order):
        prob, own_prob = probs[place]
        attended = jnp.dot(prob, v_ref[slot, 0], preferred_element_type=F32)
        attended = attended + own_prob.astype(F32) * own_value_ref[pl.ds(slot, 1), :]
        att_ref[pl.ds(place * 8, heads), :] = attended
    rows = jnp.concatenate(
        [att_ref[pl.ds(head, slots, stride=8), :] for head in range(heads)], axis=1
    ).astype(BF16)
    copies[7].wait()
    columns = w_ref.shape[1]
    step = min(columns, 1024)
    for start in range(0, columns, step):
        part = jnp.dot(rows, w_ref[:, start : start + step], preferred_element_type=F32)
        keep_ref[:, start : start + step] = part[:half]
        send_ref[:, start : start + step] = part[half:].astype(send_ref.dtype)
    for copy in copies[8:]:
        copy.wait()
    lines = lax.broadcasted_iota(jnp.int32, (half, LANES), 0)
    lanes = lax.broadcasted_iota(jnp.int32, (half, LANES), 1)
    picks = jnp.zeros((half, LANES), jnp.int32)
    for place, slot in enumerate(order[:half]):
        named = jnp.where(lanes == 0, chosen_ref[0, slot], chosen_ref[1, slot])
        picks = jnp.where(lines == place, named, picks)
    pick_ref[...] = picks
    residual = res_ref[...].astype(F32)
    kept = []
    for block in range(0, blocks, 2):
        owner = lax.bitwise_xor(me, block)
        value = residual[:per]
        for other in range(1, blocks):
            value = jnp.where(owner == other, residual[other * per : (other + 1) * per], value)
        kept.append(value)
    base_ref[...] = jnp.concatenate(kept, axis=0)


def attend(
    blocks, axis, queries, key_new, value_new, key_cache, value_cache, lens, new, out_weight,
    residual, gain, chosen,
):
    slots, heads, width = queries.shape
    columns = out_weight.shape[1]
    half = slots // 2
    sources = (
        lens,
        new,
        queries,
        key_new.reshape(slots, width),
        key_cache,
        value_new.reshape(slots, width),
        value_cache,
        out_weight,
        chosen.T,
        residual,
        gain.reshape(1, columns),
    )
    return pl.pallas_call(
        functools.partial(attend_kernel, blocks, axis),
        out_shape=(
            jax.ShapeDtypeStruct((half, columns), F32),
            jax.ShapeDtypeStruct((half, columns), F32),
            jax.ShapeDtypeStruct((half, columns), F32),
            jax.ShapeDtypeStruct((1, columns), F32),
            jax.ShapeDtypeStruct((half, LANES), jnp.int32),
        ),
        in_specs=[pl.BlockSpec(memory_space=pltpu.HBM)] * len(sources),
        out_specs=tuple(vmem(5)),
        scratch_shapes=[
            pltpu.VMEM(key_cache.shape, BF16),
            pltpu.VMEM(value_cache.shape, BF16),
            pltpu.VMEM(out_weight.shape, BF16),
            pltpu.VMEM(queries.shape, BF16),
            pltpu.VMEM((slots, width), BF16),
            pltpu.VMEM((slots, width), BF16),
            pltpu.SMEM(lens.shape, jnp.int32),
            pltpu.SMEM(new.shape, jnp.int32),
            pltpu.SMEM((chosen.shape[1], slots), jnp.int32),
            pltpu.VMEM(residual.shape, BF16),
            pltpu.VMEM((slots, width), F32),
            pltpu.VMEM((slots, width), F32),
            pltpu.VMEM((slots * 8, width), F32),
            pltpu.SemaphoreType.DMA((len(sources),)),
        ],
        compiler_params=pltpu.CompilerParams(vmem_limit_bytes=9 * MIB),
        name="attend",
    )(*[pinned(x) for x in sources])


def fold_kernel(keep_ref, got_ref, mine_ref, send_ref):
    total = keep_ref[...] + got_ref[...].astype(F32)
    mine_ref[...] = total
    half = total.shape[0] // 2
    send_ref[0:half, :] = total[half:].astype(send_ref.dtype)
    send_ref[half:, :] = total[:half].astype(send_ref.dtype)


def fold(keep, got):
    return pl.pallas_call(
        fold_kernel,
        out_shape=(
            jax.ShapeDtypeStruct(keep.shape, F32),
            jax.ShapeDtypeStruct(keep.shape, BF16),
        ),
        in_specs=vmem(2),
        out_specs=tuple(vmem(2)),
        compiler_params=pltpu.CompilerParams(vmem_limit_bytes=2 * MIB),
        name="fold",
    )(keep, got)


def norm_kernel(mine_ref, got_ref, base_ref, gain_ref, router_ref, pick_ref, stream_ref, packet_ref):
    rows, model = mine_ref.shape
    per = rows // 2
    experts = router_ref.shape[0]
    total = base_ref[...] + (mine_ref[...] + got_ref[...].astype(F32))
    stream = total.astype(BF16)
    stream_ref[...] = stream[:per]
    values = stream.astype(F32)
    scaling = lax.rsqrt(jnp.mean(values * values, axis=1, keepdims=True) + EPSILON)
    normed = (values * scaling * gain_ref[...]).astype(BF16)
    packet_ref[:, :model] = normed
    logits = lax.dot_general(
        normed, router_ref[...], (((1,), (1,)), ((), ())), preferred_element_type=F32
    )
    first, second = pick_ref[:, 0:1], pick_ref[:, 1:2]
    labels = lax.broadcasted_iota(jnp.int32, logits.shape, 1)
    first_logit = jnp.sum(jnp.where(labels == first, logits, 0.0), axis=1, keepdims=True)
    second_logit = jnp.sum(jnp.where(labels == second, logits, 0.0), axis=1, keepdims=True)
    leading = 1.0 / (1.0 + jnp.exp(second_logit - first_logit))
    lanes = lax.broadcasted_iota(jnp.int32, (rows, LANES), 1)
    expert = lax.rem(lanes, experts)
    coef = jnp.where(
        expert == first, leading, jnp.where(expert == second, 1.0 - leading, F32(0.0))
    )
    high = coef.astype(BF16).astype(F32)
    packet_ref[:, model:] = jnp.where(lanes < experts, high, coef - high).astype(BF16)


def norm(mine, got, base, gain, router, pick):
    rows, model = mine.shape
    return pl.pallas_call(
        norm_kernel,
        out_shape=(
            jax.ShapeDtypeStruct((rows // 2, model), BF16),
            jax.ShapeDtypeStruct((rows, model + LANES), BF16),
        ),
        in_specs=vmem(6),
        out_specs=tuple(vmem(2)),
        compiler_params=pltpu.CompilerParams(vmem_limit_bytes=2 * MIB),
        name="norm",
    )(mine, got, base, gain, router.T, pick)


def join_kernel(a_ref, b_ref, out_ref):
    rows = a_ref.shape[0]
    out_ref[0:rows, :] = a_ref[...]
    out_ref[rows:, :] = b_ref[...]


def join(a, b):
    return pl.pallas_call(
        join_kernel,
        out_shape=jax.ShapeDtypeStruct((2 * a.shape[0], a.shape[1]), a.dtype),
        in_specs=vmem(2),
        out_specs=vmem(1)[0],
        compiler_params=pltpu.CompilerParams(vmem_limit_bytes=2 * MIB),
        name="join",
    )(a, b)


def expert_kernel(axis, experts, parts, *refs):
    packets = refs[:parts]
    gate_ref, up_ref, down_hbm, keep_ref, send_ref = refs[parts : parts + 5]
    x_ref, hidden_ref, down_ref, sems = refs[parts + 5 :]
    me = lax.axis_index(axis)
    _, model, hidden = gate_ref.shape
    chunk = min(hidden, 512)
    slots, _, down_chunk = down_ref.shape

    def down_copy(j):
        cols = pl.ds(j * down_chunk, down_chunk)
        slot = j % slots
        return pltpu.make_async_copy(down_hbm.at[0, :, cols], down_ref.at[slot], sems.at[slot])

    for j in range(slots):
        down_copy(j).start()
    rows = packets[0].shape[0]
    coefs = []
    for i, packet in enumerate(packets):
        x_ref[i * rows : (i + 1) * rows, :] = packet[:, :model]
        tail = packet[:, model:].astype(F32)
        lanes = lax.broadcasted_iota(jnp.int32, tail.shape, 1)
        mine = (lanes == me) | (lanes == me + experts)
        coefs.append(jnp.sum(jnp.where(mine, tail, 0.0), axis=1, keepdims=True))
    coef = jnp.concatenate(coefs, axis=0)
    for start in range(0, hidden, chunk):
        cols = slice(start, start + chunk)
        gate = jnp.dot(x_ref[...], gate_ref[0, :, cols], preferred_element_type=F32)
        up = jnp.dot(x_ref[...], up_ref[0, :, cols], preferred_element_type=F32)
        hidden_ref[:, cols] = (gate / (1.0 + jnp.exp(-gate)) * up).astype(BF16)
    half = x_ref.shape[0] // 2
    count = model // down_chunk
    for j in range(count):
        cols = slice(j * down_chunk, (j + 1) * down_chunk)
        down_copy(j).wait()
        out = jnp.dot(hidden_ref[...], down_ref[j % slots], preferred_element_type=F32) * coef
        keep_ref[:, cols] = out[:half]
        send_ref[:, cols] = out[half:].astype(BF16)
        if j + slots < count:
            down_copy(j + slots).start()


def expert_ffn(axis, experts, packets, w_gate, w_up, w_down):
    parts = len(packets)
    rows = parts * packets[0].shape[0]
    model, hidden = w_gate.shape[1:]
    half = rows // 2
    down_chunk = min(model, 512)
    slots = min(SLOTS, model // down_chunk)
    limit = rows * (model + hidden) * 2 + slots * hidden * down_chunk * 2 + 1 * MIB
    return pl.pallas_call(
        functools.partial(expert_kernel, axis, experts, parts),
        out_shape=(
            jax.ShapeDtypeStruct((half, model), F32),
            jax.ShapeDtypeStruct((half, model), BF16),
        ),
        in_specs=vmem(parts + 2) + [pl.BlockSpec(memory_space=pltpu.HBM)],
        out_specs=tuple(vmem(2)),
        scratch_shapes=[
            pltpu.VMEM((rows, model), BF16),
            pltpu.VMEM((rows, hidden), BF16),
            pltpu.VMEM((slots, hidden, down_chunk), BF16),
            pltpu.SemaphoreType.DMA((slots,)),
        ],
        compiler_params=pltpu.CompilerParams(vmem_limit_bytes=limit),
        name="experts",
    )(*packets, w_gate, w_up, pinned(w_down))


def halve_kernel(keep_ref, got_ref, mine_ref, send_ref):
    half = keep_ref.shape[0] // 2
    total = keep_ref[...] + got_ref[...].astype(F32)
    mine_ref[...] = total[:half]
    send_ref[...] = total[half:].astype(BF16)


def halve(keep, got):
    rows, model = keep.shape
    return pl.pallas_call(
        halve_kernel,
        out_shape=(
            jax.ShapeDtypeStruct((rows // 2, model), F32),
            jax.ShapeDtypeStruct((rows // 2, model), BF16),
        ),
        in_specs=vmem(2),
        out_specs=tuple(vmem(2)),
        compiler_params=pltpu.CompilerParams(vmem_limit_bytes=rows * model * 12 + 2 * MIB),
        name="halve",
    )(keep, got)


def last_kernel(keep_ref, got_ref, stream_ref, out_ref):
    total = keep_ref[...] + got_ref[...].astype(F32) + stream_ref[...].astype(F32)
    out_ref[...] = total.astype(BF16)


def last(keep, got, stream):
    return pl.pallas_call(
        last_kernel,
        out_shape=jax.ShapeDtypeStruct(stream.shape, BF16),
        in_specs=vmem(3),
        out_specs=vmem(1)[0],
        compiler_params=pltpu.CompilerParams(vmem_limit_bytes=2 * MIB),
        name="last",
    )(keep, got, stream)


def body(
    experts,
    batches,
    residual_in,
    queries,
    key_new,
    value_new,
    key_cache,
    value_cache,
    cache_len,
    new_slot,
    out_weight,
    norm_gain,
    router,
    chosen,
    w_gate,
    w_up,
    w_down,
):
    def swap(x, axis, size, bit):
        return lax.ppermute(x, axis, [(i, i ^ bit) for i in range(size)])

    batch_bits = []
    bit = 1
    while bit < batches:
        batch_bits.append(bit)
        bit *= 2

    keep, send, base, gain, pick = attend(
        experts, "expert", queries, key_new, value_new, key_cache, value_cache, cache_len, new_slot,
        out_weight, residual_in, norm_gain, chosen,
    )
    w_gate, w_up, pick = lax.optimization_barrier((w_gate, w_up, pick))
    w_gate, w_up = [
        lax.ppermute(w, "expert", [(i, i) for i in range(experts)]) for w in (w_gate, w_up)
    ]
    mine, send = fold(keep, swap(send, "expert", experts, 1))
    got = swap(send, "expert", experts, 2)
    stream, packet = norm(mine, got, base, gain, router, pick)
    for bit in batch_bits[:0:-1]:
        packet = join(packet, swap(packet, "batch", batches, bit))
    near = [packet] + [swap(packet, "batch", batches, bit) for bit in batch_bits[:1]]
    packets = near + [swap(p, "expert", experts, 1) for p in near]
    keep, send = expert_ffn("expert", experts, packets, *(w_gate, w_up, w_down))
    got = swap(send, "expert", experts, 1)
    for bit in batch_bits:
        keep, send = halve(keep, got)
        got = swap(send, "batch", batches, bit)
    keep, send = halve(keep, got)
    got = swap(send, "expert", experts, 2)
    return last(keep, got, stream)


def solution(mesh):
    rows = P(("group", "batch"), None)
    heads = P(("group", "batch"), "expert", None)
    cache = P(("group", "batch"), "expert", None, None)
    slot = P(("group", "batch"))
    in_specs = (
        rows,
        heads,
        heads,
        heads,
        cache,
        cache,
        slot,
        slot,
        P("expert", None),
        P(),
        P(),
        rows,
        P("expert", None, "batch"),
        P("expert", None, "batch"),
        P("expert", "batch", None),
    )
    out_specs = P(("group", "batch", "expert"), None)
    inner = functools.partial(body, mesh.shape["expert"], mesh.shape["batch"])
    return jax.shard_map(inner, mesh=mesh, in_specs=in_specs, out_specs=out_specs, check_vma=False)
```

```python
import functools

import jax
import jax.numpy as jnp
from jax import lax
from jax.experimental import pallas as pl
from jax.experimental.pallas import tpu as pltpu
from jax.sharding import PartitionSpec as P

EPSILON = 1e-05
LANES = 128
MIB = 1 << 20
SLOTS = 6
FETCH = (1, 3)

F32 = jnp.float32
BF16 = jnp.bfloat16


def vmem(count=1):
    return [pl.BlockSpec(memory_space=pltpu.VMEM)] * count


def pinned(x):
    return pltpu.with_memory_space_constraint(x, pltpu.HBM)


def attend_kernel(blocks, axis, *refs):
    sources, outs, rest = refs[:12], refs[12:18], refs[18:]
    keep_ref, send_ref, base_ref, gain_ref, router_ref, pick_ref = outs
    (
        k_ref,
        v_ref,
        w_ref,
        q_ref,
        kn_ref,
        vn_ref,
        len_ref,
        new_ref,
        chosen_ref,
        res_ref,
        own_key_ref,
        own_value_ref,
        att_ref,
        sems,
    ) = rest
    slots, heads, width = q_ref.shape
    length = k_ref.shape[2]
    per = slots // blocks
    half = slots // 2
    me = lax.axis_index(axis)
    targets = (len_ref, new_ref, q_ref, kn_ref, k_ref, vn_ref, v_ref, w_ref, chosen_ref, res_ref)
    targets += (gain_ref, router_ref)
    copies = []
    for i, (source, target) in enumerate(zip(sources, targets)):
        copies.append(pltpu.make_async_copy(source, target, sems.at[i]))
        copies[-1].start()
    scaling = float(width) ** (-0.5)
    places = lax.broadcasted_iota(jnp.int32, (heads, length), 1)
    order = []
    for block in list(range(0, blocks, 2)) + list(range(1, blocks, 2)):
        owner = lax.bitwise_xor(me, block)
        order += [owner * per + i for i in range(per)]
    for copy in copies[:4]:
        copy.wait()
    own_key_ref[...] = kn_ref[...].astype(F32)
    copies[4].wait()
    probs = []
    for slot in order:
        query = q_ref[slot]
        scores = (
            lax.dot_general(
                query, k_ref[slot, 0], (((1,), (1,)), ((), ())), preferred_element_type=F32
            )
            * scaling
        )
        own = (
            jnp.sum(query.astype(F32) * own_key_ref[pl.ds(slot, 1), :], axis=1, keepdims=True)
            * scaling
        )
        usable = (places < len_ref[slot]) & (new_ref[slot] == 0)
        scores = jnp.where(usable, scores, F32(-1e30))
        highest = jnp.maximum(jnp.max(scores, axis=1, keepdims=True), own)
        weights = jnp.where(usable, jnp.exp(scores - highest), F32(0.0))
        own_weight = jnp.exp(own - highest)
        total = jnp.sum(weights, axis=1, keepdims=True) + own_weight
        probs.append(((weights / total).astype(BF16), (own_weight / total).astype(BF16)))
    copies[5].wait()
    own_value_ref[...] = vn_ref[...].astype(F32)
    copies[6].wait()
    for place, slot in enumerate(order):
        prob, own_prob = probs[place]
        attended = jnp.dot(prob, v_ref[slot, 0], preferred_element_type=F32)
        attended = attended + own_prob.astype(F32) * own_value_ref[pl.ds(slot, 1), :]
        att_ref[pl.ds(place * 8, heads), :] = attended
    rows = jnp.concatenate(
        [att_ref[pl.ds(head, slots, stride=8), :] for head in range(heads)], axis=1
    ).astype(BF16)
    copies[7].wait()
    columns = w_ref.shape[1]
    step = min(columns, 1024)
    for start in range(0, columns, step):
        part = jnp.dot(rows, w_ref[:, start : start + step], preferred_element_type=F32)
        keep_ref[:, start : start + step] = part[:half]
        send_ref[:, start : start + step] = part[half:].astype(send_ref.dtype)
    for copy in copies[8:]:
        copy.wait()
    lines = lax.broadcasted_iota(jnp.int32, (half, LANES), 0)
    lanes = lax.broadcasted_iota(jnp.int32, (half, LANES), 1)
    picks = jnp.zeros((half, LANES), jnp.int32)
    for place, slot in enumerate(order[:half]):
        named = jnp.where(lanes == 0, chosen_ref[0, slot], chosen_ref[1, slot])
        picks = jnp.where(lines == place, named, picks)
    pick_ref[...] = picks
    residual = res_ref[...].astype(F32)
    kept = []
    for block in range(0, blocks, 2):
        owner = lax.bitwise_xor(me, block)
        value = residual[:per]
        for other in range(1, blocks):
            value = jnp.where(owner == other, residual[other * per : (other + 1) * per], value)
        kept.append(value)
    base_ref[...] = jnp.concatenate(kept, axis=0)


def attend(
    blocks, axis, queries, key_new, value_new, key_cache, value_cache, lens, new, out_weight,
    residual, gain, router, chosen,
):
    slots, heads, width = queries.shape
    columns = out_weight.shape[1]
    half = slots // 2
    sources = (
        lens,
        new,
        queries,
        key_new.reshape(slots, width),
        key_cache,
        value_new.reshape(slots, width),
        value_cache,
        out_weight,
        chosen.T,
        residual,
        gain.reshape(1, columns),
        router.T,
    )
    return pl.pallas_call(
        functools.partial(attend_kernel, blocks, axis),
        out_shape=(
            jax.ShapeDtypeStruct((half, columns), F32),
            jax.ShapeDtypeStruct((half, columns), F32),
            jax.ShapeDtypeStruct((half, columns), F32),
            jax.ShapeDtypeStruct((1, columns), F32),
            jax.ShapeDtypeStruct(router.shape[::-1], BF16),
            jax.ShapeDtypeStruct((half, LANES), jnp.int32),
        ),
        in_specs=[pl.BlockSpec(memory_space=pltpu.HBM)] * len(sources),
        out_specs=tuple(vmem(6)),
        scratch_shapes=[
            pltpu.VMEM(key_cache.shape, BF16),
            pltpu.VMEM(value_cache.shape, BF16),
            pltpu.VMEM(out_weight.shape, BF16),
            pltpu.VMEM(queries.shape, BF16),
            pltpu.VMEM((slots, width), BF16),
            pltpu.VMEM((slots, width), BF16),
            pltpu.SMEM(lens.shape, jnp.int32),
            pltpu.SMEM(new.shape, jnp.int32),
            pltpu.SMEM((chosen.shape[1], slots), jnp.int32),
            pltpu.VMEM(residual.shape, BF16),
            pltpu.VMEM((slots, width), F32),
            pltpu.VMEM((slots, width), F32),
            pltpu.VMEM((slots * 8, width), F32),
            pltpu.SemaphoreType.DMA((len(sources),)),
        ],
        compiler_params=pltpu.CompilerParams(vmem_limit_bytes=9 * MIB),
        name="attend",
    )(*[pinned(x) for x in sources])


def fold_kernel(keep_ref, got_ref, mine_ref, send_ref):
    total = keep_ref[...] + got_ref[...].astype(F32)
    mine_ref[...] = total
    half = total.shape[0] // 2
    send_ref[0:half, :] = total[half:].astype(send_ref.dtype)
    send_ref[half:, :] = total[:half].astype(send_ref.dtype)


def fold(keep, got):
    return pl.pallas_call(
        fold_kernel,
        out_shape=(
            jax.ShapeDtypeStruct(keep.shape, F32),
            jax.ShapeDtypeStruct(keep.shape, BF16),
        ),
        in_specs=vmem(2),
        out_specs=tuple(vmem(2)),
        compiler_params=pltpu.CompilerParams(vmem_limit_bytes=2 * MIB),
        name="fold",
    )(keep, got)


def norm_kernel(mine_ref, got_ref, base_ref, gain_ref, router_ref, pick_ref, _, stream_ref, packet_ref):
    rows, model = mine_ref.shape
    per = rows // 2
    experts = router_ref.shape[0]
    total = base_ref[...] + (mine_ref[...] + got_ref[...].astype(F32))
    stream = total.astype(BF16)
    stream_ref[...] = stream[:per]
    values = stream.astype(F32)
    scaling = lax.rsqrt(jnp.mean(values * values, axis=1, keepdims=True) + EPSILON)
    normed = (values * scaling * gain_ref[...]).astype(BF16)
    packet_ref[:, :model] = normed
    logits = lax.dot_general(
        normed, router_ref[...], (((1,), (1,)), ((), ())), preferred_element_type=F32
    )
    first, second = pick_ref[:, 0:1], pick_ref[:, 1:2]
    labels = lax.broadcasted_iota(jnp.int32, logits.shape, 1)
    first_logit = jnp.sum(jnp.where(labels == first, logits, 0.0), axis=1, keepdims=True)
    second_logit = jnp.sum(jnp.where(labels == second, logits, 0.0), axis=1, keepdims=True)
    leading = 1.0 / (1.0 + jnp.exp(second_logit - first_logit))
    lanes = lax.broadcasted_iota(jnp.int32, (rows, LANES), 1)
    expert = lax.rem(lanes, experts)
    coef = jnp.where(
        expert == first, leading, jnp.where(expert == second, 1.0 - leading, F32(0.0))
    )
    high = coef.astype(BF16).astype(F32)
    packet_ref[:, model:] = jnp.where(lanes < experts, high, coef - high).astype(BF16)


def norm(mine, got, base, gain, router, pick, token):
    rows, model = mine.shape
    return pl.pallas_call(
        norm_kernel,
        out_shape=(
            jax.ShapeDtypeStruct((rows // 2, model), BF16),
            jax.ShapeDtypeStruct((rows, model + LANES), BF16),
        ),
        in_specs=vmem(6) + [pl.BlockSpec(memory_space=pl.ANY)],
        out_specs=tuple(vmem(2)),
        compiler_params=pltpu.CompilerParams(vmem_limit_bytes=2 * MIB),
        name="norm",
    )(mine, got, base, gain, router, pick, token)


def join_kernel(*refs):
    parts, out_ref = refs[:-2], refs[-1]
    rows = parts[0].shape[0]
    for i, part in enumerate(parts):
        out_ref[i * rows : (i + 1) * rows, :] = part[...]


def join(parts, token):
    rows, columns = parts[0].shape
    return pl.pallas_call(
        join_kernel,
        out_shape=jax.ShapeDtypeStruct((len(parts) * rows, columns), parts[0].dtype),
        in_specs=vmem(len(parts)) + [pl.BlockSpec(memory_space=pl.ANY)],
        out_specs=vmem(1)[0],
        compiler_params=pltpu.CompilerParams(vmem_limit_bytes=2 * MIB),
        name="join",
    )(*parts, token)


def fetch_kernel(starts, width, *refs):
    count = len(starts)
    sources, outs = refs[:count], refs[count + 1 : 2 * count + 1]
    done_ref, sems = refs[2 * count + 1 :]
    copies = []
    for i, (start, source, out) in enumerate(zip(starts, sources, outs)):
        columns = pl.ds(start, width)
        copies.append(pltpu.make_async_copy(source.at[0, :, columns], out, sems.at[i]))
        copies[-1].start()
    done_ref[...] = jnp.zeros_like(done_ref)
    for copy in copies:
        copy.wait()


def fetch(pieces, width, token):
    count = len(pieces)
    if not count:
        return [], token
    rows = pieces[0][0].shape[1]
    size = rows * width * 2 * count
    *got, done = pl.pallas_call(
        functools.partial(fetch_kernel, [start for _, start in pieces], width),
        out_shape=[pltpu.VMEM((rows, width), BF16)] * count
        + [jax.ShapeDtypeStruct((8, LANES), F32)],
        in_specs=[pl.BlockSpec(memory_space=pltpu.HBM)] * count
        + [pl.BlockSpec(memory_space=pl.ANY)],
        out_specs=vmem(count + 1),
        scratch_shapes=[pltpu.SemaphoreType.DMA((count,))],
        compiler_params=pltpu.CompilerParams(vmem_limit_bytes=MIB),
        cost_estimate=pl.CostEstimate(flops=0, bytes_accessed=size, transcendentals=0),
        name="fetch",
    )(*[pinned(w) for w, _ in pieces], token)
    return got, done


def expert_kernel(axis, experts, parts, held, chunk, *refs):
    packets, ready = refs[:parts], refs[parts : parts + held]
    refs = refs[parts + held :]
    gate_hbm, up_hbm, down_hbm, keep_ref, send_ref, x_ref, hidden_ref, piece_ref, down_ref = refs[:9]
    piece_sems, down_sems = refs[9:]
    me = lax.axis_index(axis)
    model = x_ref.shape[1]
    hidden = hidden_ref.shape[1]
    slots, _, down_chunk = down_ref.shape
    pieces = [(w, start) for start in range(0, hidden, chunk) for w in (gate_hbm, up_hbm)]
    copies = {}
    for i in range(held, len(pieces)):
        source, start = pieces[i]
        copies[i] = pltpu.make_async_copy(
            source.at[0, :, pl.ds(start, chunk)], piece_ref.at[i - held], piece_sems.at[i - held]
        )
        copies[i].start()

    def down_copy(j):
        columns = pl.ds(j * down_chunk, down_chunk)
        slot = j % slots
        return pltpu.make_async_copy(down_hbm.at[0, :, columns], down_ref.at[slot], down_sems.at[slot])

    for j in range(slots):
        down_copy(j).start()
    rows = packets[0].shape[0]
    coefs = []
    for i, packet in enumerate(packets):
        x_ref[i * rows : (i + 1) * rows, :] = packet[:, :model]
        tail = packet[:, model:].astype(F32)
        lanes = lax.broadcasted_iota(jnp.int32, tail.shape, 1)
        mine = (lanes == me) | (lanes == me + experts)
        coefs.append(jnp.sum(jnp.where(mine, tail, 0.0), axis=1, keepdims=True))
    coef = jnp.concatenate(coefs, axis=0)

    def product(i):
        if i < held:
            return jnp.dot(x_ref[...], ready[i][...], preferred_element_type=F32)
        copies[i].wait()
        return jnp.dot(x_ref[...], piece_ref[i - held], preferred_element_type=F32)

    for j in range(hidden // chunk):
        gate, up = product(2 * j), product(2 * j + 1)
        hidden_ref[:, j * chunk : (j + 1) * chunk] = (gate / (1.0 + jnp.exp(-gate)) * up).astype(BF16)
    half = x_ref.shape[0] // 2
    count = model // down_chunk
    for j in range(count):
        cols = slice(j * down_chunk, (j + 1) * down_chunk)
        down_copy(j).wait()
        out = jnp.dot(hidden_ref[...], down_ref[j % slots], preferred_element_type=F32) * coef
        keep_ref[:, cols] = out[:half]
        send_ref[:, cols] = out[half:].astype(BF16)
        if j + slots < count:
            down_copy(j + slots).start()


def expert_ffn(axis, experts, packets, ready, chunk, w_gate, w_up, w_down):
    parts, held = len(packets), len(ready)
    rows = parts * packets[0].shape[0]
    model, hidden = w_gate.shape[1:]
    half = rows // 2
    down_chunk = min(model, 512)
    slots = min(SLOTS, model // down_chunk)
    left = max(2 * (hidden // chunk) - held, 1)
    scratch = left * model * chunk * 2 + slots * hidden * down_chunk * 2
    limit = rows * (model + hidden) * 2 + scratch + 1 * MIB
    return pl.pallas_call(
        functools.partial(expert_kernel, axis, experts, parts, held, chunk),
        out_shape=(
            jax.ShapeDtypeStruct((half, model), F32),
            jax.ShapeDtypeStruct((half, model), BF16),
        ),
        in_specs=vmem(parts + held) + [pl.BlockSpec(memory_space=pltpu.HBM)] * 3,
        out_specs=tuple(vmem(2)),
        scratch_shapes=[
            pltpu.VMEM((rows, model), BF16),
            pltpu.VMEM((rows, hidden), BF16),
            pltpu.VMEM((left, model, chunk), BF16),
            pltpu.VMEM((slots, hidden, down_chunk), BF16),
            pltpu.SemaphoreType.DMA((left,)),
            pltpu.SemaphoreType.DMA((slots,)),
        ],
        compiler_params=pltpu.CompilerParams(vmem_limit_bytes=limit),
        cost_estimate=pl.CostEstimate(
            flops=6 * rows * model * hidden,
            bytes_accessed=6 * model * hidden,
            transcendentals=rows * hidden,
        ),
        name="experts",
    )(*packets, *ready, pinned(w_gate), pinned(w_up), pinned(w_down))


def spread_kernel(keep_ref, got_ref, mine_ref, *send_refs):
    part = mine_ref.shape[0]
    mine_ref[...] = keep_ref[:part] + got_ref[:part].astype(F32)
    for i, send_ref in enumerate(send_refs):
        rows = slice((i + 1) * part, (i + 2) * part)
        send_ref[...] = (keep_ref[rows] + got_ref[rows].astype(F32)).astype(BF16)


def spread(count, keep, got):
    rows, model = keep.shape
    part = rows // count
    return pl.pallas_call(
        spread_kernel,
        out_shape=[jax.ShapeDtypeStruct((part, model), F32)]
        + [jax.ShapeDtypeStruct((part, model), BF16)] * (count - 1),
        in_specs=vmem(2),
        out_specs=vmem(count),
        compiler_params=pltpu.CompilerParams(vmem_limit_bytes=rows * model * 4 + 2 * MIB),
        name="spread",
    )(keep, got)


def collect_kernel(mine_ref, *refs):
    gots, keep_ref, send_ref = refs[:-2], refs[-2], refs[-1]
    total = mine_ref[...]
    for got in gots:
        total = total + got[...].astype(F32)
    half = total.shape[0] // 2
    keep_ref[...] = total[:half]
    send_ref[...] = total[half:].astype(BF16)


def collect(mine, gots):
    rows, model = mine.shape
    return pl.pallas_call(
        collect_kernel,
        out_shape=(
            jax.ShapeDtypeStruct((rows // 2, model), F32),
            jax.ShapeDtypeStruct((rows // 2, model), BF16),
        ),
        in_specs=vmem(1 + len(gots)),
        out_specs=tuple(vmem(2)),
        compiler_params=pltpu.CompilerParams(vmem_limit_bytes=rows * model * 4 + 2 * MIB),
        name="collect",
    )(mine, *gots)


def last_kernel(keep_ref, got_ref, stream_ref, out_ref):
    total = keep_ref[...] + got_ref[...].astype(F32) + stream_ref[...].astype(F32)
    out_ref[...] = total.astype(BF16)


def last(keep, got, stream):
    return pl.pallas_call(
        last_kernel,
        out_shape=jax.ShapeDtypeStruct(stream.shape, BF16),
        in_specs=vmem(3),
        out_specs=vmem(1)[0],
        compiler_params=pltpu.CompilerParams(vmem_limit_bytes=2 * MIB),
        name="last",
    )(keep, got, stream)


def body(
    experts,
    batches,
    residual_in,
    queries,
    key_new,
    value_new,
    key_cache,
    value_cache,
    cache_len,
    new_slot,
    out_weight,
    norm_gain,
    router,
    chosen,
    w_gate,
    w_up,
    w_down,
):
    def swap(x, axis, size, bit):
        return lax.ppermute(x, axis, [(i, i ^ bit) for i in range(size)])

    near = min(batches, 4)
    far_bits = []
    bit = near
    while bit < batches:
        far_bits.append(bit)
        bit *= 2
    hidden = w_gate.shape[2]
    chunk = min(hidden, 512)
    pieces = [(w, start) for start in range(0, hidden, chunk) for w in (w_gate, w_up)]
    early = [pieces[:FETCH[0]], pieces[FETCH[0] : FETCH[1]]]

    keep, send, base, gain, routing, pick = attend(
        experts, "expert", queries, key_new, value_new, key_cache, value_cache, cache_len, new_slot,
        out_weight, residual_in, norm_gain, router, chosen,
    )
    mine, send = fold(keep, swap(send, "expert", experts, 1))
    got = swap(send, "expert", experts, 2)
    ready, token = fetch(early[0], chunk, send)
    stream, packet = norm(mine, got, base, gain, routing, pick, token)
    for bit in far_bits[::-1]:
        packet = join([packet, swap(packet, "batch", batches, bit)], token)
    around = [swap(packet, "batch", batches, bit) for bit in range(1, near)]
    more, token = fetch(early[1], chunk, packet)
    ready += more
    packet = join([packet] + around, token)
    packets = [packet, swap(packet, "expert", experts, 1)]
    keep, send = expert_ffn("expert", experts, packets, ready, chunk, w_gate, w_up, w_down)
    got = swap(send, "expert", experts, 1)
    if near > 1:
        keep, *sends = spread(near, keep, got)
        gots = [swap(s, "batch", batches, i + 1) for i, s in enumerate(sends)]
    else:
        gots = [got]
    for bit in far_bits:
        keep, send = collect(keep, gots)
        gots = [swap(send, "batch", batches, bit)]
    keep, send = collect(keep, gots)
    got = swap(send, "expert", experts, 2)
    return last(keep, got, stream)


def solution(mesh):
    rows = P(("group", "batch"), None)
    heads = P(("group", "batch"), "expert", None)
    cache = P(("group", "batch"), "expert", None, None)
    slot = P(("group", "batch"))
    in_specs = (
        rows,
        heads,
        heads,
        heads,
        cache,
        cache,
        slot,
        slot,
        P("expert", None),
        P(),
        P(),
        rows,
        P("expert", None, "batch"),
        P("expert", None, "batch"),
        P("expert", "batch", None),
    )
    out_specs = P(("group", "batch", "expert"), None)
    inner = functools.partial(body, mesh.shape["expert"], mesh.shape["batch"])
    return jax.shard_map(inner, mesh=mesh, in_specs=in_specs, out_specs=out_specs, check_vma=False)
```

```python
import functools

import jax
import jax.numpy as jnp
from jax import lax
from jax.experimental import pallas as pl
from jax.experimental.pallas import tpu as pltpu
from jax.sharding import PartitionSpec as P

EPSILON = 1e-05
LANES = 128
MIB = 1 << 20
SLOTS = 6
FETCH = (1, 3)

F32 = jnp.float32
BF16 = jnp.bfloat16


def vmem(count=1):
    return [pl.BlockSpec(memory_space=pltpu.VMEM)] * count


def pinned(x):
    return pltpu.with_memory_space_constraint(x, pltpu.HBM)


def attend_kernel(blocks, axis, *refs):
    sources, outs, rest = refs[:12], refs[12:18], refs[18:]
    keep_ref, send_ref, base_ref, gain_ref, router_ref, pick_ref = outs
    (
        k_ref,
        v_ref,
        w_ref,
        q_ref,
        kn_ref,
        vn_ref,
        len_ref,
        new_ref,
        chosen_ref,
        res_ref,
        own_key_ref,
        own_value_ref,
        att_ref,
        sems,
    ) = rest
    slots, heads, width = q_ref.shape
    length = k_ref.shape[2]
    per = slots // blocks
    half = slots // 2
    me = lax.axis_index(axis)
    targets = (len_ref, new_ref, q_ref, kn_ref, k_ref, vn_ref, v_ref, w_ref, chosen_ref, res_ref)
    targets += (gain_ref, router_ref)
    copies = []
    for i, (source, target) in enumerate(zip(sources, targets)):
        copies.append(pltpu.make_async_copy(source, target, sems.at[i]))
        copies[-1].start()
    scaling = float(width) ** (-0.5)
    places = lax.broadcasted_iota(jnp.int32, (heads, length), 1)
    order = []
    for block in list(range(0, blocks, 2)) + list(range(1, blocks, 2)):
        owner = lax.bitwise_xor(me, block)
        order += [owner * per + i for i in range(per)]
    for copy in copies[:4]:
        copy.wait()
    own_key_ref[...] = kn_ref[...].astype(F32)
    copies[4].wait()
    probs = []
    for slot in order:
        query = q_ref[slot]
        scores = (
            lax.dot_general(
                query, k_ref[slot, 0], (((1,), (1,)), ((), ())), preferred_element_type=F32
            )
            * scaling
        )
        own = (
            jnp.sum(query.astype(F32) * own_key_ref[pl.ds(slot, 1), :], axis=1, keepdims=True)
            * scaling
        )
        usable = (places < len_ref[slot]) & (new_ref[slot] == 0)
        scores = jnp.where(usable, scores, F32(-1e30))
        highest = jnp.maximum(jnp.max(scores, axis=1, keepdims=True), own)
        weights = jnp.where(usable, jnp.exp(scores - highest), F32(0.0))
        own_weight = jnp.exp(own - highest)
        total = jnp.sum(weights, axis=1, keepdims=True) + own_weight
        probs.append(((weights / total).astype(BF16), (own_weight / total).astype(BF16)))
    copies[5].wait()
    own_value_ref[...] = vn_ref[...].astype(F32)
    copies[6].wait()
    for place, slot in enumerate(order):
        prob, own_prob = probs[place]
        attended = jnp.dot(prob, v_ref[slot, 0], preferred_element_type=F32)
        attended = attended + own_prob.astype(F32) * own_value_ref[pl.ds(slot, 1), :]
        att_ref[pl.ds(place * 8, heads), :] = attended
    rows = jnp.concatenate(
        [att_ref[pl.ds(head, slots, stride=8), :] for head in range(heads)], axis=1
    ).astype(BF16)
    copies[7].wait()
    columns = w_ref.shape[1]
    step = min(columns, 1024)
    for start in range(0, columns, step):
        part = jnp.dot(rows, w_ref[:, start : start + step], preferred_element_type=F32)
        keep_ref[:, start : start + step] = part[:half]
        send_ref[:, start : start + step] = part[half:].astype(send_ref.dtype)
    for copy in copies[8:]:
        copy.wait()
    lines = lax.broadcasted_iota(jnp.int32, (half, LANES), 0)
    lanes = lax.broadcasted_iota(jnp.int32, (half, LANES), 1)
    picks = jnp.zeros((half, LANES), jnp.int32)
    for place, slot in enumerate(order[:half]):
        named = jnp.where(lanes == 0, chosen_ref[0, slot], chosen_ref[1, slot])
        picks = jnp.where(lines == place, named, picks)
    pick_ref[...] = picks
    residual = res_ref[...].astype(F32)
    kept = []
    for block in range(0, blocks, 2):
        owner = lax.bitwise_xor(me, block)
        value = residual[:per]
        for other in range(1, blocks):
            value = jnp.where(owner == other, residual[other * per : (other + 1) * per], value)
        kept.append(value)
    base_ref[...] = jnp.concatenate(kept, axis=0)


def attend(
    blocks, axis, queries, key_new, value_new, key_cache, value_cache, lens, new, out_weight,
    residual, gain, router, chosen,
):
    slots, heads, width = queries.shape
    columns = out_weight.shape[1]
    half = slots // 2
    sources = (
        lens,
        new,
        queries,
        key_new.reshape(slots, width),
        key_cache,
        value_new.reshape(slots, width),
        value_cache,
        out_weight,
        chosen.T,
        residual,
        gain.reshape(1, columns),
        router.T,
    )
    return pl.pallas_call(
        functools.partial(attend_kernel, blocks, axis),
        out_shape=(
            jax.ShapeDtypeStruct((half, columns), F32),
            jax.ShapeDtypeStruct((half, columns), F32),
            jax.ShapeDtypeStruct((half, columns), F32),
            jax.ShapeDtypeStruct((1, columns), F32),
            jax.ShapeDtypeStruct(router.shape[::-1], BF16),
            jax.ShapeDtypeStruct((half, LANES), jnp.int32),
        ),
        in_specs=[pl.BlockSpec(memory_space=pltpu.HBM)] * len(sources),
        out_specs=tuple(vmem(6)),
        scratch_shapes=[
            pltpu.VMEM(key_cache.shape, BF16),
            pltpu.VMEM(value_cache.shape, BF16),
            pltpu.VMEM(out_weight.shape, BF16),
            pltpu.VMEM(queries.shape, BF16),
            pltpu.VMEM((slots, width), BF16),
            pltpu.VMEM((slots, width), BF16),
            pltpu.SMEM(lens.shape, jnp.int32),
            pltpu.SMEM(new.shape, jnp.int32),
            pltpu.SMEM((chosen.shape[1], slots), jnp.int32),
            pltpu.VMEM(residual.shape, BF16),
            pltpu.VMEM((slots, width), F32),
            pltpu.VMEM((slots, width), F32),
            pltpu.VMEM((slots * 8, width), F32),
            pltpu.SemaphoreType.DMA((len(sources),)),
        ],
        compiler_params=pltpu.CompilerParams(vmem_limit_bytes=9 * MIB),
        name="attend",
    )(*[pinned(x) for x in sources])


def fold_kernel(keep_ref, got_ref, mine_ref, send_ref):
    total = keep_ref[...] + got_ref[...].astype(F32)
    mine_ref[...] = total
    half = total.shape[0] // 2
    send_ref[0:half, :] = total[half:].astype(send_ref.dtype)
    send_ref[half:, :] = total[:half].astype(send_ref.dtype)


def fold(keep, got):
    return pl.pallas_call(
        fold_kernel,
        out_shape=(
            jax.ShapeDtypeStruct(keep.shape, F32),
            jax.ShapeDtypeStruct(keep.shape, BF16),
        ),
        in_specs=vmem(2),
        out_specs=tuple(vmem(2)),
        compiler_params=pltpu.CompilerParams(vmem_limit_bytes=2 * MIB),
        name="fold",
    )(keep, got)


def norm_kernel(mine_ref, got_ref, base_ref, gain_ref, router_ref, pick_ref, _, stream_ref, packet_ref):
    rows, model = mine_ref.shape
    per = rows // 2
    experts = router_ref.shape[0]
    total = base_ref[...] + (mine_ref[...] + got_ref[...].astype(F32))
    stream = total.astype(BF16)
    stream_ref[...] = stream[:per]
    values = stream.astype(F32)
    scaling = lax.rsqrt(jnp.mean(values * values, axis=1, keepdims=True) + EPSILON)
    normed = (values * scaling * gain_ref[...]).astype(BF16)
    packet_ref[:, :model] = normed
    logits = lax.dot_general(
        normed, router_ref[...], (((1,), (1,)), ((), ())), preferred_element_type=F32
    )
    first, second = pick_ref[:, 0:1], pick_ref[:, 1:2]
    labels = lax.broadcasted_iota(jnp.int32, logits.shape, 1)
    first_logit = jnp.sum(jnp.where(labels == first, logits, 0.0), axis=1, keepdims=True)
    second_logit = jnp.sum(jnp.where(labels == second, logits, 0.0), axis=1, keepdims=True)
    leading = 1.0 / (1.0 + jnp.exp(second_logit - first_logit))
    lanes = lax.broadcasted_iota(jnp.int32, (rows, LANES), 1)
    expert = lax.rem(lanes, experts)
    coef = jnp.where(
        expert == first, leading, jnp.where(expert == second, 1.0 - leading, F32(0.0))
    )
    high = coef.astype(BF16).astype(F32)
    packet_ref[:, model:] = jnp.where(lanes < experts, high, coef - high).astype(BF16)


def norm(mine, got, base, gain, router, pick, token):
    rows, model = mine.shape
    return pl.pallas_call(
        norm_kernel,
        out_shape=(
            jax.ShapeDtypeStruct((rows // 2, model), BF16),
            jax.ShapeDtypeStruct((rows, model + LANES), BF16),
        ),
        in_specs=vmem(6) + [pl.BlockSpec(memory_space=pl.ANY)],
        out_specs=tuple(vmem(2)),
        compiler_params=pltpu.CompilerParams(vmem_limit_bytes=2 * MIB),
        name="norm",
    )(mine, got, base, gain, router, pick, token)


def join_kernel(*refs):
    parts, out_ref = refs[:-2], refs[-1]
    rows = parts[0].shape[0]
    for i, part in enumerate(parts):
        out_ref[i * rows : (i + 1) * rows, :] = part[...]


def join(parts, token):
    rows, columns = parts[0].shape
    return pl.pallas_call(
        join_kernel,
        out_shape=jax.ShapeDtypeStruct((len(parts) * rows, columns), parts[0].dtype),
        in_specs=vmem(len(parts)) + [pl.BlockSpec(memory_space=pl.ANY)],
        out_specs=vmem(1)[0],
        compiler_params=pltpu.CompilerParams(vmem_limit_bytes=2 * MIB),
        name="join",
    )(*parts, token)


def fetch_kernel(starts, width, *refs):
    count = len(starts)
    sources, outs = refs[:count], refs[count + 1 : 2 * count + 1]
    done_ref, sems = refs[2 * count + 1 :]
    copies = []
    for i, (start, source, out) in enumerate(zip(starts, sources, outs)):
        columns = pl.ds(start, width)
        copies.append(pltpu.make_async_copy(source.at[0, :, columns], out, sems.at[i]))
        copies[-1].start()
    done_ref[...] = jnp.zeros_like(done_ref)
    for copy in copies:
        copy.wait()


def fetch(pieces, width, token):
    count = len(pieces)
    if not count:
        return [], token
    rows = pieces[0][0].shape[1]
    size = rows * width * 2 * count
    *got, done = pl.pallas_call(
        functools.partial(fetch_kernel, [start for _, start in pieces], width),
        out_shape=[pltpu.VMEM((rows, width), BF16)] * count
        + [jax.ShapeDtypeStruct((8, LANES), F32)],
        in_specs=[pl.BlockSpec(memory_space=pltpu.HBM)] * count
        + [pl.BlockSpec(memory_space=pl.ANY)],
        out_specs=vmem(count + 1),
        scratch_shapes=[pltpu.SemaphoreType.DMA((count,))],
        compiler_params=pltpu.CompilerParams(vmem_limit_bytes=MIB),
        cost_estimate=pl.CostEstimate(flops=0, bytes_accessed=size, transcendentals=0),
        name="fetch",
    )(*[pinned(w) for w, _ in pieces], token)
    return got, done


def expert_kernel(axis, experts, parts, held, chunk, *refs):
    packets, ready = refs[:parts], refs[parts : parts + held]
    refs = refs[parts + held :]
    gate_hbm, up_hbm, down_hbm, keep_ref, send_ref, x_ref, hidden_ref, piece_ref, down_ref = refs[:9]
    piece_sems, down_sems = refs[9:]
    me = lax.axis_index(axis)
    model = x_ref.shape[0] * LANES
    hidden = hidden_ref.shape[0] * LANES
    slots, _, down_chunk = down_ref.shape
    pieces = [(w, start) for start in range(0, hidden, chunk) for w in (gate_hbm, up_hbm)]
    copies = {}
    for i in range(held, len(pieces)):
        source, start = pieces[i]
        copies[i] = pltpu.make_async_copy(
            source.at[0, :, pl.ds(start, chunk)], piece_ref.at[i - held], piece_sems.at[i - held]
        )
        copies[i].start()

    def down_copy(j):
        columns = pl.ds(j * down_chunk, down_chunk)
        slot = j % slots
        return pltpu.make_async_copy(down_hbm.at[0, :, columns], down_ref.at[slot], down_sems.at[slot])

    for j in range(slots):
        down_copy(j).start()
    rows = packets[0].shape[0]
    coefs = []
    for packet in packets:
        tail = packet[:, model:].astype(F32)
        lanes = lax.broadcasted_iota(jnp.int32, tail.shape, 1)
        mine = (lanes == me) | (lanes == me + experts)
        coefs.append(jnp.sum(jnp.where(mine, tail, 0.0), axis=1, keepdims=True))
    coef = jnp.concatenate(coefs, axis=0)

    def place(k, carry):
        columns = pl.ds(pl.multiple_of(k * LANES, LANES), LANES)
        for i, packet in enumerate(packets):
            x_ref[k, i * rows : (i + 1) * rows, :] = packet[:, columns]
        return carry

    lax.fori_loop(0, model // LANES, place, 0)

    def wide(ref):
        return jnp.concatenate([ref[k] for k in range(ref.shape[0])], axis=1)

    def product(i):
        if i < held:
            return jnp.dot(wide(x_ref), ready[i][...], preferred_element_type=F32)
        copies[i].wait()
        return jnp.dot(wide(x_ref), piece_ref[i - held], preferred_element_type=F32)

    for j in range(hidden // chunk):
        gate, up = product(2 * j), product(2 * j + 1)
        inner = (gate / (1.0 + jnp.exp(-gate)) * up).astype(BF16)
        for k in range(chunk // LANES):
            hidden_ref[j * chunk // LANES + k] = inner[:, k * LANES : (k + 1) * LANES]
    half = x_ref.shape[1] // 2
    count = model // down_chunk
    for j in range(count):
        cols = slice(j * down_chunk, (j + 1) * down_chunk)
        down_copy(j).wait()
        out = jnp.dot(wide(hidden_ref), down_ref[j % slots], preferred_element_type=F32) * coef
        keep_ref[:, cols] = out[:half]
        send_ref[:, cols] = out[half:].astype(BF16)
        if j + slots < count:
            down_copy(j + slots).start()


def expert_ffn(axis, experts, packets, ready, chunk, w_gate, w_up, w_down):
    parts, held = len(packets), len(ready)
    rows = parts * packets[0].shape[0]
    model, hidden = w_gate.shape[1:]
    half = rows // 2
    down_chunk = min(model, 512)
    slots = min(SLOTS, model // down_chunk)
    left = max(2 * (hidden // chunk) - held, 1)
    scratch = left * model * chunk * 2 + slots * hidden * down_chunk * 2
    limit = rows * (model + hidden) * 2 + scratch + 1 * MIB
    return pl.pallas_call(
        functools.partial(expert_kernel, axis, experts, parts, held, chunk),
        out_shape=(
            jax.ShapeDtypeStruct((half, model), F32),
            jax.ShapeDtypeStruct((half, model), BF16),
        ),
        in_specs=vmem(parts + held) + [pl.BlockSpec(memory_space=pltpu.HBM)] * 3,
        out_specs=tuple(vmem(2)),
        scratch_shapes=[
            pltpu.VMEM((model // LANES, rows, LANES), BF16),
            pltpu.VMEM((hidden // LANES, rows, LANES), BF16),
            pltpu.VMEM((left, model, chunk), BF16),
            pltpu.VMEM((slots, hidden, down_chunk), BF16),
            pltpu.SemaphoreType.DMA((left,)),
            pltpu.SemaphoreType.DMA((slots,)),
        ],
        compiler_params=pltpu.CompilerParams(vmem_limit_bytes=limit),
        cost_estimate=pl.CostEstimate(
            flops=6 * rows * model * hidden,
            bytes_accessed=6 * model * hidden,
            transcendentals=rows * hidden,
        ),
        name="experts",
    )(*packets, *ready, pinned(w_gate), pinned(w_up), pinned(w_down))


def spread_kernel(keep_ref, got_ref, mine_ref, *send_refs):
    part = mine_ref.shape[0]
    mine_ref[...] = keep_ref[:part] + got_ref[:part].astype(F32)
    for i, send_ref in enumerate(send_refs):
        rows = slice((i + 1) * part, (i + 2) * part)
        send_ref[...] = (keep_ref[rows] + got_ref[rows].astype(F32)).astype(BF16)


def spread(count, keep, got):
    rows, model = keep.shape
    part = rows // count
    return pl.pallas_call(
        spread_kernel,
        out_shape=[jax.ShapeDtypeStruct((part, model), F32)]
        + [jax.ShapeDtypeStruct((part, model), BF16)] * (count - 1),
        in_specs=vmem(2),
        out_specs=vmem(count),
        compiler_params=pltpu.CompilerParams(vmem_limit_bytes=rows * model * 4 + 2 * MIB),
        name="spread",
    )(keep, got)


def collect_kernel(mine_ref, *refs):
    gots, keep_ref, send_ref = refs[:-2], refs[-2], refs[-1]
    total = mine_ref[...]
    for got in gots:
        total = total + got[...].astype(F32)
    half = total.shape[0] // 2
    keep_ref[...] = total[:half]
    send_ref[...] = total[half:].astype(BF16)


def collect(mine, gots):
    rows, model = mine.shape
    return pl.pallas_call(
        collect_kernel,
        out_shape=(
            jax.ShapeDtypeStruct((rows // 2, model), F32),
            jax.ShapeDtypeStruct((rows // 2, model), BF16),
        ),
        in_specs=vmem(1 + len(gots)),
        out_specs=tuple(vmem(2)),
        compiler_params=pltpu.CompilerParams(vmem_limit_bytes=rows * model * 4 + 2 * MIB),
        name="collect",
    )(mine, *gots)


def last_kernel(keep_ref, got_ref, stream_ref, out_ref):
    total = keep_ref[...] + got_ref[...].astype(F32) + stream_ref[...].astype(F32)
    out_ref[...] = total.astype(BF16)


def last(keep, got, stream):
    return pl.pallas_call(
        last_kernel,
        out_shape=jax.ShapeDtypeStruct(stream.shape, BF16),
        in_specs=vmem(3),
        out_specs=vmem(1)[0],
        compiler_params=pltpu.CompilerParams(vmem_limit_bytes=2 * MIB),
        name="last",
    )(keep, got, stream)


def body(
    experts,
    batches,
    residual_in,
    queries,
    key_new,
    value_new,
    key_cache,
    value_cache,
    cache_len,
    new_slot,
    out_weight,
    norm_gain,
    router,
    chosen,
    w_gate,
    w_up,
    w_down,
):
    def swap(x, axis, size, bit):
        return lax.ppermute(x, axis, [(i, i ^ bit) for i in range(size)])

    near = min(batches, 4)
    far_bits = []
    bit = near
    while bit < batches:
        far_bits.append(bit)
        bit *= 2
    hidden = w_gate.shape[2]
    chunk = min(hidden, 512)
    pieces = [(w, start) for start in range(0, hidden, chunk) for w in (w_gate, w_up)]
    early = [pieces[:FETCH[0]], pieces[FETCH[0] : FETCH[1]]]

    keep, send, base, gain, routing, pick = attend(
        experts, "expert", queries, key_new, value_new, key_cache, value_cache, cache_len, new_slot,
        out_weight, residual_in, norm_gain, router, chosen,
    )
    mine, send = fold(keep, swap(send, "expert", experts, 1))
    got = swap(send, "expert", experts, 2)
    ready, token = fetch(early[0], chunk, send)
    stream, packet = norm(mine, got, base, gain, routing, pick, token)
    for bit in far_bits[::-1]:
        packet = join([packet, swap(packet, "batch", batches, bit)], token)
    around = [swap(packet, "batch", batches, bit) for bit in range(1, near)]
    more, token = fetch(early[1], chunk, packet)
    ready += more
    packet = join([packet] + around, token)
    packets = [packet, swap(packet, "expert", experts, 1)]
    keep, send = expert_ffn("expert", experts, packets, ready, chunk, w_gate, w_up, w_down)
    got = swap(send, "expert", experts, 1)
    if near > 1:
        keep, *sends = spread(near, keep, got)
        gots = [swap(s, "batch", batches, i + 1) for i, s in enumerate(sends)]
    else:
        gots = [got]
    for bit in far_bits:
        keep, send = collect(keep, gots)
        gots = [swap(send, "batch", batches, bit)]
    keep, send = collect(keep, gots)
    got = swap(send, "expert", experts, 2)
    return last(keep, got, stream)


def solution(mesh):
    rows = P(("group", "batch"), None)
    heads = P(("group", "batch"), "expert", None)
    cache = P(("group", "batch"), "expert", None, None)
    slot = P(("group", "batch"))
    in_specs = (
        rows,
        heads,
        heads,
        heads,
        cache,
        cache,
        slot,
        slot,
        P("expert", None),
        P(),
        P(),
        rows,
        P("expert", None, "batch"),
        P("expert", None, "batch"),
        P("expert", "batch", None),
    )
    out_specs = P(("group", "batch", "expert"), None)
    inner = functools.partial(body, mesh.shape["expert"], mesh.shape["batch"])
    return jax.shard_map(inner, mesh=mesh, in_specs=in_specs, out_specs=out_specs, check_vma=False)
```

```python
import functools

import jax
import jax.numpy as jnp
from jax import lax
from jax.experimental import pallas as pl
from jax.experimental.pallas import tpu as pltpu
from jax.sharding import PartitionSpec as P

EPSILON = 1e-05
LANES = 128
MIB = 1 << 20
AHEAD = 6
FETCH = (1, 3)

F32 = jnp.float32
BF16 = jnp.bfloat16


def vmem(count=1):
    return [pl.BlockSpec(memory_space=pltpu.VMEM)] * count


def pinned(x):
    return pltpu.with_memory_space_constraint(x, pltpu.HBM)


def attend_kernel(blocks, axis, *refs):
    sources, outs, rest = refs[:13], refs[13:20], refs[20:]
    keep_ref, send_ref, base_ref, gain_ref, router_ref, pick_ref, down_ref = outs
    (
        k_ref,
        v_ref,
        w_ref,
        q_ref,
        kn_ref,
        vn_ref,
        len_ref,
        new_ref,
        chosen_ref,
        res_ref,
        own_key_ref,
        own_value_ref,
        att_ref,
        sems,
    ) = rest
    slots, heads, width = q_ref.shape
    length = k_ref.shape[2]
    per = slots // blocks
    half = slots // 2
    me = lax.axis_index(axis)
    targets = (len_ref, new_ref, q_ref, kn_ref, k_ref, vn_ref, v_ref, w_ref, chosen_ref, res_ref)
    targets += (gain_ref, router_ref)
    columns = w_ref.shape[1]
    step = min(columns, 1024)
    copies, w_copies = [], []
    for i, (source, target) in enumerate(zip(sources, targets)):
        if target is w_ref:
            copies.append(None)
            for j in range(columns // step):
                part = pl.ds(j * step, step)
                sem = sems.at[len(sources) + j]
                w_copies.append(pltpu.make_async_copy(source.at[:, part], target.at[:, part], sem))
                w_copies[-1].start()
        else:
            copies.append(pltpu.make_async_copy(source, target, sems.at[i]))
            copies[-1].start()
    part = pl.ds(0, down_ref.shape[1])
    copies.append(pltpu.make_async_copy(sources[-1].at[0, :, part], down_ref, sems.at[len(copies)]))
    copies[-1].start()
    scaling = float(width) ** (-0.5)
    places = lax.broadcasted_iota(jnp.int32, (heads, length), 1)
    order = []
    for block in list(range(0, blocks, 2)) + list(range(1, blocks, 2)):
        owner = lax.bitwise_xor(me, block)
        order += [owner * per + i for i in range(per)]
    for copy in copies[:4]:
        copy.wait()
    own_key_ref[...] = kn_ref[...].astype(F32)
    copies[4].wait()
    probs = []
    for slot in order:
        query = q_ref[slot]
        scores = (
            lax.dot_general(
                query, k_ref[slot, 0], (((1,), (1,)), ((), ())), preferred_element_type=F32
            )
            * scaling
        )
        own = (
            jnp.sum(query.astype(F32) * own_key_ref[pl.ds(slot, 1), :], axis=1, keepdims=True)
            * scaling
        )
        usable = (places < len_ref[slot]) & (new_ref[slot] == 0)
        scores = jnp.where(usable, scores, F32(-1e30))
        highest = jnp.maximum(jnp.max(scores, axis=1, keepdims=True), own)
        weights = jnp.where(usable, jnp.exp(scores - highest), F32(0.0))
        own_weight = jnp.exp(own - highest)
        total = jnp.sum(weights, axis=1, keepdims=True) + own_weight
        probs.append(((weights / total).astype(BF16), (own_weight / total).astype(BF16)))
    copies[5].wait()
    own_value_ref[...] = vn_ref[...].astype(F32)
    copies[6].wait()
    for place, slot in enumerate(order):
        prob, own_prob = probs[place]
        attended = jnp.dot(prob, v_ref[slot, 0], preferred_element_type=F32)
        attended = attended + own_prob.astype(F32) * own_value_ref[pl.ds(slot, 1), :]
        att_ref[pl.ds(place * 8, heads), :] = attended
    rows = jnp.concatenate(
        [att_ref[pl.ds(head, slots, stride=8), :] for head in range(heads)], axis=1
    ).astype(BF16)
    for j, start in enumerate(range(0, columns, step)):
        w_copies[j].wait()
        part = jnp.dot(rows, w_ref[:, start : start + step], preferred_element_type=F32)
        keep_ref[:, start : start + step] = part[:half]
        send_ref[:, start : start + step] = part[half:].astype(send_ref.dtype)
    for copy in copies[8:]:
        copy.wait()
    lines = lax.broadcasted_iota(jnp.int32, (half, LANES), 0)
    lanes = lax.broadcasted_iota(jnp.int32, (half, LANES), 1)
    picks = jnp.zeros((half, LANES), jnp.int32)
    for place, slot in enumerate(order[:half]):
        named = jnp.where(lanes == 0, chosen_ref[0, slot], chosen_ref[1, slot])
        picks = jnp.where(lines == place, named, picks)
    pick_ref[...] = picks
    residual = res_ref[...].astype(F32)
    kept = []
    for block in range(0, blocks, 2):
        owner = lax.bitwise_xor(me, block)
        value = residual[:per]
        for other in range(1, blocks):
            value = jnp.where(owner == other, residual[other * per : (other + 1) * per], value)
        kept.append(value)
    base_ref[...] = jnp.concatenate(kept, axis=0)


def attend(
    blocks, axis, queries, key_new, value_new, key_cache, value_cache, lens, new, out_weight,
    residual, gain, router, chosen, w_down, down_chunk,
):
    slots, heads, width = queries.shape
    columns = out_weight.shape[1]
    half = slots // 2
    sources = (
        lens,
        new,
        queries,
        key_new.reshape(slots, width),
        key_cache,
        value_new.reshape(slots, width),
        value_cache,
        out_weight,
        chosen.T,
        residual,
        gain.reshape(1, columns),
        router.T,
        w_down,
    )
    return pl.pallas_call(
        functools.partial(attend_kernel, blocks, axis),
        out_shape=(
            jax.ShapeDtypeStruct((half, columns), F32),
            jax.ShapeDtypeStruct((half, columns), F32),
            jax.ShapeDtypeStruct((half, columns), F32),
            jax.ShapeDtypeStruct((1, columns), F32),
            jax.ShapeDtypeStruct(router.shape[::-1], BF16),
            jax.ShapeDtypeStruct((half, LANES), jnp.int32),
            pltpu.VMEM((w_down.shape[1], down_chunk), BF16),
        ),
        in_specs=[pl.BlockSpec(memory_space=pltpu.HBM)] * len(sources),
        out_specs=tuple(vmem(7)),
        scratch_shapes=[
            pltpu.VMEM(key_cache.shape, BF16),
            pltpu.VMEM(value_cache.shape, BF16),
            pltpu.VMEM(out_weight.shape, BF16),
            pltpu.VMEM(queries.shape, BF16),
            pltpu.VMEM((slots, width), BF16),
            pltpu.VMEM((slots, width), BF16),
            pltpu.SMEM(lens.shape, jnp.int32),
            pltpu.SMEM(new.shape, jnp.int32),
            pltpu.SMEM((chosen.shape[1], slots), jnp.int32),
            pltpu.VMEM(residual.shape, BF16),
            pltpu.VMEM((slots, width), F32),
            pltpu.VMEM((slots, width), F32),
            pltpu.VMEM((slots * 8, width), F32),
            pltpu.SemaphoreType.DMA((len(sources) + columns // min(columns, 1024),)),
        ],
        compiler_params=pltpu.CompilerParams(vmem_limit_bytes=9 * MIB),
        name="attend",
    )(*[pinned(x) for x in sources])


def fold_kernel(keep_ref, got_ref, mine_ref, send_ref):
    total = keep_ref[...] + got_ref[...].astype(F32)
    mine_ref[...] = total
    half = total.shape[0] // 2
    send_ref[0:half, :] = total[half:].astype(send_ref.dtype)
    send_ref[half:, :] = total[:half].astype(send_ref.dtype)


def fold(keep, got):
    return pl.pallas_call(
        fold_kernel,
        out_shape=(
            jax.ShapeDtypeStruct(keep.shape, F32),
            jax.ShapeDtypeStruct(keep.shape, BF16),
        ),
        in_specs=vmem(2),
        out_specs=tuple(vmem(2)),
        compiler_params=pltpu.CompilerParams(vmem_limit_bytes=2 * MIB),
        name="fold",
    )(keep, got)


def norm_kernel(mine_ref, got_ref, base_ref, gain_ref, router_ref, pick_ref, _, stream_ref, packet_ref):
    rows, model = mine_ref.shape
    per = rows // 2
    experts = router_ref.shape[0]
    total = base_ref[...] + (mine_ref[...] + got_ref[...].astype(F32))
    stream = total.astype(BF16)
    stream_ref[...] = stream[:per]
    values = stream.astype(F32)
    scaling = lax.rsqrt(jnp.mean(values * values, axis=1, keepdims=True) + EPSILON)
    normed = (values * scaling * gain_ref[...]).astype(BF16)
    packet_ref[:, :model] = normed
    logits = lax.dot_general(
        normed, router_ref[...], (((1,), (1,)), ((), ())), preferred_element_type=F32
    )
    first, second = pick_ref[:, 0:1], pick_ref[:, 1:2]
    labels = lax.broadcasted_iota(jnp.int32, logits.shape, 1)
    first_logit = jnp.sum(jnp.where(labels == first, logits, 0.0), axis=1, keepdims=True)
    second_logit = jnp.sum(jnp.where(labels == second, logits, 0.0), axis=1, keepdims=True)
    leading = 1.0 / (1.0 + jnp.exp(second_logit - first_logit))
    lanes = lax.broadcasted_iota(jnp.int32, (rows, LANES), 1)
    expert = lax.rem(lanes, experts)
    coef = jnp.where(
        expert == first, leading, jnp.where(expert == second, 1.0 - leading, F32(0.0))
    )
    high = coef.astype(BF16).astype(F32)
    packet_ref[:, model:] = jnp.where(lanes < experts, high, coef - high).astype(BF16)


def norm(mine, got, base, gain, router, pick, token):
    rows, model = mine.shape
    return pl.pallas_call(
        norm_kernel,
        out_shape=(
            jax.ShapeDtypeStruct((rows // 2, model), BF16),
            jax.ShapeDtypeStruct((rows, model + LANES), BF16),
        ),
        in_specs=vmem(6) + [pl.BlockSpec(memory_space=pl.ANY)],
        out_specs=tuple(vmem(2)),
        compiler_params=pltpu.CompilerParams(vmem_limit_bytes=2 * MIB),
        name="norm",
    )(mine, got, base, gain, router, pick, token)


def join_kernel(*refs):
    parts, out_ref = refs[:-2], refs[-1]
    rows = parts[0].shape[0]
    for i, part in enumerate(parts):
        out_ref[i * rows : (i + 1) * rows, :] = part[...]


def join(parts, token):
    rows, columns = parts[0].shape
    return pl.pallas_call(
        join_kernel,
        out_shape=jax.ShapeDtypeStruct((len(parts) * rows, columns), parts[0].dtype),
        in_specs=vmem(len(parts)) + [pl.BlockSpec(memory_space=pl.ANY)],
        out_specs=vmem(1)[0],
        compiler_params=pltpu.CompilerParams(vmem_limit_bytes=2 * MIB),
        name="join",
    )(*parts, token)


def fetch_kernel(starts, *refs):
    count = len(starts)
    sources, outs = refs[:count], refs[count + 1 : 2 * count + 1]
    done_ref, sems = refs[2 * count + 1 :]
    copies = []
    for i, (start, source, out) in enumerate(zip(starts, sources, outs)):
        columns = pl.ds(start, out.shape[1])
        copies.append(pltpu.make_async_copy(source.at[0, :, columns], out, sems.at[i]))
        copies[-1].start()
    done_ref[...] = jnp.zeros_like(done_ref)
    for copy in copies:
        copy.wait()


def fetch(pieces, token):
    count = len(pieces)
    if not count:
        return [], token
    shapes = [(w.shape[1], width) for w, _, width in pieces]
    size = sum(rows * width * 2 for rows, width in shapes)
    *got, done = pl.pallas_call(
        functools.partial(fetch_kernel, [start for _, start, _ in pieces]),
        out_shape=[pltpu.VMEM(shape, BF16) for shape in shapes]
        + [jax.ShapeDtypeStruct((8, LANES), F32)],
        in_specs=[pl.BlockSpec(memory_space=pltpu.HBM)] * count
        + [pl.BlockSpec(memory_space=pl.ANY)],
        out_specs=vmem(count + 1),
        scratch_shapes=[pltpu.SemaphoreType.DMA((count,))],
        compiler_params=pltpu.CompilerParams(vmem_limit_bytes=MIB),
        cost_estimate=pl.CostEstimate(flops=0, bytes_accessed=size, transcendentals=0),
        name="fetch",
    )(*[pinned(w) for w, _, _ in pieces], token)
    return got, done


def expert_kernel(axis, experts, parts, held, held_down, chunk, *refs):
    packets, ready = refs[:parts], refs[parts : parts + held]
    refs = refs[parts + held :]
    ready_down, refs = refs[:held_down], refs[held_down:]
    gate_hbm, up_hbm, down_hbm, keep_ref, send_ref, x_ref, hidden_ref, piece_ref, down_ref = refs[:9]
    piece_sems, down_sems = refs[9:]
    me = lax.axis_index(axis)
    model = x_ref.shape[0] * LANES
    hidden = hidden_ref.shape[0] * LANES
    down_chunk = down_ref.shape[2]
    count = model // down_chunk
    pieces = [(w, start) for start in range(0, hidden, chunk) for w in (gate_hbm, up_hbm)]
    stream = []
    for i in range(held, len(pieces)):
        source, start = pieces[i]
        source = source.at[0, :, pl.ds(start, chunk)]
        stream.append(pltpu.make_async_copy(source, piece_ref.at[i - held], piece_sems.at[i - held]))
    for j in range(held_down, count):
        source = down_hbm.at[0, :, pl.ds(j * down_chunk, down_chunk)]
        slot = j - held_down
        stream.append(pltpu.make_async_copy(source, down_ref.at[slot], down_sems.at[slot]))
    for copy in stream[:AHEAD]:
        copy.start()

    def arrive(n):
        stream[n].wait()
        if n + AHEAD < len(stream):
            stream[n + AHEAD].start()

    rows = packets[0].shape[0]
    coefs = []
    for packet in packets:
        tail = packet[:, model:].astype(F32)
        lanes = lax.broadcasted_iota(jnp.int32, tail.shape, 1)
        mine = (lanes == me) | (lanes == me + experts)
        coefs.append(jnp.sum(jnp.where(mine, tail, 0.0), axis=1, keepdims=True))
    coef = jnp.concatenate(coefs, axis=0)

    def place(k, carry):
        columns = pl.ds(pl.multiple_of(k * LANES, LANES), LANES)
        for i, packet in enumerate(packets):
            x_ref[k, i * rows : (i + 1) * rows, :] = packet[:, columns]
        return carry

    lax.fori_loop(0, model // LANES, place, 0)

    def wide(ref):
        return jnp.concatenate([ref[k] for k in range(ref.shape[0])], axis=1)

    def product(i):
        if i < held:
            return jnp.dot(wide(x_ref), ready[i][...], preferred_element_type=F32)
        arrive(i - held)
        return jnp.dot(wide(x_ref), piece_ref[i - held], preferred_element_type=F32)

    for j in range(hidden // chunk):
        gate, up = product(2 * j), product(2 * j + 1)
        inner = (gate / (1.0 + jnp.exp(-gate)) * up).astype(BF16)
        for k in range(chunk // LANES):
            hidden_ref[j * chunk // LANES + k] = inner[:, k * LANES : (k + 1) * LANES]
    half = x_ref.shape[1] // 2
    for j in range(count):
        cols = slice(j * down_chunk, (j + 1) * down_chunk)
        if j < held_down:
            weight = ready_down[j][...]
        else:
            arrive(len(pieces) - held + j - held_down)
            weight = down_ref[j - held_down]
        out = jnp.dot(wide(hidden_ref), weight, preferred_element_type=F32) * coef
        keep_ref[:, cols] = out[:half]
        send_ref[:, cols] = out[half:].astype(BF16)


def expert_ffn(axis, experts, packets, ready, ready_down, chunk, down_chunk, w_gate, w_up, w_down):
    parts, held, held_down = len(packets), len(ready), len(ready_down)
    rows = parts * packets[0].shape[0]
    model, hidden = w_gate.shape[1:]
    half = rows // 2
    left = max(2 * (hidden // chunk) - held, 1)
    left_down = max(model // down_chunk - held_down, 1)
    scratch = left * model * chunk * 2 + left_down * hidden * down_chunk * 2
    limit = rows * (model + hidden) * 2 + scratch + 1 * MIB
    return pl.pallas_call(
        functools.partial(expert_kernel, axis, experts, parts, held, held_down, chunk),
        out_shape=(
            jax.ShapeDtypeStruct((half, model), F32),
            jax.ShapeDtypeStruct((half, model), BF16),
        ),
        in_specs=vmem(parts + held + held_down) + [pl.BlockSpec(memory_space=pltpu.HBM)] * 3,
        out_specs=tuple(vmem(2)),
        scratch_shapes=[
            pltpu.VMEM((model // LANES, rows, LANES), BF16),
            pltpu.VMEM((hidden // LANES, rows, LANES), BF16),
            pltpu.VMEM((left, model, chunk), BF16),
            pltpu.VMEM((left_down, hidden, down_chunk), BF16),
            pltpu.SemaphoreType.DMA((left,)),
            pltpu.SemaphoreType.DMA((left_down,)),
        ],
        compiler_params=pltpu.CompilerParams(vmem_limit_bytes=limit),
        cost_estimate=pl.CostEstimate(
            flops=6 * rows * model * hidden,
            bytes_accessed=6 * model * hidden,
            transcendentals=rows * hidden,
        ),
        name="experts",
    )(*packets, *ready, *ready_down, pinned(w_gate), pinned(w_up), pinned(w_down))


def spread_kernel(keep_ref, got_ref, mine_ref, *send_refs):
    part = mine_ref.shape[0]
    mine_ref[...] = keep_ref[:part] + got_ref[:part].astype(F32)
    for i, send_ref in enumerate(send_refs):
        rows = slice((i + 1) * part, (i + 2) * part)
        send_ref[...] = (keep_ref[rows] + got_ref[rows].astype(F32)).astype(BF16)


def spread(count, keep, got):
    rows, model = keep.shape
    part = rows // count
    return pl.pallas_call(
        spread_kernel,
        out_shape=[jax.ShapeDtypeStruct((part, model), F32)]
        + [jax.ShapeDtypeStruct((part, model), BF16)] * (count - 1),
        in_specs=vmem(2),
        out_specs=vmem(count),
        compiler_params=pltpu.CompilerParams(vmem_limit_bytes=rows * model * 4 + 2 * MIB),
        name="spread",
    )(keep, got)


def collect_kernel(mine_ref, *refs):
    gots, keep_ref, send_ref = refs[:-2], refs[-2], refs[-1]
    total = mine_ref[...]
    for got in gots:
        total = total + got[...].astype(F32)
    half = total.shape[0] // 2
    keep_ref[...] = total[:half]
    send_ref[...] = total[half:].astype(BF16)


def collect(mine, gots):
    rows, model = mine.shape
    return pl.pallas_call(
        collect_kernel,
        out_shape=(
            jax.ShapeDtypeStruct((rows // 2, model), F32),
            jax.ShapeDtypeStruct((rows // 2, model), BF16),
        ),
        in_specs=vmem(1 + len(gots)),
        out_specs=tuple(vmem(2)),
        compiler_params=pltpu.CompilerParams(vmem_limit_bytes=rows * model * 4 + 2 * MIB),
        name="collect",
    )(mine, *gots)


def last_kernel(keep_ref, got_ref, stream_ref, out_ref):
    total = keep_ref[...] + got_ref[...].astype(F32) + stream_ref[...].astype(F32)
    out_ref[...] = total.astype(BF16)


def last(keep, got, stream):
    return pl.pallas_call(
        last_kernel,
        out_shape=jax.ShapeDtypeStruct(stream.shape, BF16),
        in_specs=vmem(3),
        out_specs=vmem(1)[0],
        compiler_params=pltpu.CompilerParams(vmem_limit_bytes=2 * MIB),
        name="last",
    )(keep, got, stream)


def body(
    experts,
    batches,
    residual_in,
    queries,
    key_new,
    value_new,
    key_cache,
    value_cache,
    cache_len,
    new_slot,
    out_weight,
    norm_gain,
    router,
    chosen,
    w_gate,
    w_up,
    w_down,
):
    def swap(x, axis, size, bit):
        return lax.ppermute(x, axis, [(i, i ^ bit) for i in range(size)])

    near = min(batches, 4)
    far_bits = []
    bit = near
    while bit < batches:
        far_bits.append(bit)
        bit *= 2
    hidden = w_gate.shape[2]
    chunk = min(hidden, 512)
    down_chunk = min(w_down.shape[2], 512)
    pieces = [(w, start, chunk) for start in range(0, hidden, chunk) for w in (w_gate, w_up)]
    early = [pieces[:FETCH[0]], pieces[FETCH[0] : FETCH[1]]]

    keep, send, base, gain, routing, pick, first_down = attend(
        experts, "expert", queries, key_new, value_new, key_cache, value_cache, cache_len, new_slot,
        out_weight, residual_in, norm_gain, router, chosen, w_down, down_chunk,
    )
    mine, send = fold(keep, swap(send, "expert", experts, 1))
    got = swap(send, "expert", experts, 2)
    (*ready, second_down), token = fetch(early[0] + [(w_down, down_chunk, down_chunk)], send)
    stream, packet = norm(mine, got, base, gain, routing, pick, token)
    for bit in far_bits[::-1]:
        packet = join([packet, swap(packet, "batch", batches, bit)], token)
    around = [swap(packet, "batch", batches, bit) for bit in range(1, near)]
    more, token = fetch(early[1], packet)
    ready += more
    packet = join([packet] + around, token)
    packets = [packet, swap(packet, "expert", experts, 1)]
    keep, send = expert_ffn(
        "expert", experts, packets, ready, [first_down, second_down], chunk, down_chunk, w_gate, w_up,
        w_down,
    )
    got = swap(send, "expert", experts, 1)
    if near > 1:
        keep, *sends = spread(near, keep, got)
        gots = [swap(s, "batch", batches, i + 1) for i, s in enumerate(sends)]
    else:
        gots = [got]
    for bit in far_bits:
        keep, send = collect(keep, gots)
        gots = [swap(send, "batch", batches, bit)]
    keep, send = collect(keep, gots)
    got = swap(send, "expert", experts, 2)
    return last(keep, got, stream)


def solution(mesh):
    rows = P(("group", "batch"), None)
    heads = P(("group", "batch"), "expert", None)
    cache = P(("group", "batch"), "expert", None, None)
    slot = P(("group", "batch"))
    in_specs = (
        rows,
        heads,
        heads,
        heads,
        cache,
        cache,
        slot,
        slot,
        P("expert", None),
        P(),
        P(),
        rows,
        P("expert", None, "batch"),
        P("expert", None, "batch"),
        P("expert", "batch", None),
    )
    out_specs = P(("group", "batch", "expert"), None)
    inner = functools.partial(body, mesh.shape["expert"], mesh.shape["batch"])
    return jax.shard_map(inner, mesh=mesh, in_specs=in_specs, out_specs=out_specs, check_vma=False)
```

```python
import functools

import jax
import jax.numpy as jnp
from jax import lax
from jax.experimental import pallas as pl
from jax.experimental.pallas import tpu as pltpu
from jax.sharding import PartitionSpec as P

EPSILON = 1e-05
LANES = 128
MIB = 1 << 20
AHEAD = 6
FETCH = (1, 3)

F32 = jnp.float32
BF16 = jnp.bfloat16


def vmem(count=1):
    return [pl.BlockSpec(memory_space=pltpu.VMEM)] * count


def pinned(x):
    return pltpu.with_memory_space_constraint(x, pltpu.HBM)


def attend_kernel(blocks, axis, *refs):
    sources, outs, rest = refs[:13], refs[13:20], refs[20:]
    keep_ref, send_ref, base_ref, gain_ref, router_ref, pick_ref, down_ref = outs
    (
        k_ref,
        v_ref,
        w_ref,
        q_ref,
        kn_ref,
        vn_ref,
        len_ref,
        new_ref,
        chosen_ref,
        res_ref,
        own_key_ref,
        own_value_ref,
        att_ref,
        sems,
    ) = rest
    slots, heads, width = q_ref.shape
    length = k_ref.shape[2]
    per = slots // blocks
    half = slots // 2
    me = lax.axis_index(axis)
    targets = (len_ref, new_ref, q_ref, kn_ref, k_ref, vn_ref, v_ref, w_ref, chosen_ref, res_ref)
    targets += (gain_ref, router_ref)
    columns = w_ref.shape[1]
    step = min(columns, 1024)
    copies, w_copies = [], []
    for i, (source, target) in enumerate(zip(sources, targets)):
        if target is w_ref:
            copies.append(None)
            for j in range(columns // step):
                part = pl.ds(j * step, step)
                sem = sems.at[len(sources) + j]
                w_copies.append(pltpu.make_async_copy(source.at[:, part], target.at[:, part], sem))
                w_copies[-1].start()
        else:
            copies.append(pltpu.make_async_copy(source, target, sems.at[i]))
            copies[-1].start()
    part = pl.ds(0, down_ref.shape[1])
    copies.append(pltpu.make_async_copy(sources[-1].at[0, :, part], down_ref, sems.at[len(copies)]))
    scaling = float(width) ** (-0.5)
    places = lax.broadcasted_iota(jnp.int32, (heads, length), 1)
    order = []
    for block in list(range(0, blocks, 2)) + list(range(1, blocks, 2)):
        owner = lax.bitwise_xor(me, block)
        order += [owner * per + i for i in range(per)]
    for copy in copies[:4]:
        copy.wait()
    own_key_ref[...] = kn_ref[...].astype(F32)
    copies[4].wait()
    probs = []
    for slot in order:
        query = q_ref[slot]
        scores = (
            lax.dot_general(
                query, k_ref[slot, 0], (((1,), (1,)), ((), ())), preferred_element_type=F32
            )
            * scaling
        )
        own = (
            jnp.sum(query.astype(F32) * own_key_ref[pl.ds(slot, 1), :], axis=1, keepdims=True)
            * scaling
        )
        usable = (places < len_ref[slot]) & (new_ref[slot] == 0)
        scores = jnp.where(usable, scores, F32(-1e30))
        highest = jnp.maximum(jnp.max(scores, axis=1, keepdims=True), own)
        weights = jnp.where(usable, jnp.exp(scores - highest), F32(0.0))
        own_weight = jnp.exp(own - highest)
        total = jnp.sum(weights, axis=1, keepdims=True) + own_weight
        probs.append(((weights / total).astype(BF16), (own_weight / total).astype(BF16)))
    copies[5].wait()
    own_value_ref[...] = vn_ref[...].astype(F32)
    copies[6].wait()
    copies[-1].start()
    for place, slot in enumerate(order):
        prob, own_prob = probs[place]
        attended = jnp.dot(prob, v_ref[slot, 0], preferred_element_type=F32)
        attended = attended + own_prob.astype(F32) * own_value_ref[pl.ds(slot, 1), :]
        att_ref[pl.ds(place * 8, heads), :] = attended
    rows = jnp.concatenate(
        [att_ref[pl.ds(head, slots, stride=8), :] for head in range(heads)], axis=1
    ).astype(BF16)
    for j, start in enumerate(range(0, columns, step)):
        w_copies[j].wait()
        part = jnp.dot(rows, w_ref[:, start : start + step], preferred_element_type=F32)
        keep_ref[:, start : start + step] = part[:half]
        send_ref[:, start : start + step] = part[half:].astype(send_ref.dtype)
    for copy in copies[8:]:
        copy.wait()
    lines = lax.broadcasted_iota(jnp.int32, (half, LANES), 0)
    lanes = lax.broadcasted_iota(jnp.int32, (half, LANES), 1)
    picks = jnp.zeros((half, LANES), jnp.int32)
    for place, slot in enumerate(order[:half]):
        named = jnp.where(lanes == 0, chosen_ref[0, slot], chosen_ref[1, slot])
        picks = jnp.where(lines == place, named, picks)
    pick_ref[...] = picks
    residual = res_ref[...].astype(F32)
    kept = []
    for block in range(0, blocks, 2):
        owner = lax.bitwise_xor(me, block)
        value = residual[:per]
        for other in range(1, blocks):
            value = jnp.where(owner == other, residual[other * per : (other + 1) * per], value)
        kept.append(value)
    base_ref[...] = jnp.concatenate(kept, axis=0)


def attend(
    blocks, axis, queries, key_new, value_new, key_cache, value_cache, lens, new, out_weight,
    residual, gain, router, chosen, w_down, down_chunk,
):
    slots, heads, width = queries.shape
    columns = out_weight.shape[1]
    half = slots // 2
    sources = (
        lens,
        new,
        queries,
        key_new.reshape(slots, width),
        key_cache,
        value_new.reshape(slots, width),
        value_cache,
        out_weight,
        chosen.T,
        residual,
        gain.reshape(1, columns),
        router.T,
        w_down,
    )
    return pl.pallas_call(
        functools.partial(attend_kernel, blocks, axis),
        out_shape=(
            jax.ShapeDtypeStruct((half, columns), F32),
            jax.ShapeDtypeStruct((half, columns), F32),
            jax.ShapeDtypeStruct((half, columns), F32),
            jax.ShapeDtypeStruct((1, columns), F32),
            jax.ShapeDtypeStruct(router.shape[::-1], BF16),
            jax.ShapeDtypeStruct((half, LANES), jnp.int32),
            pltpu.VMEM((w_down.shape[1], down_chunk), BF16),
        ),
        in_specs=[pl.BlockSpec(memory_space=pltpu.HBM)] * len(sources),
        out_specs=tuple(vmem(7)),
        scratch_shapes=[
            pltpu.VMEM(key_cache.shape, BF16),
            pltpu.VMEM(value_cache.shape, BF16),
            pltpu.VMEM(out_weight.shape, BF16),
            pltpu.VMEM(queries.shape, BF16),
            pltpu.VMEM((slots, width), BF16),
            pltpu.VMEM((slots, width), BF16),
            pltpu.SMEM(lens.shape, jnp.int32),
            pltpu.SMEM(new.shape, jnp.int32),
            pltpu.SMEM((chosen.shape[1], slots), jnp.int32),
            pltpu.VMEM(residual.shape, BF16),
            pltpu.VMEM((slots, width), F32),
            pltpu.VMEM((slots, width), F32),
            pltpu.VMEM((slots * 8, width), F32),
            pltpu.SemaphoreType.DMA((len(sources) + columns // min(columns, 1024),)),
        ],
        compiler_params=pltpu.CompilerParams(vmem_limit_bytes=9 * MIB),
        name="attend",
    )(*[pinned(x) for x in sources])


def fold_kernel(keep_ref, got_ref, mine_ref, send_ref):
    total = keep_ref[...] + got_ref[...].astype(F32)
    mine_ref[...] = total
    half = total.shape[0] // 2
    send_ref[0:half, :] = total[half:].astype(send_ref.dtype)
    send_ref[half:, :] = total[:half].astype(send_ref.dtype)


def fold(keep, got):
    return pl.pallas_call(
        fold_kernel,
        out_shape=(
            jax.ShapeDtypeStruct(keep.shape, F32),
            jax.ShapeDtypeStruct(keep.shape, BF16),
        ),
        in_specs=vmem(2),
        out_specs=tuple(vmem(2)),
        compiler_params=pltpu.CompilerParams(vmem_limit_bytes=2 * MIB),
        name="fold",
    )(keep, got)


def norm_kernel(mine_ref, got_ref, base_ref, gain_ref, router_ref, pick_ref, _, stream_ref, packet_ref):
    rows, model = mine_ref.shape
    per = rows // 2
    experts = router_ref.shape[0]
    total = base_ref[...] + (mine_ref[...] + got_ref[...].astype(F32))
    stream = total.astype(BF16)
    stream_ref[...] = stream[:per]
    values = stream.astype(F32)
    scaling = lax.rsqrt(jnp.mean(values * values, axis=1, keepdims=True) + EPSILON)
    normed = (values * scaling * gain_ref[...]).astype(BF16)
    packet_ref[:, :model] = normed
    logits = lax.dot_general(
        normed, router_ref[...], (((1,), (1,)), ((), ())), preferred_element_type=F32
    )
    first, second = pick_ref[:, 0:1], pick_ref[:, 1:2]
    labels = lax.broadcasted_iota(jnp.int32, logits.shape, 1)
    first_logit = jnp.sum(jnp.where(labels == first, logits, 0.0), axis=1, keepdims=True)
    second_logit = jnp.sum(jnp.where(labels == second, logits, 0.0), axis=1, keepdims=True)
    leading = 1.0 / (1.0 + jnp.exp(second_logit - first_logit))
    lanes = lax.broadcasted_iota(jnp.int32, (rows, LANES), 1)
    expert = lax.rem(lanes, experts)
    coef = jnp.where(
        expert == first, leading, jnp.where(expert == second, 1.0 - leading, F32(0.0))
    )
    high = coef.astype(BF16).astype(F32)
    packet_ref[:, model:] = jnp.where(lanes < experts, high, coef - high).astype(BF16)


def norm(mine, got, base, gain, router, pick, token):
    rows, model = mine.shape
    return pl.pallas_call(
        norm_kernel,
        out_shape=(
            jax.ShapeDtypeStruct((rows // 2, model), BF16),
            jax.ShapeDtypeStruct((rows, model + LANES), BF16),
        ),
        in_specs=vmem(6) + [pl.BlockSpec(memory_space=pl.ANY)],
        out_specs=tuple(vmem(2)),
        compiler_params=pltpu.CompilerParams(vmem_limit_bytes=2 * MIB),
        name="norm",
    )(mine, got, base, gain, router, pick, token)


def join_kernel(*refs):
    parts, out_ref = refs[:-2], refs[-1]
    rows = parts[0].shape[0]
    for i, part in enumerate(parts):
        out_ref[i * rows : (i + 1) * rows, :] = part[...]


def join(parts, token):
    rows, columns = parts[0].shape
    return pl.pallas_call(
        join_kernel,
        out_shape=jax.ShapeDtypeStruct((len(parts) * rows, columns), parts[0].dtype),
        in_specs=vmem(len(parts)) + [pl.BlockSpec(memory_space=pl.ANY)],
        out_specs=vmem(1)[0],
        compiler_params=pltpu.CompilerParams(vmem_limit_bytes=2 * MIB),
        name="join",
    )(*parts, token)


def fetch_kernel(starts, *refs):
    count = len(starts)
    sources, outs = refs[:count], refs[count + 1 : 2 * count + 1]
    done_refs, sems = refs[2 * count + 1 : -1], refs[-1]
    copies = []
    for i, (start, source, out) in enumerate(zip(starts, sources, outs)):
        columns = pl.ds(start, out.shape[1])
        copies.append(pltpu.make_async_copy(source.at[0, :, columns], out, sems.at[i]))
        copies[-1].start()
    for done_ref in done_refs:
        done_ref[...] = jnp.zeros_like(done_ref)
    for copy in copies:
        copy.wait()


def fetch(pieces, token, signal=True):
    count = len(pieces)
    if not count:
        return [], token
    shapes = [(w.shape[1], width) for w, _, width in pieces]
    size = sum(rows * width * 2 for rows, width in shapes)
    got = pl.pallas_call(
        functools.partial(fetch_kernel, [start for _, start, _ in pieces]),
        out_shape=[pltpu.VMEM(shape, BF16) for shape in shapes]
        + [jax.ShapeDtypeStruct((8, LANES), F32)] * signal,
        in_specs=[pl.BlockSpec(memory_space=pltpu.HBM)] * count
        + [pl.BlockSpec(memory_space=pl.ANY)],
        out_specs=vmem(count + signal),
        scratch_shapes=[pltpu.SemaphoreType.DMA((count,))],
        compiler_params=pltpu.CompilerParams(vmem_limit_bytes=MIB),
        cost_estimate=pl.CostEstimate(flops=0, bytes_accessed=size, transcendentals=0),
        name="fetch",
    )(*[pinned(w) for w, _, _ in pieces], token)
    return got[:count], got[-1]


def expert_kernel(axis, experts, parts, held, held_down, chunk, *refs):
    packets, ready = refs[:parts], refs[parts : parts + held]
    refs = refs[parts + held :]
    ready_down, refs = refs[:held_down], refs[held_down:]
    gate_hbm, up_hbm, down_hbm, keep_ref, send_ref, x_ref, hidden_ref, piece_ref, down_ref = refs[:9]
    piece_sems, down_sems = refs[9:]
    me = lax.axis_index(axis)
    model = x_ref.shape[0] * LANES
    hidden = hidden_ref.shape[0] * LANES
    down_chunk = down_ref.shape[2]
    count = model // down_chunk
    pieces = [(w, start) for start in range(0, hidden, chunk) for w in (gate_hbm, up_hbm)]
    stream = []
    for i in range(held, len(pieces)):
        source, start = pieces[i]
        source = source.at[0, :, pl.ds(start, chunk)]
        stream.append(pltpu.make_async_copy(source, piece_ref.at[i - held], piece_sems.at[i - held]))
    for j in range(held_down, count):
        source = down_hbm.at[0, :, pl.ds(j * down_chunk, down_chunk)]
        slot = j - held_down
        stream.append(pltpu.make_async_copy(source, down_ref.at[slot], down_sems.at[slot]))
    for copy in stream[:AHEAD]:
        copy.start()

    def arrive(n):
        stream[n].wait()
        if n + AHEAD < len(stream):
            stream[n + AHEAD].start()

    rows = packets[0].shape[0]
    coefs = []
    for packet in packets:
        tail = packet[:, model:].astype(F32)
        lanes = lax.broadcasted_iota(jnp.int32, tail.shape, 1)
        mine = (lanes == me) | (lanes == me + experts)
        coefs.append(jnp.sum(jnp.where(mine, tail, 0.0), axis=1, keepdims=True))
    coef = jnp.concatenate(coefs, axis=0)

    def place(k, carry):
        columns = pl.ds(pl.multiple_of(k * LANES, LANES), LANES)
        for i, packet in enumerate(packets):
            x_ref[k, i * rows : (i + 1) * rows, :] = packet[:, columns]
        return carry

    lax.fori_loop(0, model // LANES, place, 0)

    def wide(ref):
        return jnp.concatenate([ref[k] for k in range(ref.shape[0])], axis=1)

    def product(i):
        if i < held:
            return jnp.dot(wide(x_ref), ready[i][...], preferred_element_type=F32)
        arrive(i - held)
        return jnp.dot(wide(x_ref), piece_ref[i - held], preferred_element_type=F32)

    for j in range(hidden // chunk):
        gate, up = product(2 * j), product(2 * j + 1)
        inner = (gate / (1.0 + jnp.exp(-gate)) * up).astype(BF16)
        for k in range(chunk // LANES):
            hidden_ref[j * chunk // LANES + k] = inner[:, k * LANES : (k + 1) * LANES]
    half = x_ref.shape[1] // 2
    for j in range(count):
        cols = slice(j * down_chunk, (j + 1) * down_chunk)
        if j < held_down:
            weight = ready_down[j][...]
        else:
            arrive(len(pieces) - held + j - held_down)
            weight = down_ref[j - held_down]
        out = jnp.dot(wide(hidden_ref), weight, preferred_element_type=F32) * coef
        keep_ref[:, cols] = out[:half]
        send_ref[:, cols] = out[half:].astype(BF16)


def expert_ffn(axis, experts, packets, ready, ready_down, chunk, down_chunk, w_gate, w_up, w_down):
    parts, held, held_down = len(packets), len(ready), len(ready_down)
    rows = parts * packets[0].shape[0]
    model, hidden = w_gate.shape[1:]
    half = rows // 2
    left = max(2 * (hidden // chunk) - held, 1)
    left_down = max(model // down_chunk - held_down, 1)
    scratch = left * model * chunk * 2 + left_down * hidden * down_chunk * 2
    limit = rows * (model + hidden) * 2 + scratch + 1 * MIB
    return pl.pallas_call(
        functools.partial(expert_kernel, axis, experts, parts, held, held_down, chunk),
        out_shape=(
            jax.ShapeDtypeStruct((half, model), F32),
            jax.ShapeDtypeStruct((half, model), BF16),
        ),
        in_specs=vmem(parts + held + held_down) + [pl.BlockSpec(memory_space=pltpu.HBM)] * 3,
        out_specs=tuple(vmem(2)),
        scratch_shapes=[
            pltpu.VMEM((model // LANES, rows, LANES), BF16),
            pltpu.VMEM((hidden // LANES, rows, LANES), BF16),
            pltpu.VMEM((left, model, chunk), BF16),
            pltpu.VMEM((left_down, hidden, down_chunk), BF16),
            pltpu.SemaphoreType.DMA((left,)),
            pltpu.SemaphoreType.DMA((left_down,)),
        ],
        compiler_params=pltpu.CompilerParams(vmem_limit_bytes=limit),
        cost_estimate=pl.CostEstimate(
            flops=6 * rows * model * hidden,
            bytes_accessed=6 * model * hidden,
            transcendentals=rows * hidden,
        ),
        name="experts",
    )(*packets, *ready, *ready_down, pinned(w_gate), pinned(w_up), pinned(w_down))


def spread_kernel(keep_ref, got_ref, mine_ref, *send_refs):
    part = mine_ref.shape[0]
    mine_ref[...] = keep_ref[:part] + got_ref[:part].astype(F32)
    for i, send_ref in enumerate(send_refs[::-1]):
        rows = slice((i + 1) * part, (i + 2) * part)
        send_ref[...] = (keep_ref[rows] + got_ref[rows].astype(F32)).astype(BF16)


def spread(count, keep, got):
    rows, model = keep.shape
    part = rows // count
    return pl.pallas_call(
        spread_kernel,
        out_shape=[jax.ShapeDtypeStruct((part, model), F32)]
        + [jax.ShapeDtypeStruct((part, model), BF16)] * (count - 1),
        in_specs=vmem(2),
        out_specs=vmem(count),
        compiler_params=pltpu.CompilerParams(vmem_limit_bytes=rows * model * 4 + 2 * MIB),
        name="spread",
    )(keep, got)


def collect_kernel(mine_ref, *refs):
    gots, keep_ref, send_ref = refs[:-2], refs[-2], refs[-1]
    total = mine_ref[...]
    for got in gots:
        total = total + got[...].astype(F32)
    half = total.shape[0] // 2
    keep_ref[...] = total[:half]
    send_ref[...] = total[half:].astype(BF16)


def collect(mine, gots):
    rows, model = mine.shape
    return pl.pallas_call(
        collect_kernel,
        out_shape=(
            jax.ShapeDtypeStruct((rows // 2, model), F32),
            jax.ShapeDtypeStruct((rows // 2, model), BF16),
        ),
        in_specs=vmem(1 + len(gots)),
        out_specs=tuple(vmem(2)),
        compiler_params=pltpu.CompilerParams(vmem_limit_bytes=rows * model * 4 + 2 * MIB),
        name="collect",
    )(mine, *gots)


def last_kernel(keep_ref, got_ref, stream_ref, out_ref):
    total = keep_ref[...] + got_ref[...].astype(F32) + stream_ref[...].astype(F32)
    out_ref[...] = total.astype(BF16)


def last(keep, got, stream):
    return pl.pallas_call(
        last_kernel,
        out_shape=jax.ShapeDtypeStruct(stream.shape, BF16),
        in_specs=vmem(3),
        out_specs=vmem(1)[0],
        compiler_params=pltpu.CompilerParams(vmem_limit_bytes=2 * MIB),
        name="last",
    )(keep, got, stream)


def body(
    experts,
    batches,
    residual_in,
    queries,
    key_new,
    value_new,
    key_cache,
    value_cache,
    cache_len,
    new_slot,
    out_weight,
    norm_gain,
    router,
    chosen,
    w_gate,
    w_up,
    w_down,
):
    def swap(x, axis, size, bit):
        return lax.ppermute(x, axis, [(i, i ^ bit) for i in range(size)])

    near = min(batches, 4)
    far_bits = []
    bit = near
    while bit < batches:
        far_bits.append(bit)
        bit *= 2
    hidden = w_gate.shape[2]
    chunk = min(hidden, 512)
    down_chunk = min(w_down.shape[2], 512)
    pieces = [(w, start, chunk) for start in range(0, hidden, chunk) for w in (w_gate, w_up)]
    early = [pieces[:FETCH[0]], pieces[FETCH[0] : FETCH[1]]]

    keep, send, base, gain, routing, pick, first_down = attend(
        experts, "expert", queries, key_new, value_new, key_cache, value_cache, cache_len, new_slot,
        out_weight, residual_in, norm_gain, router, chosen, w_down, down_chunk,
    )
    mine, send = fold(keep, swap(send, "expert", experts, 1))
    got = swap(send, "expert", experts, 2)
    (*ready, second_down), token = fetch(early[0] + [(w_down, down_chunk, down_chunk)], send)
    stream, packet = norm(mine, got, base, gain, routing, pick, token)
    for bit in far_bits[::-1]:
        packet = join([packet, swap(packet, "batch", batches, bit)], token)
    around = [swap(packet, "batch", batches, bit) for bit in range(1, near)]
    more, token = fetch(early[1], packet)
    ready += more
    packet = join([packet] + around, token)
    packets = [packet, swap(packet, "expert", experts, 1)]
    (third_down,), _ = fetch([(w_down, 2 * down_chunk, down_chunk)], packet, signal=False)
    keep, send = expert_ffn(
        "expert", experts, packets, ready, [first_down, second_down, third_down], chunk, down_chunk, w_gate, w_up,
        w_down,
    )
    got = swap(send, "expert", experts, 1)
    if near > 1:
        keep, *sends = spread(near, keep, got)
        gots = [swap(s, "batch", batches, near - 1 - i) for i, s in enumerate(sends)]
    else:
        gots = [got]
    for bit in far_bits:
        keep, send = collect(keep, gots)
        gots = [swap(send, "batch", batches, bit)]
    keep, send = collect(keep, gots)
    got = swap(send, "expert", experts, 2)
    return last(keep, got, stream)


def solution(mesh):
    rows = P(("group", "batch"), None)
    heads = P(("group", "batch"), "expert", None)
    cache = P(("group", "batch"), "expert", None, None)
    slot = P(("group", "batch"))
    in_specs = (
        rows,
        heads,
        heads,
        heads,
        cache,
        cache,
        slot,
        slot,
        P("expert", None),
        P(),
        P(),
        rows,
        P("expert", None, "batch"),
        P("expert", None, "batch"),
        P("expert", "batch", None),
    )
    out_specs = P(("group", "batch", "expert"), None)
    inner = functools.partial(body, mesh.shape["expert"], mesh.shape["batch"])
    return jax.shard_map(inner, mesh=mesh, in_specs=in_specs, out_specs=out_specs, check_vma=False)
```

```python
import functools

import jax
import jax.numpy as jnp
from jax import lax
from jax.experimental import pallas as pl
from jax.experimental.pallas import tpu as pltpu
from jax.sharding import PartitionSpec as P

EPSILON = 1e-05
LANES = 128
MIB = 1 << 20
AHEAD = 6
FETCH = (1, 3)

F32 = jnp.float32
BF16 = jnp.bfloat16


def vmem(count=1):
    return [pl.BlockSpec(memory_space=pltpu.VMEM)] * count


def pinned(x):
    return pltpu.with_memory_space_constraint(x, pltpu.HBM)


def attend_kernel(blocks, axis, *refs):
    sources, outs, rest = refs[:13], refs[13:20], refs[20:]
    keep_ref, send_ref, base_ref, gain_ref, router_ref, pick_ref, down_ref = outs
    (
        k_ref,
        v_ref,
        w_ref,
        q_ref,
        kn_ref,
        vn_ref,
        len_ref,
        new_ref,
        chosen_ref,
        res_ref,
        own_key_ref,
        own_value_ref,
        att_ref,
        sems,
    ) = rest
    slots, heads, width = q_ref.shape
    length = k_ref.shape[2]
    per = slots // blocks
    half = slots // 2
    me = lax.axis_index(axis)
    targets = (len_ref, new_ref, q_ref, kn_ref, k_ref, vn_ref, v_ref, w_ref, chosen_ref, res_ref)
    targets += (gain_ref, router_ref)
    columns = w_ref.shape[1]
    step = min(columns, 1024)
    copies, w_copies = [], []
    for i, (source, target) in enumerate(zip(sources, targets)):
        if target is w_ref:
            copies.append(None)
            for j in range(columns // step):
                part = pl.ds(j * step, step)
                sem = sems.at[len(sources) + j]
                w_copies.append(pltpu.make_async_copy(source.at[:, part], target.at[:, part], sem))
                w_copies[-1].start(priority=1)
        else:
            copies.append(pltpu.make_async_copy(source, target, sems.at[i]))
            copies[-1].start()
    part = pl.ds(0, down_ref.shape[1])
    copies.append(pltpu.make_async_copy(sources[-1].at[0, :, part], down_ref, sems.at[len(copies)]))
    copies[-1].start(priority=1)
    scaling = float(width) ** (-0.5)
    places = lax.broadcasted_iota(jnp.int32, (heads, length), 1)
    order = []
    for block in list(range(0, blocks, 2)) + list(range(1, blocks, 2)):
        owner = lax.bitwise_xor(me, block)
        order += [owner * per + i for i in range(per)]
    for copy in copies[:4]:
        copy.wait()
    own_key_ref[...] = kn_ref[...].astype(F32)
    copies[4].wait()
    probs = []
    for slot in order:
        query = q_ref[slot]
        scores = (
            lax.dot_general(
                query, k_ref[slot, 0], (((1,), (1,)), ((), ())), preferred_element_type=F32
            )
            * scaling
        )
        own = (
            jnp.sum(query.astype(F32) * own_key_ref[pl.ds(slot, 1), :], axis=1, keepdims=True)
            * scaling
        )
        usable = (places < len_ref[slot]) & (new_ref[slot] == 0)
        scores = jnp.where(usable, scores, F32(-1e30))
        highest = jnp.maximum(jnp.max(scores, axis=1, keepdims=True), own)
        weights = jnp.where(usable, jnp.exp(scores - highest), F32(0.0))
        own_weight = jnp.exp(own - highest)
        total = jnp.sum(weights, axis=1, keepdims=True) + own_weight
        probs.append(((weights / total).astype(BF16), (own_weight / total).astype(BF16)))
    copies[5].wait()
    own_value_ref[...] = vn_ref[...].astype(F32)
    copies[6].wait()
    for place, slot in enumerate(order):
        prob, own_prob = probs[place]
        attended = jnp.dot(prob, v_ref[slot, 0], preferred_element_type=F32)
        attended = attended + own_prob.astype(F32) * own_value_ref[pl.ds(slot, 1), :]
        att_ref[pl.ds(place * 8, heads), :] = attended
    rows = jnp.concatenate(
        [att_ref[pl.ds(head, slots, stride=8), :] for head in range(heads)], axis=1
    ).astype(BF16)
    for j, start in enumerate(range(0, columns, step)):
        w_copies[j].wait()
        part = jnp.dot(rows, w_ref[:, start : start + step], preferred_element_type=F32)
        keep_ref[:, start : start + step] = part[:half]
        send_ref[:, start : start + step] = part[half:].astype(send_ref.dtype)
    for copy in copies[8:]:
        copy.wait()
    lines = lax.broadcasted_iota(jnp.int32, (half, LANES), 0)
    lanes = lax.broadcasted_iota(jnp.int32, (half, LANES), 1)
    picks = jnp.zeros((half, LANES), jnp.int32)
    for place, slot in enumerate(order[:half]):
        named = jnp.where(lanes == 0, chosen_ref[0, slot], chosen_ref[1, slot])
        picks = jnp.where(lines == place, named, picks)
    pick_ref[...] = picks
    residual = res_ref[...].astype(F32)
    kept = []
    for block in range(0, blocks, 2):
        owner = lax.bitwise_xor(me, block)
        value = residual[:per]
        for other in range(1, blocks):
            value = jnp.where(owner == other, residual[other * per : (other + 1) * per], value)
        kept.append(value)
    base_ref[...] = jnp.concatenate(kept, axis=0)


def attend(
    blocks, axis, queries, key_new, value_new, key_cache, value_cache, lens, new, out_weight,
    residual, gain, router, chosen, w_down, down_chunk,
):
    slots, heads, width = queries.shape
    columns = out_weight.shape[1]
    half = slots // 2
    sources = (
        lens,
        new,
        queries,
        key_new.reshape(slots, width),
        key_cache,
        value_new.reshape(slots, width),
        value_cache,
        out_weight,
        chosen.T,
        residual,
        gain.reshape(1, columns),
        router.T,
        w_down,
    )
    return pl.pallas_call(
        functools.partial(attend_kernel, blocks, axis),
        out_shape=(
            jax.ShapeDtypeStruct((half, columns), F32),
            jax.ShapeDtypeStruct((half, columns), F32),
            jax.ShapeDtypeStruct((half, columns), F32),
            jax.ShapeDtypeStruct((1, columns), F32),
            jax.ShapeDtypeStruct(router.shape[::-1], BF16),
            jax.ShapeDtypeStruct((half, LANES), jnp.int32),
            pltpu.VMEM((w_down.shape[1], down_chunk), BF16),
        ),
        in_specs=[pl.BlockSpec(memory_space=pltpu.HBM)] * len(sources),
        out_specs=tuple(vmem(7)),
        scratch_shapes=[
            pltpu.VMEM(key_cache.shape, BF16),
            pltpu.VMEM(value_cache.shape, BF16),
            pltpu.VMEM(out_weight.shape, BF16),
            pltpu.VMEM(queries.shape, BF16),
            pltpu.VMEM((slots, width), BF16),
            pltpu.VMEM((slots, width), BF16),
            pltpu.SMEM(lens.shape, jnp.int32),
            pltpu.SMEM(new.shape, jnp.int32),
            pltpu.SMEM((chosen.shape[1], slots), jnp.int32),
            pltpu.VMEM(residual.shape, BF16),
            pltpu.VMEM((slots, width), F32),
            pltpu.VMEM((slots, width), F32),
            pltpu.VMEM((slots * 8, width), F32),
            pltpu.SemaphoreType.DMA((len(sources) + columns // min(columns, 1024),)),
        ],
        compiler_params=pltpu.CompilerParams(vmem_limit_bytes=9 * MIB),
        name="attend",
    )(*[pinned(x) for x in sources])


def fold_kernel(keep_ref, got_ref, mine_ref, send_ref):
    total = keep_ref[...] + got_ref[...].astype(F32)
    mine_ref[...] = total
    half = total.shape[0] // 2
    send_ref[0:half, :] = total[half:].astype(send_ref.dtype)
    send_ref[half:, :] = total[:half].astype(send_ref.dtype)


def fold(keep, got):
    return pl.pallas_call(
        fold_kernel,
        out_shape=(
            jax.ShapeDtypeStruct(keep.shape, F32),
            jax.ShapeDtypeStruct(keep.shape, BF16),
        ),
        in_specs=vmem(2),
        out_specs=tuple(vmem(2)),
        compiler_params=pltpu.CompilerParams(vmem_limit_bytes=2 * MIB),
        name="fold",
    )(keep, got)


def norm_kernel(mine_ref, got_ref, base_ref, gain_ref, router_ref, pick_ref, _, stream_ref, packet_ref):
    rows, model = mine_ref.shape
    per = rows // 2
    experts = router_ref.shape[0]
    total = base_ref[...] + (mine_ref[...] + got_ref[...].astype(F32))
    stream = total.astype(BF16)
    stream_ref[...] = stream[:per]
    values = stream.astype(F32)
    scaling = lax.rsqrt(jnp.mean(values * values, axis=1, keepdims=True) + EPSILON)
    normed = (values * scaling * gain_ref[...]).astype(BF16)
    packet_ref[:, :model] = normed
    logits = lax.dot_general(
        normed, router_ref[...], (((1,), (1,)), ((), ())), preferred_element_type=F32
    )
    first, second = pick_ref[:, 0:1], pick_ref[:, 1:2]
    labels = lax.broadcasted_iota(jnp.int32, logits.shape, 1)
    first_logit = jnp.sum(jnp.where(labels == first, logits, 0.0), axis=1, keepdims=True)
    second_logit = jnp.sum(jnp.where(labels == second, logits, 0.0), axis=1, keepdims=True)
    leading = 1.0 / (1.0 + jnp.exp(second_logit - first_logit))
    lanes = lax.broadcasted_iota(jnp.int32, (rows, LANES), 1)
    expert = lax.rem(lanes, experts)
    coef = jnp.where(
        expert == first, leading, jnp.where(expert == second, 1.0 - leading, F32(0.0))
    )
    high = coef.astype(BF16).astype(F32)
    packet_ref[:, model:] = jnp.where(lanes < experts, high, coef - high).astype(BF16)


def norm(mine, got, base, gain, router, pick, token):
    rows, model = mine.shape
    return pl.pallas_call(
        norm_kernel,
        out_shape=(
            jax.ShapeDtypeStruct((rows // 2, model), BF16),
            jax.ShapeDtypeStruct((rows, model + LANES), BF16),
        ),
        in_specs=vmem(6) + [pl.BlockSpec(memory_space=pl.ANY)],
        out_specs=tuple(vmem(2)),
        compiler_params=pltpu.CompilerParams(vmem_limit_bytes=2 * MIB),
        name="norm",
    )(mine, got, base, gain, router, pick, token)


def join_kernel(*refs):
    parts, out_ref = refs[:-2], refs[-1]
    rows = parts[0].shape[0]
    for i, part in enumerate(parts):
        out_ref[i * rows : (i + 1) * rows, :] = part[...]


def join(parts, token):
    rows, columns = parts[0].shape
    return pl.pallas_call(
        join_kernel,
        out_shape=jax.ShapeDtypeStruct((len(parts) * rows, columns), parts[0].dtype),
        in_specs=vmem(len(parts)) + [pl.BlockSpec(memory_space=pl.ANY)],
        out_specs=vmem(1)[0],
        compiler_params=pltpu.CompilerParams(vmem_limit_bytes=2 * MIB),
        name="join",
    )(*parts, token)


def fetch_kernel(starts, *refs):
    count = len(starts)
    sources, outs = refs[:count], refs[count + 1 : 2 * count + 1]
    done_ref, sems = refs[2 * count + 1 :]
    copies = []
    for i, (start, source, out) in enumerate(zip(starts, sources, outs)):
        columns = pl.ds(start, out.shape[1])
        copies.append(pltpu.make_async_copy(source.at[0, :, columns], out, sems.at[i]))
        copies[-1].start()
    done_ref[...] = jnp.zeros_like(done_ref)
    for copy in copies:
        copy.wait()


def fetch(pieces, token):
    count = len(pieces)
    if not count:
        return [], token
    shapes = [(w.shape[1], width) for w, _, width in pieces]
    size = sum(rows * width * 2 for rows, width in shapes)
    *got, done = pl.pallas_call(
        functools.partial(fetch_kernel, [start for _, start, _ in pieces]),
        out_shape=[pltpu.VMEM(shape, BF16) for shape in shapes]
        + [jax.ShapeDtypeStruct((8, LANES), F32)],
        in_specs=[pl.BlockSpec(memory_space=pltpu.HBM)] * count
        + [pl.BlockSpec(memory_space=pl.ANY)],
        out_specs=vmem(count + 1),
        scratch_shapes=[pltpu.SemaphoreType.DMA((count,))],
        compiler_params=pltpu.CompilerParams(vmem_limit_bytes=MIB),
        cost_estimate=pl.CostEstimate(flops=0, bytes_accessed=size, transcendentals=0),
        name="fetch",
    )(*[pinned(w) for w, _, _ in pieces], token)
    return got, done


def expert_kernel(axis, experts, parts, held, held_down, chunk, *refs):
    packets, ready = refs[:parts], refs[parts : parts + held]
    refs = refs[parts + held :]
    ready_down, refs = refs[:held_down], refs[held_down:]
    gate_hbm, up_hbm, down_hbm, keep_ref, send_ref, x_ref, hidden_ref, piece_ref, down_ref = refs[:9]
    piece_sems, down_sems = refs[9:]
    me = lax.axis_index(axis)
    model = x_ref.shape[0] * LANES
    hidden = hidden_ref.shape[0] * LANES
    down_chunk = down_ref.shape[2]
    count = model // down_chunk
    pieces = [(w, start) for start in range(0, hidden, chunk) for w in (gate_hbm, up_hbm)]
    stream = []
    for i in range(held, len(pieces)):
        source, start = pieces[i]
        source = source.at[0, :, pl.ds(start, chunk)]
        stream.append(pltpu.make_async_copy(source, piece_ref.at[i - held], piece_sems.at[i - held]))
    for j in range(held_down, count):
        source = down_hbm.at[0, :, pl.ds(j * down_chunk, down_chunk)]
        slot = j - held_down
        stream.append(pltpu.make_async_copy(source, down_ref.at[slot], down_sems.at[slot]))
    for copy in stream[:AHEAD]:
        copy.start()

    def arrive(n):
        stream[n].wait()
        if n + AHEAD < len(stream):
            stream[n + AHEAD].start()

    rows = packets[0].shape[0]
    coefs = []
    for packet in packets:
        tail = packet[:, model:].astype(F32)
        lanes = lax.broadcasted_iota(jnp.int32, tail.shape, 1)
        mine = (lanes == me) | (lanes == me + experts)
        coefs.append(jnp.sum(jnp.where(mine, tail, 0.0), axis=1, keepdims=True))
    coef = jnp.concatenate(coefs, axis=0)

    def place(k, carry):
        columns = pl.ds(pl.multiple_of(k * LANES, LANES), LANES)
        for i, packet in enumerate(packets):
            x_ref[k, i * rows : (i + 1) * rows, :] = packet[:, columns]
        return carry

    lax.fori_loop(0, model // LANES, place, 0)

    def wide(ref):
        return jnp.concatenate([ref[k] for k in range(ref.shape[0])], axis=1)

    def product(i):
        if i < held:
            return jnp.dot(wide(x_ref), ready[i][...], preferred_element_type=F32)
        arrive(i - held)
        return jnp.dot(wide(x_ref), piece_ref[i - held], preferred_element_type=F32)

    for j in range(hidden // chunk):
        gate, up = product(2 * j), product(2 * j + 1)
        inner = (gate / (1.0 + jnp.exp(-gate)) * up).astype(BF16)
        for k in range(chunk // LANES):
            hidden_ref[j * chunk // LANES + k] = inner[:, k * LANES : (k + 1) * LANES]
    half = x_ref.shape[1] // 2
    for j in range(count):
        cols = slice(j * down_chunk, (j + 1) * down_chunk)
        if j < held_down:
            weight = ready_down[j][...]
        else:
            arrive(len(pieces) - held + j - held_down)
            weight = down_ref[j - held_down]
        out = jnp.dot(wide(hidden_ref), weight, preferred_element_type=F32) * coef
        keep_ref[:, cols] = out[:half]
        send_ref[:, cols] = out[half:].astype(BF16)


def expert_ffn(axis, experts, packets, ready, ready_down, chunk, down_chunk, w_gate, w_up, w_down):
    parts, held, held_down = len(packets), len(ready), len(ready_down)
    rows = parts * packets[0].shape[0]
    model, hidden = w_gate.shape[1:]
    half = rows // 2
    left = max(2 * (hidden // chunk) - held, 1)
    left_down = max(model // down_chunk - held_down, 1)
    scratch = left * model * chunk * 2 + left_down * hidden * down_chunk * 2
    limit = rows * (model + hidden) * 2 + scratch + 1 * MIB
    return pl.pallas_call(
        functools.partial(expert_kernel, axis, experts, parts, held, held_down, chunk),
        out_shape=(
            jax.ShapeDtypeStruct((half, model), F32),
            jax.ShapeDtypeStruct((half, model), BF16),
        ),
        in_specs=vmem(parts + held + held_down) + [pl.BlockSpec(memory_space=pltpu.HBM)] * 3,
        out_specs=tuple(vmem(2)),
        scratch_shapes=[
            pltpu.VMEM((model // LANES, rows, LANES), BF16),
            pltpu.VMEM((hidden // LANES, rows, LANES), BF16),
            pltpu.VMEM((left, model, chunk), BF16),
            pltpu.VMEM((left_down, hidden, down_chunk), BF16),
            pltpu.SemaphoreType.DMA((left,)),
            pltpu.SemaphoreType.DMA((left_down,)),
        ],
        compiler_params=pltpu.CompilerParams(vmem_limit_bytes=limit),
        cost_estimate=pl.CostEstimate(
            flops=6 * rows * model * hidden,
            bytes_accessed=6 * model * hidden,
            transcendentals=rows * hidden,
        ),
        name="experts",
    )(*packets, *ready, *ready_down, pinned(w_gate), pinned(w_up), pinned(w_down))


def spread_kernel(keep_ref, got_ref, mine_ref, *send_refs):
    part = mine_ref.shape[0]
    mine_ref[...] = keep_ref[:part] + got_ref[:part].astype(F32)
    for i, send_ref in enumerate(send_refs):
        rows = slice((i + 1) * part, (i + 2) * part)
        send_ref[...] = (keep_ref[rows] + got_ref[rows].astype(F32)).astype(BF16)


def spread(count, keep, got):
    rows, model = keep.shape
    part = rows // count
    return pl.pallas_call(
        spread_kernel,
        out_shape=[jax.ShapeDtypeStruct((part, model), F32)]
        + [jax.ShapeDtypeStruct((part, model), BF16)] * (count - 1),
        in_specs=vmem(2),
        out_specs=vmem(count),
        compiler_params=pltpu.CompilerParams(vmem_limit_bytes=rows * model * 4 + 2 * MIB),
        name="spread",
    )(keep, got)


def collect_kernel(mine_ref, *refs):
    gots, keep_ref, send_ref = refs[:-2], refs[-2], refs[-1]
    total = mine_ref[...]
    for got in gots:
        total = total + got[...].astype(F32)
    half = total.shape[0] // 2
    keep_ref[...] = total[:half]
    send_ref[...] = total[half:].astype(BF16)


def collect(mine, gots):
    rows, model = mine.shape
    return pl.pallas_call(
        collect_kernel,
        out_shape=(
            jax.ShapeDtypeStruct((rows // 2, model), F32),
            jax.ShapeDtypeStruct((rows // 2, model), BF16),
        ),
        in_specs=vmem(1 + len(gots)),
        out_specs=tuple(vmem(2)),
        compiler_params=pltpu.CompilerParams(vmem_limit_bytes=rows * model * 4 + 2 * MIB),
        name="collect",
    )(mine, *gots)


def last_kernel(keep_ref, got_ref, stream_ref, out_ref):
    total = keep_ref[...] + got_ref[...].astype(F32) + stream_ref[...].astype(F32)
    out_ref[...] = total.astype(BF16)


def last(keep, got, stream):
    return pl.pallas_call(
        last_kernel,
        out_shape=jax.ShapeDtypeStruct(stream.shape, BF16),
        in_specs=vmem(3),
        out_specs=vmem(1)[0],
        compiler_params=pltpu.CompilerParams(vmem_limit_bytes=2 * MIB),
        name="last",
    )(keep, got, stream)


def body(
    experts,
    batches,
    residual_in,
    queries,
    key_new,
    value_new,
    key_cache,
    value_cache,
    cache_len,
    new_slot,
    out_weight,
    norm_gain,
    router,
    chosen,
    w_gate,
    w_up,
    w_down,
):
    def swap(x, axis, size, bit):
        return lax.ppermute(x, axis, [(i, i ^ bit) for i in range(size)])

    near = min(batches, 4)
    far_bits = []
    bit = near
    while bit < batches:
        far_bits.append(bit)
        bit *= 2
    hidden = w_gate.shape[2]
    chunk = min(hidden, 512)
    down_chunk = min(w_down.shape[2], 512)
    pieces = [(w, start, chunk) for start in range(0, hidden, chunk) for w in (w_gate, w_up)]
    early = [pieces[:FETCH[0]], pieces[FETCH[0] : FETCH[1]]]

    keep, send, base, gain, routing, pick, first_down = attend(
        experts, "expert", queries, key_new, value_new, key_cache, value_cache, cache_len, new_slot,
        out_weight, residual_in, norm_gain, router, chosen, w_down, down_chunk,
    )
    mine, send = fold(keep, swap(send, "expert", experts, 1))
    got = swap(send, "expert", experts, 2)
    (*ready, second_down), token = fetch(early[0] + [(w_down, down_chunk, down_chunk)], send)
    stream, packet = norm(mine, got, base, gain, routing, pick, token)
    for bit in far_bits[::-1]:
        packet = join([packet, swap(packet, "batch", batches, bit)], token)
    around = [swap(packet, "batch", batches, bit) for bit in range(1, near)]
    more, token = fetch(early[1], packet)
    ready += more
    packet = join([packet] + around, token)
    packets = [packet, swap(packet, "expert", experts, 1)]
    keep, send = expert_ffn(
        "expert", experts, packets, ready, [first_down, second_down], chunk, down_chunk, w_gate, w_up,
        w_down,
    )
    got = swap(send, "expert", experts, 1)
    if near > 1:
        keep, *sends = spread(near, keep, got)
        gots = [swap(s, "batch", batches, i + 1) for i, s in enumerate(sends)]
    else:
        gots = [got]
    for bit in far_bits:
        keep, send = collect(keep, gots)
        gots = [swap(send, "batch", batches, bit)]
    keep, send = collect(keep, gots)
    got = swap(send, "expert", experts, 2)
    return last(keep, got, stream)


def solution(mesh):
    rows = P(("group", "batch"), None)
    heads = P(("group", "batch"), "expert", None)
    cache = P(("group", "batch"), "expert", None, None)
    slot = P(("group", "batch"))
    in_specs = (
        rows,
        heads,
        heads,
        heads,
        cache,
        cache,
        slot,
        slot,
        P("expert", None),
        P(),
        P(),
        rows,
        P("expert", None, "batch"),
        P("expert", None, "batch"),
        P("expert", "batch", None),
    )
    out_specs = P(("group", "batch", "expert"), None)
    inner = functools.partial(body, mesh.shape["expert"], mesh.shape["batch"])
    return jax.shard_map(inner, mesh=mesh, in_specs=in_specs, out_specs=out_specs, check_vma=False)
```

```python
import functools

import jax
import jax.numpy as jnp
from jax import lax
from jax.experimental import pallas as pl
from jax.experimental.pallas import tpu as pltpu
from jax.sharding import PartitionSpec as P

EPSILON = 1e-05
LANES = 128
MIB = 1 << 20
AHEAD = 6
FETCH = (1, 3)

F32 = jnp.float32
BF16 = jnp.bfloat16


def vmem(count=1):
    return [pl.BlockSpec(memory_space=pltpu.VMEM)] * count


def pinned(x):
    return pltpu.with_memory_space_constraint(x, pltpu.HBM)


def attend_kernel(blocks, axis, *refs):
    sources, outs, rest = refs[:13], refs[13:20], refs[20:]
    keep_ref, send_ref, base_ref, gain_ref, router_ref, pick_ref, down_ref = outs
    (
        k_ref,
        v_ref,
        w_ref,
        q_ref,
        kn_ref,
        vn_ref,
        len_ref,
        new_ref,
        chosen_ref,
        res_ref,
        own_key_ref,
        own_value_ref,
        att_ref,
        sems,
    ) = rest
    slots, heads, width = q_ref.shape
    length = k_ref.shape[2]
    per = slots // blocks
    half = slots // 2
    me = lax.axis_index(axis)
    targets = (len_ref, new_ref, q_ref, kn_ref, k_ref, vn_ref, v_ref, w_ref, chosen_ref, res_ref)
    targets += (gain_ref, router_ref)
    columns = w_ref.shape[1]
    step = min(columns, 1024)
    copies, w_copies = [], []
    for i, (source, target) in enumerate(zip(sources, targets)):
        if target is w_ref:
            copies.append(None)
            for j in range(columns // step):
                part = pl.ds(j * step, step)
                sem = sems.at[len(sources) + j]
                w_copies.append(pltpu.make_async_copy(source.at[:, part], target.at[:, part], sem))
                w_copies[-1].start()
        else:
            copies.append(pltpu.make_async_copy(source, target, sems.at[i]))
            copies[-1].start()
    part = pl.ds(0, down_ref.shape[1])
    copies.append(pltpu.make_async_copy(sources[-1].at[0, :, part], down_ref, sems.at[len(copies)]))
    copies[-1].start()
    scaling = float(width) ** (-0.5)
    places = lax.broadcasted_iota(jnp.int32, (heads, length), 1)
    order = []
    for block in list(range(0, blocks, 2)) + list(range(1, blocks, 2)):
        owner = lax.bitwise_xor(me, block)
        order += [owner * per + i for i in range(per)]
    for copy in copies[:4]:
        copy.wait()
    own_key_ref[...] = kn_ref[...].astype(F32)
    copies[4].wait()
    probs = []
    for slot in order:
        query = q_ref[slot]
        scores = (
            lax.dot_general(
                query, k_ref[slot, 0], (((1,), (1,)), ((), ())), preferred_element_type=F32
            )
            * scaling
        )
        own = (
            jnp.sum(query.astype(F32) * own_key_ref[pl.ds(slot, 1), :], axis=1, keepdims=True)
            * scaling
        )
        usable = (places < len_ref[slot]) & (new_ref[slot] == 0)
        scores = jnp.where(usable, scores, F32(-1e30))
        highest = jnp.maximum(jnp.max(scores, axis=1, keepdims=True), own)
        weights = jnp.where(usable, jnp.exp(scores - highest), F32(0.0))
        own_weight = jnp.exp(own - highest)
        total = jnp.sum(weights, axis=1, keepdims=True) + own_weight
        probs.append(((weights / total).astype(BF16), (own_weight / total).astype(BF16)))
    copies[5].wait()
    own_value_ref[...] = vn_ref[...].astype(F32)
    copies[6].wait()
    for place, slot in enumerate(order):
        prob, own_prob = probs[place]
        attended = jnp.dot(prob, v_ref[slot, 0], preferred_element_type=F32)
        attended = attended + own_prob.astype(F32) * own_value_ref[pl.ds(slot, 1), :]
        att_ref[pl.ds(place * 8, heads), :] = attended
    rows = jnp.concatenate(
        [att_ref[pl.ds(head, slots, stride=8), :] for head in range(heads)], axis=1
    ).astype(BF16)
    for j, start in enumerate(range(0, columns, step)):
        w_copies[j].wait()
        part = jnp.dot(rows, w_ref[:, start : start + step], preferred_element_type=F32)
        keep_ref[:, start : start + step] = part[:half]
        send_ref[:, start : start + step] = part[half:].astype(send_ref.dtype)
    for copy in copies[8:]:
        copy.wait()
    lines = lax.broadcasted_iota(jnp.int32, (half, LANES), 0)
    lanes = lax.broadcasted_iota(jnp.int32, (half, LANES), 1)
    picks = jnp.zeros((half, LANES), jnp.int32)
    for place, slot in enumerate(order[:half]):
        named = jnp.where(lanes == 0, chosen_ref[0, slot], chosen_ref[1, slot])
        picks = jnp.where(lines == place, named, picks)
    pick_ref[...] = picks
    residual = res_ref[...].astype(F32)
    kept = []
    for block in range(0, blocks, 2):
        owner = lax.bitwise_xor(me, block)
        value = residual[:per]
        for other in range(1, blocks):
            value = jnp.where(owner == other, residual[other * per : (other + 1) * per], value)
        kept.append(value)
    base_ref[...] = jnp.concatenate(kept, axis=0)


def attend(
    blocks, axis, queries, key_new, value_new, key_cache, value_cache, lens, new, out_weight,
    residual, gain, router, chosen, w_down, down_chunk,
):
    slots, heads, width = queries.shape
    columns = out_weight.shape[1]
    half = slots // 2
    sources = (
        lens,
        new,
        queries,
        key_new.reshape(slots, width),
        key_cache,
        value_new.reshape(slots, width),
        value_cache,
        out_weight,
        chosen.T,
        residual,
        gain.reshape(1, columns),
        router.T,
        w_down,
    )
    return pl.pallas_call(
        functools.partial(attend_kernel, blocks, axis),
        out_shape=(
            jax.ShapeDtypeStruct((half, columns), F32),
            jax.ShapeDtypeStruct((half, columns), F32),
            jax.ShapeDtypeStruct((half, columns), F32),
            jax.ShapeDtypeStruct((1, columns), F32),
            jax.ShapeDtypeStruct(router.shape[::-1], BF16),
            jax.ShapeDtypeStruct((half, LANES), jnp.int32),
            pltpu.VMEM((w_down.shape[1], down_chunk), BF16),
        ),
        in_specs=[pl.BlockSpec(memory_space=pltpu.HBM)] * len(sources),
        out_specs=tuple(vmem(7)),
        scratch_shapes=[
            pltpu.VMEM(key_cache.shape, BF16),
            pltpu.VMEM(value_cache.shape, BF16),
            pltpu.VMEM(out_weight.shape, BF16),
            pltpu.VMEM(queries.shape, BF16),
            pltpu.VMEM((slots, width), BF16),
            pltpu.VMEM((slots, width), BF16),
            pltpu.SMEM(lens.shape, jnp.int32),
            pltpu.SMEM(new.shape, jnp.int32),
            pltpu.SMEM((chosen.shape[1], slots), jnp.int32),
            pltpu.VMEM(residual.shape, BF16),
            pltpu.VMEM((slots, width), F32),
            pltpu.VMEM((slots, width), F32),
            pltpu.VMEM((slots * 8, width), F32),
            pltpu.SemaphoreType.DMA((len(sources) + columns // min(columns, 1024),)),
        ],
        compiler_params=pltpu.CompilerParams(vmem_limit_bytes=9 * MIB),
        name="attend",
    )(*[pinned(x) for x in sources])


def fold_kernel(keep_ref, got_ref, mine_ref, send_ref):
    total = keep_ref[...] + got_ref[...].astype(F32)
    mine_ref[...] = total
    half = total.shape[0] // 2
    send_ref[0:half, :] = total[half:].astype(send_ref.dtype)
    send_ref[half:, :] = total[:half].astype(send_ref.dtype)


def fold(keep, got):
    return pl.pallas_call(
        fold_kernel,
        out_shape=(
            jax.ShapeDtypeStruct(keep.shape, F32),
            jax.ShapeDtypeStruct(keep.shape, BF16),
        ),
        in_specs=vmem(2),
        out_specs=tuple(vmem(2)),
        compiler_params=pltpu.CompilerParams(vmem_limit_bytes=2 * MIB),
        name="fold",
    )(keep, got)


def norm_kernel(mine_ref, got_ref, base_ref, gain_ref, router_ref, pick_ref, _, stream_ref, packet_ref):
    rows, model = mine_ref.shape
    per = rows // 2
    experts = router_ref.shape[0]
    total = base_ref[...] + (mine_ref[...] + got_ref[...].astype(F32))
    stream = total.astype(BF16)
    stream_ref[...] = stream[:per]
    values = stream.astype(F32)
    scaling = lax.rsqrt(jnp.mean(values * values, axis=1, keepdims=True) + EPSILON)
    normed = (values * scaling * gain_ref[...]).astype(BF16)
    packet_ref[:, :model] = normed
    logits = lax.dot_general(
        normed, router_ref[...], (((1,), (1,)), ((), ())), preferred_element_type=F32
    )
    first, second = pick_ref[:, 0:1], pick_ref[:, 1:2]
    labels = lax.broadcasted_iota(jnp.int32, logits.shape, 1)
    first_logit = jnp.sum(jnp.where(labels == first, logits, 0.0), axis=1, keepdims=True)
    second_logit = jnp.sum(jnp.where(labels == second, logits, 0.0), axis=1, keepdims=True)
    leading = 1.0 / (1.0 + jnp.exp(second_logit - first_logit))
    lanes = lax.broadcasted_iota(jnp.int32, (rows, LANES), 1)
    expert = lax.rem(lanes, experts)
    coef = jnp.where(
        expert == first, leading, jnp.where(expert == second, 1.0 - leading, F32(0.0))
    )
    high = coef.astype(BF16).astype(F32)
    packet_ref[:, model:] = jnp.where(lanes < experts, high, coef - high).astype(BF16)


def norm(mine, got, base, gain, router, pick, token):
    rows, model = mine.shape
    return pl.pallas_call(
        norm_kernel,
        out_shape=(
            jax.ShapeDtypeStruct((rows // 2, model), BF16),
            jax.ShapeDtypeStruct((rows, model + LANES), BF16),
        ),
        in_specs=vmem(6) + [pl.BlockSpec(memory_space=pl.ANY)],
        out_specs=tuple(vmem(2)),
        compiler_params=pltpu.CompilerParams(vmem_limit_bytes=2 * MIB),
        name="norm",
    )(mine, got, base, gain, router, pick, token)


def join_kernel(*refs):
    parts, out_ref = refs[:-2], refs[-1]
    rows = parts[0].shape[0]
    for i, part in enumerate(parts):
        out_ref[i * rows : (i + 1) * rows, :] = part[...]


def join(parts, token):
    rows, columns = parts[0].shape
    return pl.pallas_call(
        join_kernel,
        out_shape=jax.ShapeDtypeStruct((len(parts) * rows, columns), parts[0].dtype),
        in_specs=vmem(len(parts)) + [pl.BlockSpec(memory_space=pl.ANY)],
        out_specs=vmem(1)[0],
        compiler_params=pltpu.CompilerParams(vmem_limit_bytes=2 * MIB),
        name="join",
    )(*parts, token)


def fetch_kernel(starts, *refs):
    count = len(starts)
    sources, outs = refs[:count], refs[count + 1 : 2 * count + 1]
    done_ref, sems = refs[2 * count + 1 :]
    copies = []
    for i, (start, source, out) in enumerate(zip(starts, sources, outs)):
        columns = pl.ds(start, out.shape[1])
        copies.append(pltpu.make_async_copy(source.at[0, :, columns], out, sems.at[i]))
        copies[-1].start()
    done_ref[...] = jnp.zeros_like(done_ref)
    for copy in copies:
        copy.wait()


def fetch(pieces, token):
    count = len(pieces)
    if not count:
        return [], token
    shapes = [(w.shape[1], width) for w, _, width in pieces]
    size = sum(rows * width * 2 for rows, width in shapes)
    *got, done = pl.pallas_call(
        functools.partial(fetch_kernel, [start for _, start, _ in pieces]),
        out_shape=[pltpu.VMEM(shape, BF16) for shape in shapes]
        + [jax.ShapeDtypeStruct((8, LANES), F32)],
        in_specs=[pl.BlockSpec(memory_space=pltpu.HBM)] * count
        + [pl.BlockSpec(memory_space=pl.ANY)],
        out_specs=vmem(count + 1),
        scratch_shapes=[pltpu.SemaphoreType.DMA((count,))],
        compiler_params=pltpu.CompilerParams(vmem_limit_bytes=MIB),
        cost_estimate=pl.CostEstimate(flops=0, bytes_accessed=size, transcendentals=0),
        name="fetch",
    )(*[pinned(w) for w, _, _ in pieces], token)
    return got, done


def expert_kernel(axis, experts, parts, held, held_down, chunk, *refs):
    packets, ready = refs[:parts], refs[parts : parts + held]
    refs = refs[parts + held :]
    ready_down, refs = refs[:held_down], refs[held_down:]
    gate_hbm, up_hbm, down_hbm, keep_ref, send_ref, x_ref, hidden_ref, piece_ref, down_ref = refs[:9]
    piece_sems, down_sems = refs[9:]
    me = lax.axis_index(axis)
    model = x_ref.shape[0] * LANES
    hidden = hidden_ref.shape[0] * LANES
    down_chunk = down_ref.shape[2]
    count = model // down_chunk
    pieces = [(w, start) for start in range(0, hidden, chunk) for w in (gate_hbm, up_hbm)]
    stream = []
    for i in range(held, len(pieces)):
        source, start = pieces[i]
        source = source.at[0, :, pl.ds(start, chunk)]
        stream.append(pltpu.make_async_copy(source, piece_ref.at[i - held], piece_sems.at[i - held]))
    for j in range(held_down, count):
        source = down_hbm.at[0, :, pl.ds(j * down_chunk, down_chunk)]
        slot = j - held_down
        stream.append(pltpu.make_async_copy(source, down_ref.at[slot], down_sems.at[slot]))
    for copy in stream[:AHEAD]:
        copy.start()

    def arrive(n):
        stream[n].wait()
        if n + AHEAD < len(stream):
            stream[n + AHEAD].start()

    rows = packets[0].shape[0]
    coefs = []
    for packet in packets:
        tail = packet[:, model:].astype(F32)
        lanes = lax.broadcasted_iota(jnp.int32, tail.shape, 1)
        mine = (lanes == me) | (lanes == me + experts)
        coefs.append(jnp.sum(jnp.where(mine, tail, 0.0), axis=1, keepdims=True))
    coef = jnp.concatenate(coefs, axis=0)

    def place(k, carry):
        columns = pl.ds(pl.multiple_of(k * LANES, LANES), LANES)
        for i, packet in enumerate(packets):
            x_ref[k, i * rows : (i + 1) * rows, :] = packet[:, columns]
        return carry

    lax.fori_loop(0, model // LANES, place, 0)

    def wide(ref):
        return jnp.concatenate([ref[k] for k in range(ref.shape[0])], axis=1)

    def product(i):
        if i < held:
            return jnp.dot(wide(x_ref), ready[i][...], preferred_element_type=F32)
        arrive(i - held)
        return jnp.dot(wide(x_ref), piece_ref[i - held], preferred_element_type=F32)

    for j in range(hidden // chunk):
        gate, up = product(2 * j), product(2 * j + 1)
        inner = (gate / (1.0 + jnp.exp(-gate)) * up).astype(BF16)
        for k in range(chunk // LANES):
            hidden_ref[j * chunk // LANES + k] = inner[:, k * LANES : (k + 1) * LANES]
    half = x_ref.shape[1] // 2
    for j in range(count):
        cols = slice(j * down_chunk, (j + 1) * down_chunk)
        if j < held_down:
            weight = ready_down[j][...]
        else:
            arrive(len(pieces) - held + j - held_down)
            weight = down_ref[j - held_down]
        out = jnp.dot(wide(hidden_ref), weight, preferred_element_type=F32) * coef
        keep_ref[:, cols] = out[:half]
        send_ref[:, cols] = out[half:].astype(BF16)


def expert_ffn(axis, experts, packets, ready, ready_down, chunk, down_chunk, w_gate, w_up, w_down):
    parts, held, held_down = len(packets), len(ready), len(ready_down)
    rows = parts * packets[0].shape[0]
    model, hidden = w_gate.shape[1:]
    half = rows // 2
    left = max(2 * (hidden // chunk) - held, 1)
    left_down = max(model // down_chunk - held_down, 1)
    scratch = left * model * chunk * 2 + left_down * hidden * down_chunk * 2
    limit = rows * (model + hidden) * 2 + scratch + 1 * MIB
    return pl.pallas_call(
        functools.partial(expert_kernel, axis, experts, parts, held, held_down, chunk),
        out_shape=(
            jax.ShapeDtypeStruct((half, model), F32),
            jax.ShapeDtypeStruct((half, model), BF16),
        ),
        in_specs=vmem(parts + held + held_down) + [pl.BlockSpec(memory_space=pltpu.HBM)] * 3,
        out_specs=tuple(vmem(2)),
        scratch_shapes=[
            pltpu.VMEM((model // LANES, rows, LANES), BF16),
            pltpu.VMEM((hidden // LANES, rows, LANES), BF16),
            pltpu.VMEM((left, model, chunk), BF16),
            pltpu.VMEM((left_down, hidden, down_chunk), BF16),
            pltpu.SemaphoreType.DMA((left,)),
            pltpu.SemaphoreType.DMA((left_down,)),
        ],
        compiler_params=pltpu.CompilerParams(vmem_limit_bytes=limit),
        cost_estimate=pl.CostEstimate(
            flops=6 * rows * model * hidden,
            bytes_accessed=6 * model * hidden,
            transcendentals=rows * hidden,
        ),
        name="experts",
    )(*packets, *ready, *ready_down, pinned(w_gate), pinned(w_up), pinned(w_down))


def spread_kernel(keep_ref, got_ref, mine_ref, *send_refs):
    part = mine_ref.shape[0]
    mine_ref[...] = keep_ref[:part] + got_ref[:part].astype(F32)
    for i, send_ref in enumerate(send_refs):
        rows = slice((i + 1) * part, (i + 2) * part)
        send_ref[...] = (keep_ref[rows] + got_ref[rows].astype(F32)).astype(BF16)


def spread(count, keep, got):
    rows, model = keep.shape
    part = rows // count
    return pl.pallas_call(
        spread_kernel,
        out_shape=[jax.ShapeDtypeStruct((part, model), F32)]
        + [jax.ShapeDtypeStruct((part, model), BF16)] * (count - 1),
        in_specs=vmem(2),
        out_specs=vmem(count),
        compiler_params=pltpu.CompilerParams(vmem_limit_bytes=rows * model * 4 + 2 * MIB),
        name="spread",
    )(keep, got)


def collect_kernel(mine_ref, *refs):
    gots, keep_ref, send_ref = refs[:-2], refs[-2], refs[-1]
    total = mine_ref[...]
    for got in gots:
        total = total + got[...].astype(F32)
    half = total.shape[0] // 2
    keep_ref[...] = total[:half]
    send_ref[...] = total[half:].astype(BF16)


def collect(mine, gots):
    rows, model = mine.shape
    return pl.pallas_call(
        collect_kernel,
        out_shape=(
            jax.ShapeDtypeStruct((rows // 2, model), F32),
            jax.ShapeDtypeStruct((rows // 2, model), BF16),
        ),
        in_specs=vmem(1 + len(gots)),
        out_specs=tuple(vmem(2)),
        compiler_params=pltpu.CompilerParams(vmem_limit_bytes=rows * model * 4 + 2 * MIB),
        name="collect",
    )(mine, *gots)


def cross(per, keep, got):
    rows, model = keep.shape

    def kernel(keep_ref, got_ref, mine_ref, send_ref):
        total = keep_ref[...] + got_ref[...].astype(F32)
        for i in range(rows // (2 * per)):
            block = total[2 * i * per : 2 * (i + 1) * per]
            mine_ref[i * per : (i + 1) * per, :] = block[:per]
            send_ref[i * per : (i + 1) * per, :] = block[per:].astype(BF16)

    return pl.pallas_call(
        kernel,
        out_shape=(
            jax.ShapeDtypeStruct((rows // 2, model), F32),
            jax.ShapeDtypeStruct((rows // 2, model), BF16),
        ),
        in_specs=vmem(2),
        out_specs=tuple(vmem(2)),
        compiler_params=pltpu.CompilerParams(vmem_limit_bytes=rows * model * 8 + 2 * MIB),
        name="cross",
    )(keep, got)


def last_kernel(stream_ref, keep_ref, *refs):
    gots, out_ref = refs[:-1], refs[-1]
    total = keep_ref[...]
    for got in gots:
        total = total + got[...].astype(F32)
    out_ref[...] = (total + stream_ref[...].astype(F32)).astype(BF16)


def last(keep, gots, stream):
    return pl.pallas_call(
        last_kernel,
        out_shape=jax.ShapeDtypeStruct(stream.shape, BF16),
        in_specs=vmem(2 + len(gots)),
        out_specs=vmem(1)[0],
        compiler_params=pltpu.CompilerParams(vmem_limit_bytes=2 * MIB),
        name="last",
    )(stream, keep, *gots)


def body(
    experts,
    batches,
    residual_in,
    queries,
    key_new,
    value_new,
    key_cache,
    value_cache,
    cache_len,
    new_slot,
    out_weight,
    norm_gain,
    router,
    chosen,
    w_gate,
    w_up,
    w_down,
):
    def swap(x, axis, size, bit):
        return lax.ppermute(x, axis, [(i, i ^ bit) for i in range(size)])

    near = min(batches, 4)
    far_bits = []
    bit = near
    while bit < batches:
        far_bits.append(bit)
        bit *= 2
    hidden = w_gate.shape[2]
    chunk = min(hidden, 512)
    down_chunk = min(w_down.shape[2], 512)
    pieces = [(w, start, chunk) for start in range(0, hidden, chunk) for w in (w_gate, w_up)]
    early = [pieces[:FETCH[0]], pieces[FETCH[0] : FETCH[1]]]

    keep, send, base, gain, routing, pick, first_down = attend(
        experts, "expert", queries, key_new, value_new, key_cache, value_cache, cache_len, new_slot,
        out_weight, residual_in, norm_gain, router, chosen, w_down, down_chunk,
    )
    mine, send = fold(keep, swap(send, "expert", experts, 1))
    got = swap(send, "expert", experts, 2)
    (*ready, second_down), token = fetch(early[0] + [(w_down, down_chunk, down_chunk)], send)
    stream, packet = norm(mine, got, base, gain, routing, pick, token)
    for bit in far_bits[::-1]:
        packet = join([packet, swap(packet, "batch", batches, bit)], token)
    around = [swap(packet, "batch", batches, bit) for bit in range(1, near)]
    more, token = fetch(early[1], packet)
    ready += more
    packet = join([packet] + around, token)
    packets = [packet, swap(packet, "expert", experts, 1)]
    keep, send = expert_ffn(
        "expert", experts, packets, ready, [first_down, second_down], chunk, down_chunk, w_gate, w_up,
        w_down,
    )
    keep, send = cross(stream.shape[0], keep, swap(send, "expert", experts, 1))
    got = swap(send, "expert", experts, 2)
    if near > 1:
        keep, *sends = spread(near, keep, got)
        gots = [swap(s, "batch", batches, i + 1) for i, s in enumerate(sends)]
    else:
        gots = [got]
    for bit in far_bits:
        keep, send = collect(keep, gots)
        gots = [swap(send, "batch", batches, bit)]
    return last(keep, gots, stream)


def solution(mesh):
    rows = P(("group", "batch"), None)
    heads = P(("group", "batch"), "expert", None)
    cache = P(("group", "batch"), "expert", None, None)
    slot = P(("group", "batch"))
    in_specs = (
        rows,
        heads,
        heads,
        heads,
        cache,
        cache,
        slot,
        slot,
        P("expert", None),
        P(),
        P(),
        rows,
        P("expert", None, "batch"),
        P("expert", None, "batch"),
        P("expert", "batch", None),
    )
    out_specs = P(("group", "batch", "expert"), None)
    inner = functools.partial(body, mesh.shape["expert"], mesh.shape["batch"])
    return jax.shard_map(inner, mesh=mesh, in_specs=in_specs, out_specs=out_specs, check_vma=False)
```
